32 devices in a mesh: dp: 8 (over y, x, core), seq: 4 (over z).
Axes of the slice: x: 2, y: 2, z: 4, core: 2. Of those that a mesh axis runs over, the one named last changes fastest.
Arguments:
- tokens: bfloat16 [16384, 1024], P(('dp', 'seq')), may hold values from -6 to 6
- cotangent: bfloat16 [16384, 1024], P(('dp', 'seq')), may hold values from -6 to 6
- qkv_weight: bfloat16 [1024, 3072], replicated, may hold values from -0.1875 to 0.1875
- proj_weight: bfloat16 [1024, 1024], replicated, may hold values from -0.75 to 0.75
- up_weight: bfloat16 [1024, 4096], replicated, may hold values from -0.1875 to 0.1875
- down_weight: bfloat16 [4096, 1024], replicated, may hold values from -0.09375 to 0.09375
- norm_gains: float32 [2, 1024], replicated, may hold values from 0.5 to 1.5
- biases: float32 [6, 1024], replicated, may hold values from -1.5 to 1.5
- up_bias: float32 [4096], replicated, may hold values from -1.5 to 1.5
- head_slopes: float32 [16], replicated, may hold values from 0.00012207031 to 0.5, as said below
- qkv_moment: float32 [1024, 3072], P(None, 'dp'), may hold values from -1536 to 1536
- proj_moment: float32 [1024, 1024], P(None, 'dp'), may hold values from -1536 to 1536
- up_moment: float32 [1024, 4096], P(None, 'dp'), may hold values from -1536 to 1536
- down_moment: float32 [4096, 1024], P('dp'), may hold values from -1536 to 1536
- gains_moment: float32 [2, 1024], P(None, 'dp'), may hold values from -768 to 768
- biases_moment: float32 [6, 1024], P(None, 'dp'), may hold values from -768 to 768
- upbias_moment: float32 [4096], P('dp'), may hold values from -768 to 768
Outputs:
- block_out: bfloat16 [16384, 1024], P(('dp', 'seq'))
- tokens_grad: float32 [16384, 1024], P(('dp', 'seq'))
- qkv_grad: float32 [1024, 3072], P(None, 'dp')
- proj_grad: float32 [1024, 1024], P(None, 'dp')
- up_grad: float32 [1024, 4096], P(None, 'dp')
- down_grad: float32 [4096, 1024], P('dp')
- gains_grad: float32 [2, 1024], P(None, 'dp')
- biases_grad: float32 [6, 1024], P(None, 'dp')
- upbias_grad: float32 [4096], P('dp')
- qkv_state: float32 [1024, 3072], P(None, 'dp')
- proj_state: float32 [1024, 1024], P(None, 'dp')
- up_state: float32 [1024, 4096], P(None, 'dp')
- down_state: float32 [4096, 1024], P('dp')
- gains_state: float32 [2, 1024], P(None, 'dp')
- biases_state: float32 [6, 1024], P(None, 'dp')
- upbias_state: float32 [4096], P('dp')
- qkv_new: float32 [1024, 3072], P(None, 'dp')
- proj_new: float32 [1024, 1024], P(None, 'dp')
- up_new: float32 [1024, 4096], P(None, 'dp')
- down_new: float32 [4096, 1024], P('dp')
- gains_new: float32 [2, 1024], P(None, 'dp')
- biases_new: float32 [6, 1024], P(None, 'dp')
- upbias_new: float32 [4096], P('dp')
The draws below stay inside these ranges and needn't reach their ends.
Inputs may be any that keep to these rules, and one draw needn't show every extreme that they name: `head_slopes`: one positive slope a head.
All inputs are finite; a program needn't handle non-finite values.
Results may differ from the reference program's by a relative error of at most 0.025.
Values may be sent and summed in bfloat16 or wider, within the bound.
A program may use at most 256 MiB of HBM per device.

```python
import math
from functools import partial
import jax
import jax.numpy as jnp
from jax import lax

D = 1024
H = 16
FF = 4096
TOK_DEV = 512
NS_ITERS = 5
HD = 64
SEQ_LEN = 2048
TOKENS = 16384
N_DP = 8


def draw_head_slopes(key, part):
    bottom = 0.25 / SEQ_LEN
    spread_key = jax.random.fold_in(key, 29)
    levels = jax.random.uniform(spread_key, (H,), jnp.float32, jnp.log(bottom), jnp.log(0.5))
    slopes = jnp.exp(levels)
    return jnp.clip(slopes, bottom, 0.5).astype(jnp.float32)


def moment_matrix(key, row_count, col_count):
    entry_key = jax.random.fold_in(key, 41)
    row_key = jax.random.fold_in(key, 43)
    col_key = jax.random.fold_in(key, 47)
    base = 0.3 * TOKENS ** 0.5
    half_range = 0.5 * math.log(10.0)
    entries = jax.random.truncated_normal(entry_key, -4.0, 4.0, (row_count, col_count), jnp.float32)
    row_scale = jnp.exp(jax.random.uniform(row_key, (row_count, 1), jnp.float32, -half_range, half_range))
    col_scale = jnp.exp(jax.random.uniform(col_key, (1, col_count), jnp.float32, -half_range, half_range))
    return (entries * row_scale * col_scale * base).astype(jnp.float32)


def draw_qkv_moment(key, part):
    return moment_matrix(key, D, 3 * D)


def draw_proj_moment(key, part):
    return moment_matrix(key, D, D)


def draw_up_moment(key, part):
    return moment_matrix(key, D, FF)


def draw_down_moment(key, part):
    return moment_matrix(key, FF, D)


def block_levels(own_key, shape, shards, smallest, top_value):
    factor_of, own = 1.0, jax.random.fold_in(own_key, 6)
    for dim, shards_of in shards:
        draws = jnp.exp(jax.random.uniform(jax.random.fold_in(own, dim), (shards_of,), jnp.float32, smallest / len(shards), top_value / len(shards)))
        factor_of = factor_of * jnp.repeat(draws, shape[dim] // shards_of).reshape([-1 if axis == dim else 1 for axis in range(len(shape))])
    return factor_of


def gaussian(own_key, extent, scale, bound, pieces=(), held_as=jnp.bfloat16):
    values = scale * jax.random.normal(own_key, extent, jnp.float32)
    if pieces:
        values = values * block_levels(own_key, extent, pieces, -0.22, 0.18)
    return jnp.clip(values, -bound, bound).astype(held_as)


def setup_inputs(seed: int = 0) -> dict:
    key_of = jax.random.split(jax.random.key(seed), 18)
    return {
        "tokens": gaussian(key_of[0], (TOKENS, D), 1.0, 6.0, ((0, 32),)),
        "cotangent": gaussian(key_of[1], (TOKENS, D), 1.0, 6.0, ((0, 32),)),
        "qkv_weight": gaussian(key_of[2], (D, 3 * D), D ** -0.5, 0.1875),
        "proj_weight": gaussian(key_of[3], (D, D), (D // 16) ** -0.5, 0.75),
        "up_weight": gaussian(key_of[4], (D, FF), D ** -0.5, 0.1875),
        "down_weight": gaussian(key_of[5], (FF, D), FF ** -0.5, 0.09375),
        "norm_gains": jnp.clip(1.0 + 0.1 * jax.random.normal(key_of[6], (2, D), jnp.float32), 0.5, 1.5),
        "biases": gaussian(key_of[7], (6, D), 0.3, 1.5, (), jnp.float32),
        "up_bias": gaussian(key_of[8], (FF,), 0.3, 1.5, (), jnp.float32),
        "head_slopes": draw_head_slopes(jax.random.fold_in(key_of[17], 71), 0),
        "qkv_moment": draw_qkv_moment(jax.random.fold_in(key_of[17], 71), 0),
        "proj_moment": draw_proj_moment(jax.random.fold_in(key_of[17], 71), 0),
        "up_moment": draw_up_moment(jax.random.fold_in(key_of[17], 71), 0),
        "down_moment": draw_down_moment(jax.random.fold_in(key_of[17], 71), 0),
        "gains_moment": gaussian(key_of[14], (2, D), (TOKENS ** 0.5), 768.0, ((1, 8),), jnp.float32),
        "biases_moment": gaussian(key_of[15], (6, D), (TOKENS ** 0.5), 768.0, ((1, 8),), jnp.float32),
        "upbias_moment": gaussian(key_of[16], (FF,), (TOKENS ** 0.5), 768.0, ((0, 8),), jnp.float32),
    }


MOMENTUM = 0.9
RATE_MATRIX = 0.2
RATE_VECTOR = 0.0015
NORM_EPS = 1e-05
ORTHO_EPS = 1e-07
COEF_A = 2.0
COEF_B = -1.0
GELU_C = 0.7978845608028654
MASKED = -1e+30

@jax.custom_vjp
def low(v):
    return lax.optimization_barrier(v.astype(jnp.bfloat16)).astype(jnp.float32)

@jax.custom_vjp
def low_back(v):
    return v

def low_keep(v):
    return (low(v), None)

def low_pass(kept, grad):
    return (grad,)

def back_keep(v):
    return (v, None)

def back_low(kept, grad):
    return (low(grad),)
low.defvjp(low_keep, low_pass)
low_back.defvjp(back_keep, back_low)

def highest(left, right):
    return jnp.dot(left, right, precision=lax.Precision.HIGHEST)

def layer_norm(values, gain_row, offset):
    center = values - lax.optimization_barrier(jnp.mean(values, axis=-1, keepdims=True))
    variance = lax.optimization_barrier(jnp.mean(center * center, axis=-1, keepdims=True))
    return center * lax.rsqrt(variance + NORM_EPS) * gain_row + offset

def gelu_tanh(values):
    return 0.5 * values * (1.0 + jnp.tanh(GELU_C * (values + 0.044715 * values * values * values)))

def attend_block(query_block, start, key_heads, value_heads, slopes):
    query_pos = start + jnp.arange(TOK_DEV, dtype=jnp.int32)
    key_pos = jnp.arange(SEQ_LEN, dtype=jnp.int32)
    distance = (query_pos[:, None] - key_pos[None, :]).astype(slopes.dtype)
    scores = jnp.einsum('qhd,khd->hqk', query_block, key_heads, precision=lax.Precision.HIGHEST) * (1.0 / math.sqrt(HD))
    scores = scores - slopes[:, None, None] * distance[None]
    scores = jnp.where((key_pos[None, :] <= query_pos[:, None])[None], scores, MASKED)
    scores = low_back(scores)
    peak_score = lax.optimization_barrier(jnp.max(scores, axis=-1, keepdims=True))
    raised = jnp.exp(scores - peak_score)
    chances = raised / lax.optimization_barrier(jnp.sum(raised, axis=-1, keepdims=True))
    return jnp.einsum('hqk,khd->qhd', low(chances), value_heads, precision=lax.Precision.HIGHEST)

def sequence_forward(sequence, params, slopes):
    qkv_matrix, proj_matrix, up_matrix, down_matrix, gains, offsets, up_offset = params
    normed_one = low(layer_norm(sequence, gains[0], offsets[0]))
    mixed = highest(normed_one, qkv_matrix)
    queries = low(low_back(mixed[:, :D] + offsets[1]))
    keys = low(low_back(mixed[:, D:2 * D]))
    values = low(low_back(mixed[:, 2 * D:] + offsets[2]))
    key_heads = keys.reshape(SEQ_LEN, H, HD)
    value_heads = values.reshape(SEQ_LEN, H, HD)
    blocks = queries.reshape(SEQ_LEN // TOK_DEV, TOK_DEV, H, HD)
    starts = jnp.arange(SEQ_LEN // TOK_DEV, dtype=jnp.int32) * TOK_DEV

    def run_block(items):
        return attend_block(items[0], items[1], key_heads, value_heads, slopes)
    attended = lax.map(jax.checkpoint(run_block), (blocks, starts))
    attended = low(low_back(attended.reshape(SEQ_LEN, D)))
    branch = low_back(highest(attended, proj_matrix) + offsets[3])
    middle = sequence + branch
    normed_two = low(layer_norm(middle, gains[1], offsets[4]))
    before = low_back(highest(normed_two, up_matrix) + up_offset)
    hidden = low(gelu_tanh(before))
    return middle + highest(hidden, down_matrix) + offsets[5]

def layer_forward(inputs, qkv_matrix, proj_matrix, up_matrix, down_matrix, gains, offsets, up_offset, slopes):
    params = (qkv_matrix, proj_matrix, up_matrix, down_matrix, gains, offsets, up_offset)
    sequences = inputs.reshape(N_DP, SEQ_LEN, D)

    def run_sequence(sequence):
        return sequence_forward(sequence, params, slopes)
    outputs = lax.map(jax.checkpoint(run_sequence), sequences)
    return outputs.reshape(TOKENS, D)

def orthogonal(matrix):
    rounded = low(matrix)
    gram = highest(rounded, rounded.T)
    factor = 1.0 / (jnp.sqrt(jnp.trace(gram)) + ORTHO_EPS)
    square = gram * factor * factor
    iterate = low(rounded * factor)
    for iteration in range(NS_ITERS):
        if iteration > 0:
            square = highest(iterate, iterate.T)
        square_low = low(square)
        iterate = low(COEF_A * iterate + COEF_B * highest(square_low, iterate))
    return iterate

def matrix_step(state):
    return -RATE_MATRIX * math.sqrt(max(state.shape[0], state.shape[1])) * orthogonal(state)

def reference(tokens, cotangent, qkv_weight, proj_weight, up_weight, down_weight, norm_gains, biases, up_bias, head_slopes, qkv_moment, proj_moment, up_moment, down_moment, gains_moment, biases_moment, upbias_moment):
    primal = (tokens.astype(jnp.float32), qkv_weight.astype(jnp.float32), proj_weight.astype(jnp.float32), up_weight.astype(jnp.float32), down_weight.astype(jnp.float32), norm_gains, biases, up_bias)
    result, pullback = jax.vjp(partial(layer_forward, slopes=head_slopes), *primal)
    grads = pullback(cotangent.astype(jnp.float32))
    tokens_grad, qkv_grad, proj_grad, up_grad, down_grad, gains_grad, biases_grad, upbias_grad = grads
    qkv_state = MOMENTUM * qkv_moment + qkv_grad
    proj_state = MOMENTUM * proj_moment + proj_grad
    up_state = MOMENTUM * up_moment + up_grad
    down_state = MOMENTUM * down_moment + down_grad
    gains_state = MOMENTUM * gains_moment + gains_grad
    biases_state = MOMENTUM * biases_moment + biases_grad
    upbias_state = MOMENTUM * upbias_moment + upbias_grad
    qkv_new = primal[1] + matrix_step(qkv_state)
    proj_new = primal[2] + matrix_step(proj_state)
    up_new = primal[3] + matrix_step(up_state)
    down_new = primal[4] + matrix_step(down_state.T).T
    return (result.astype(jnp.bfloat16), tokens_grad, qkv_grad, proj_grad, up_grad, down_grad, gains_grad, biases_grad, upbias_grad, qkv_state, proj_state, up_state, down_state, gains_state, biases_state, upbias_state, qkv_new, proj_new, up_new, down_new, norm_gains - RATE_VECTOR * gains_state, biases - RATE_VECTOR * biases_state, up_bias - RATE_VECTOR * upbias_state)
```

```python
import functools
import math

import jax
import jax.numpy as jnp
from jax import lax
from jax.experimental import pallas as pl
from jax.experimental.pallas import tpu as pltpu
from jax.sharding import PartitionSpec as P

NS_ITERS = 5

MOMENTUM = 0.9
RATE_MATRIX = 0.2
RATE_VECTOR = 0.0015
NORM_EPS = 1e-05
ORTHO_EPS = 1e-07
GELU_C = 0.7978845608028654
MASKED = -1e30
HEAD = 64
BLOCK = 256
LOW = jnp.bfloat16
F32 = jnp.float32

NT = (((1,), (1,)), ((), ()))
NN = (((1,), (0,)), ((), ()))
TN = (((0,), (0,)), ((), ()))


def mm(left, right, dims=NN):
    return lax.dot_general(left, right, dims, preferred_element_type=F32)


def stack_heads(block, groups, scale=None):
    lane = lax.broadcasted_iota(jnp.int32, block.shape, 1)
    if scale is not None:
        block = block * scale
    zero = jnp.zeros_like(block)
    return [
        jnp.where((lane >= h * HEAD) & (lane < (h + 1) * HEAD), block, zero)
        for h in range(groups)
    ]


def bias_tiles(slope_row, block, plain_ref, edge_ref, groups):
    shape = plain_ref.shape
    row = lax.broadcasted_iota(jnp.int32, shape, 0)
    col = lax.broadcasted_iota(jnp.int32, (shape[0], block), 1)
    tile = row.astype(F32) * slope_row
    plain_ref[...] = tile
    for h in range(groups):
        part = slice(h * block, (h + 1) * block)
        edge_ref[:, part] = jnp.where(row[:, part] <= col, tile[:, part], MASKED)


def forward_kernel(
    groups, block, slope_ref, q_ref, k_ref, v_ref, out_ref, wide_ref, log_ref, plain, edge, vt, qs, acc
):
    i = pl.program_id(0)
    slope = slope_ref[...]

    @pl.when(i == 0)
    def _():
        bias_tiles(slope, block, plain, edge, groups)
        vt[...] = v_ref[0].T

    for h, part in enumerate(stack_heads(q_ref[0], groups, LOW(1.0 / math.sqrt(HEAD)))):
        qs[h * block : (h + 1) * block, :] = part
    acc[...] = jnp.zeros_like(acc)
    wide = groups * block

    def visit(j, carry, tile_ref):
        peak, total = carry
        start = pl.multiple_of(j * block, block)
        x = mm(k_ref[0, pl.ds(start, block), :], qs[...], NT) + tile_ref[...]
        shift = slope * (j * block).astype(F32)
        new = jnp.maximum(peak, jnp.max(x, axis=0, keepdims=True) + shift)
        p = jnp.exp(x + (shift - new))
        alpha = jnp.exp(peak - new)
        total = total * alpha + jnp.sum(p, axis=0, keepdims=True)
        low = p.astype(LOW)
        for h in range(groups):
            part = slice(h * block, (h + 1) * block)
            rows = slice(h * HEAD, (h + 1) * HEAD)
            acc[rows, :] = acc[rows, :] * alpha[:, part] + mm(
                vt[rows, pl.ds(start, block)], low[:, part]
            )
        return new, total

    start = (jnp.full((1, wide), MASKED, F32), jnp.zeros((1, wide), F32))
    carry = lax.fori_loop(0, i, lambda j, c: visit(j, c, plain), start)
    peak, total = visit(i, carry, edge)
    log_ref[0] = peak + jnp.log(total)
    inverse = 1.0 / total
    for h in range(groups):
        rows = slice(h * HEAD, (h + 1) * HEAD)
        acc[rows, :] = acc[rows, :] * inverse[:, h * block : (h + 1) * block]
    out = acc[...].T
    wide_ref[...] = out
    out_ref[...] = out.astype(LOW)


def attend_forward(qkv, slope_row, block):
    length, width = qkv.shape[1:]
    groups = width // HEAD
    count = length // block
    wide = groups * block
    part = pl.BlockSpec((block, width), lambda i: (i, 0))
    return pl.pallas_call(
        functools.partial(forward_kernel, groups, block),
        grid=(count,),
        in_specs=[
            pl.BlockSpec((1, wide), lambda i: (0, 0)),
            pl.BlockSpec((1, block, width), lambda i: (0, i, 0)),
            pl.BlockSpec((1, length, width), lambda i: (1, 0, 0)),
            pl.BlockSpec((1, length, width), lambda i: (2, 0, 0)),
        ],
        out_specs=[part, part, pl.BlockSpec((1, 1, wide), lambda i: (i, 0, 0))],
        out_shape=[
            jax.ShapeDtypeStruct((length, width), LOW),
            jax.ShapeDtypeStruct((length, width), F32),
            jax.ShapeDtypeStruct((count, 1, wide), F32),
        ],
        scratch_shapes=[
            pltpu.VMEM((block, wide), F32),
            pltpu.VMEM((block, wide), F32),
            pltpu.VMEM((width, length), LOW),
            pltpu.VMEM((wide, width), LOW),
            pltpu.VMEM((width, block), F32),
        ],
        compiler_params=pltpu.CompilerParams(vmem_limit_bytes=32 << 20),
        cost_estimate=pl.CostEstimate(
            flops=16 * length * length * width,
            bytes_accessed=12 * length * width,
            transcendentals=length * length * groups,
        ),
        name="attend_forward",
    )(slope_row, qkv, qkv, qkv)


def backward_kernel(
    groups, block, slope_ref, q_ref, k_ref, v_ref, grad_ref, wide_ref, log_ref,
    out_ref, plain, edge, qs, grads, delta, dq, dk, dv, ks
):
    j = pl.program_id(0)
    count = pl.num_programs(0)
    slope = slope_ref[...]
    scale = 1.0 / math.sqrt(HEAD)

    @pl.when(j == 0)
    def _():
        bias_tiles(slope, block, plain, edge, groups)
        dq[...] = jnp.zeros_like(dq)

        def prepare(i, unused):
            rows = pl.ds(pl.multiple_of(i * block, block), block)
            grad = grad_ref[rows, :]
            for h, part in enumerate(stack_heads(q_ref[0, rows, :], groups, LOW(scale))):
                qs[i, h * block : (h + 1) * block, :] = part
            for h, part in enumerate(stack_heads(grad, groups)):
                grads[i, h * block : (h + 1) * block, :] = part
            both = (wide_ref[rows, :] * grad.astype(F32)).T
            for h in range(groups):
                delta[i, :, h * block : (h + 1) * block] = jnp.sum(
                    both[h * HEAD : (h + 1) * HEAD, :], axis=0, keepdims=True
                )
            return unused

        lax.fori_loop(0, count, prepare, 0)

    keys = k_ref[0]
    values = v_ref[0]
    for h, part in enumerate(stack_heads(keys, groups)):
        ks[h] = part
    dk[...] = jnp.zeros_like(dk)
    dv[...] = jnp.zeros_like(dv)
    shift = slope * (j * block).astype(F32)

    def visit(i, tile_ref):
        heads_q = qs[i]
        heads_grad = grads[i]
        p = jnp.exp(mm(keys, heads_q, NT) + tile_ref[...] + (shift - log_ref[i]))
        ds = p * (mm(values, heads_grad, NT) - delta[i])
        p_low = p.astype(LOW)
        ds_low = ds.astype(LOW)
        dv[...] += mm(p_low, heads_grad)
        dk[...] += mm(ds_low, heads_q)
        total = mm(ds_low[:, :block], ks[0], TN)
        for h in range(1, groups):
            total += mm(ds_low[:, h * block : (h + 1) * block], ks[h], TN)
        dq[pl.ds(pl.multiple_of(i * block, block), block), :] += total

    visit(j, edge)

    def step(i, unused):
        visit(i, plain)
        return unused

    lax.fori_loop(j + 1, count, step, 0)
    out_ref[0] = (dq[pl.ds(pl.multiple_of(j * block, block), block), :] * scale).astype(LOW)
    out_ref[1] = dk[...].astype(LOW)
    out_ref[2] = dv[...].astype(LOW)


def attend_backward(qkv, grad, attended, log_totals, slope_row, block):
    length, width = qkv.shape[1:]
    groups = width // HEAD
    count = length // block
    wide = groups * block
    whole = pl.BlockSpec((length, width), lambda i: (0, 0))
    return pl.pallas_call(
        functools.partial(backward_kernel, groups, block),
        grid=(count,),
        in_specs=[
            pl.BlockSpec((1, wide), lambda i: (0, 0)),
            pl.BlockSpec((1, length, width), lambda i: (0, 0, 0)),
            pl.BlockSpec((1, block, width), lambda i: (1, i, 0)),
            pl.BlockSpec((1, block, width), lambda i: (2, i, 0)),
            whole,
            whole,
            pl.BlockSpec((count, 1, wide), lambda i: (0, 0, 0)),
        ],
        out_specs=pl.BlockSpec((3, block, width), lambda i: (0, i, 0)),
        out_shape=jax.ShapeDtypeStruct((3, length, width), LOW),
        scratch_shapes=[
            pltpu.VMEM((block, wide), F32),
            pltpu.VMEM((block, wide), F32),
            pltpu.VMEM((count, wide, width), LOW),
            pltpu.VMEM((count, wide, width), LOW),
            pltpu.VMEM((count, 1, wide), F32),
            pltpu.VMEM((length, width), F32),
            pltpu.VMEM((block, width), F32),
            pltpu.VMEM((block, width), F32),
            pltpu.VMEM((groups, block, width), LOW),
        ],
        compiler_params=pltpu.CompilerParams(vmem_limit_bytes=40 << 20),
        cost_estimate=pl.CostEstimate(
            flops=40 * length * length * width,
            bytes_accessed=18 * length * width,
            transcendentals=length * length * groups,
        ),
        name="attend_backward",
    )(slope_row, qkv, qkv, qkv, grad, attended, log_totals)


def ortho_kernel(tile, gram_ref, block_ref, out_ref, square, square_low, cross, cross_low, state):
    size = gram_ref.shape[0]
    steps = size // tile
    trace = jnp.zeros((1, 1), F32)
    for r in range(steps):
        rows = slice(r * tile, (r + 1) * tile)
        piece = gram_ref[rows, rows].astype(F32)
        same = lax.broadcasted_iota(jnp.int32, piece.shape, 0) == lax.broadcasted_iota(
            jnp.int32, piece.shape, 1
        )
        picked = jnp.where(same, piece, 0.0)
        trace += jnp.sum(jnp.sum(picked, axis=1, keepdims=True), axis=0, keepdims=True)
    factor = 1.0 / (jnp.sqrt(trace) + ORTHO_EPS)

    def load(r, unused):
        rows = pl.ds(pl.multiple_of(r * tile, tile), tile)
        first = gram_ref[rows, :].astype(F32) * factor * factor
        square[rows, :] = first
        square_low[rows, :] = first.astype(LOW)
        state[rows, :] = block_ref[rows, :].astype(F32) * factor
        out_ref[rows, :] = state[rows, :].astype(LOW)
        return unused

    lax.fori_loop(0, steps, load, 0)

    def advance():
        for r in range(steps):
            rows = slice(r * tile, (r + 1) * tile)
            state[rows, :] = 2.0 * state[rows, :] - mm(square_low[rows, :], out_ref[...])

    def settle():
        out_ref[...] = state[...].astype(LOW)

    def iterate(t, unused):
        advance()
        for r in range(steps):
            rows = slice(r * tile, (r + 1) * tile)
            value = 2.0 * square[rows, :] - mm(square_low[rows, :], square_low[...])
            cross[rows, :] = value
            cross_low[rows, :] = value.astype(LOW)
        settle()
        for r in range(steps):
            rows = slice(r * tile, (r + 1) * tile)
            square[rows, :] = 2.0 * cross[rows, :] - mm(cross_low[rows, :], square_low[...])
        square_low[...] = square[...].astype(LOW)
        return unused

    lax.fori_loop(0, NS_ITERS - 1, iterate, 0)
    advance()
    settle()


def orthogonal(gram, block):
    size, width = block.shape
    tile = min(256, size)
    return pl.pallas_call(
        functools.partial(ortho_kernel, tile),
        out_shape=jax.ShapeDtypeStruct((size, width), LOW),
        in_specs=[pl.BlockSpec(memory_space=pltpu.VMEM)] * 2,
        out_specs=pl.BlockSpec(memory_space=pltpu.VMEM),
        scratch_shapes=[
            pltpu.VMEM((size, size), F32),
            pltpu.VMEM((size, size), LOW),
            pltpu.VMEM((size, size), F32),
            pltpu.VMEM((size, size), LOW),
            pltpu.VMEM((size, width), F32),
        ],
        compiler_params=pltpu.CompilerParams(vmem_limit_bytes=40 << 20),
        cost_estimate=pl.CostEstimate(
            flops=16 * size**3 + 10 * size * size * width, bytes_accessed=4 * size * size, transcendentals=0
        ),
        name="orthogonal",
    )(gram, block)


def swap(value, axis, bit):
    return lax.ppermute(value, axis, [(i, i ^ bit) for i in range(lax.axis_size(axis))])


def pick(buffer, axis, count, stride, choice):
    size = buffer.shape[axis] // count
    run = stride * size
    parts = [
        lax.dynamic_slice_in_dim(buffer, 2 * i * run + choice * run, run, axis)
        for i in range(count // (2 * stride))
    ]
    return parts[0] if len(parts) == 1 else jnp.concatenate(parts, axis)


def reduce_blocks(buffer, axis, held):
    me = lax.axis_index("dp")
    count = 1 << len(held)

    def ladder(piece, order):
        left = list(held)
        blocks = count
        for bit in order:
            stride = 1 << (len(left) - 1 - left.index(bit))
            mine = (me // bit) % 2
            arrived = swap(pick(piece, axis, blocks, stride, 1 - mine), "dp", bit)
            kept = pick(piece, axis, blocks, stride, mine)
            piece = (kept.astype(F32) + arrived.astype(F32)).astype(LOW)
            left.remove(bit)
            blocks //= 2
        return piece

    if not held:
        return buffer
    other = 1 - axis
    half = buffer.shape[other] // 2
    ascending = sorted(held)
    orders = (ascending, ascending[1:] + ascending[:1])
    pieces = [
        ladder(lax.slice_in_dim(buffer, k * half, (k + 1) * half, axis=other), orders[k])
        for k in range(2)
    ]
    return jnp.concatenate(pieces, other)


def weight_gradient(left, right, axis):
    size = lax.axis_size("dp")
    me = lax.axis_index("dp")
    bits = [1 << b for b in range(size.bit_length() - 1)][::-1]
    mine = me % 2

    def product(choice):
        if axis == 1:
            return mm(left, pick(right, 1, size, 1, choice), TN)
        return mm(pick(left, 1, size, 1, choice), right, TN)

    arrived = swap(product(1 - mine).astype(LOW), "dp", 1)
    kept = (product(mine) + arrived.astype(F32)).astype(LOW)
    return reduce_blocks(kept, axis, bits[:-1])


def collect(value, owner, pieces):
    size = lax.axis_size("seq")
    hops = []
    left = [(i, i - 1) for i in range(size - 1, owner, -1)]
    right = [(i, i + 1) for i in range(owner)]
    while left or right:
        hops.append(left[:1] + right[:1])
        left, right = left[1:], right[1:]
        if len(hops[-1]) == 2 and hops[-1][0][1] == hops[-1][1][1]:
            hops[-1:] = [hops[-1][:1], hops[-1][1:]]
    rows = value.shape[0] // pieces
    parts = []
    for k in range(pieces):
        part = value[k * rows : (k + 1) * rows]
        for hop in hops:
            arrived = lax.ppermute(part, "seq", hop)
            part = (part.astype(F32) + arrived.astype(F32)).astype(LOW)
        parts.append(part)
    return parts[0] if pieces == 1 else jnp.concatenate(parts, 0)


def spread(value, owner, pieces):
    size = lax.axis_size("seq")
    rows = value.shape[0] // pieces
    mine = lax.axis_index("seq") == owner
    parts = []
    for k in range(pieces):
        part = value[k * rows : (k + 1) * rows]
        total = jnp.where(mine, part, jnp.zeros_like(part))
        for way, last in ((1, size - 1), (-1, 0)):
            moving = part
            for i in range(owner, last, way):
                moving = lax.ppermute(moving, "seq", [(i, i + way)])
                total = total + moving
        parts.append(total)
    return parts[0] if pieces == 1 else jnp.concatenate(parts, 0)


def gram_total(gram):
    me = lax.axis_index("dp")
    size = lax.axis_size("dp")
    bits = [1 << b for b in range(size.bit_length() - 1)]

    def ladder(piece, order):
        sizes = []
        for bit in order:
            half = piece.shape[0] // 2
            mine = (me // bit) % 2
            arrived = swap(lax.dynamic_slice_in_dim(piece, (1 - mine) * half, half, 0), "dp", bit)
            kept = lax.dynamic_slice_in_dim(piece, mine * half, half, 0)
            piece = (kept.astype(F32) + arrived.astype(F32)).astype(LOW)
            sizes.append(half)
        for bit, half in zip(reversed(order), reversed(sizes)):
            mine = (me // bit) % 2
            arrived = swap(piece, "dp", bit)
            first = jnp.where(mine == 0, piece, arrived)
            second = jnp.where(mine == 0, arrived, piece)
            piece = jnp.concatenate([first, second], 0)
        return piece

    half = gram.shape[1] // 2
    low = gram.astype(LOW)
    return jnp.concatenate(
        [
            ladder(low[:, :half], bits),
            ladder(low[:, half:], bits[:1] + bits[2:] + bits[1:2]),
        ],
        1,
    )


def sum_everywhere(value):
    for axis in ("dp", "seq"):
        bit = 1
        while bit < lax.axis_size(axis):
            value = value + swap(value, axis, bit)
            bit *= 2
    return value


def exchange(source, take, place, shape):
    size = lax.axis_size("seq")
    here = lax.axis_index("seq")
    result = jnp.zeros(shape, LOW)
    for shift in range(size):
        piece = take(source, (here + shift) % size)
        if shift:
            piece = lax.ppermute(piece, "seq", [(i, (i + shift) % size) for i in range(size)])
        result = lax.dynamic_update_slice(result, piece, place((here - shift) % size))
    return result


def norm_forward(values, gain_row, offset):
    center = values - jnp.mean(values, axis=-1, keepdims=True)
    inv_scale = lax.rsqrt(jnp.mean(center * center, axis=-1, keepdims=True) + NORM_EPS)
    unit_values = center * inv_scale
    return (unit_values * gain_row + offset, unit_values, inv_scale)


def norm_backward(upstream, unit_values, inv_scale, gain_row):
    scaled = upstream * gain_row
    inner_sum = jnp.mean(scaled * unit_values, axis=-1, keepdims=True)
    input_grad = inv_scale * (
        scaled - jnp.mean(scaled, axis=-1, keepdims=True) - unit_values * inner_sum
    )
    return (input_grad, jnp.sum(upstream * unit_values, axis=0), jnp.sum(upstream, axis=0))


def gelu_both(values):
    square = values * values
    tangent = jnp.tanh(GELU_C * (values + 0.044715 * square * values))
    slope = 0.5 * (1.0 + tangent) + 0.5 * values * (1.0 - tangent * tangent) * GELU_C * (
        1.0 + 3.0 * 0.044715 * square
    )
    return 0.5 * values * (1.0 + tangent), slope


def on_device(
    tokens,
    cotangent,
    qkv_weight,
    proj_weight,
    up_weight,
    down_weight,
    norm_gains,
    biases,
    up_bias,
    head_slopes,
    qkv_moment,
    proj_moment,
    up_moment,
    down_moment,
    gains_moment,
    biases_moment,
    upbias_moment,
):
    rows, width = tokens.shape
    ways = lax.axis_size("seq")
    here = lax.axis_index("seq")
    me = lax.axis_index("dp")
    length = rows * ways
    own_width = width // ways
    chunks = 2
    chunk = own_width // chunks
    chunk_heads = chunk // HEAD
    own_slopes = lax.dynamic_slice_in_dim(
        head_slopes, here * (own_width // HEAD), own_width // HEAD, 0
    )
    slope_rows = [
        jnp.repeat(own_slopes[c * chunk_heads : (c + 1) * chunk_heads], BLOCK)[None]
        for c in range(chunks)
    ]

    inputs = tokens.astype(F32)
    normed_one, unit_one, scale_one = norm_forward(inputs, norm_gains[0], biases[0])
    normed_one = normed_one.astype(LOW)
    bias_row = jnp.concatenate([biases[1], jnp.zeros_like(biases[1]), biases[2]])
    mixed = (mm(normed_one, qkv_weight) + bias_row).astype(LOW)

    def take_mixed(c):
        def take(source, d):
            return jnp.stack(
                [
                    lax.dynamic_slice_in_dim(
                        source, part * width + d * own_width + c * chunk, chunk, 1
                    )
                    for part in range(3)
                ]
            )

        return take

    qkv = [
        exchange(mixed, take_mixed(c), lambda d: (0, d * rows, 0), (3, length, chunk))
        for c in range(chunks)
    ]
    attended = jnp.zeros((rows, width), LOW)
    kept = []
    for c in range(chunks):
        out, wide, log_totals = attend_forward(qkv[c], slope_rows[c], BLOCK)
        kept.append((wide, log_totals))
        for shift in range(ways):
            piece = lax.dynamic_slice_in_dim(out, ((here + shift) % ways) * rows, rows, 0)
            if shift:
                piece = lax.ppermute(piece, "seq", [(i, (i + shift) % ways) for i in range(ways)])
            attended = lax.dynamic_update_slice(
                attended, piece, (0, ((here - shift) % ways) * own_width + c * chunk)
            )

    middle = inputs + mm(attended, proj_weight) + biases[3]
    normed_two, unit_two, scale_two = norm_forward(middle, norm_gains[1], biases[4])
    normed_two = normed_two.astype(LOW)
    before = mm(normed_two, up_weight) + up_bias
    hidden, slope = gelu_both(before)
    hidden = hidden.astype(LOW)
    block_out = (middle + mm(hidden, down_weight) + biases[5]).astype(LOW)
    upstream = cotangent.astype(F32)
    hidden_grad = mm(cotangent, down_weight, NT)
    before_grad = (hidden_grad * slope).astype(LOW)
    normed_two_grad = mm(before_grad, up_weight, NT)
    middle_back, gain_two_grad, offset_two_grad = norm_backward(
        normed_two_grad, unit_two, scale_two, norm_gains[1]
    )
    middle_grad = upstream + middle_back
    branch_grad = middle_grad.astype(LOW)
    heads_grad = mm(branch_grad, proj_weight, NT).astype(LOW)

    mixed_grad = jnp.zeros((3, rows, width), LOW)
    for c in range(chunks):
        grad = exchange(
            heads_grad,
            lambda source, d: lax.dynamic_slice_in_dim(source, d * own_width + c * chunk, chunk, 1),
            lambda d: (d * rows, 0),
            (length, chunk),
        )
        back = attend_backward(qkv[c], grad, *kept[c], slope_rows[c], BLOCK)
        for shift in range(ways):
            piece = lax.dynamic_slice_in_dim(back, ((here + shift) % ways) * rows, rows, 1)
            if shift:
                piece = lax.ppermute(piece, "seq", [(i, (i + shift) % ways) for i in range(ways)])
            mixed_grad = lax.dynamic_update_slice(
                mixed_grad, piece, (0, 0, ((here - shift) % ways) * own_width + c * chunk)
            )
    mixed_flat = jnp.concatenate([mixed_grad[0], mixed_grad[1], mixed_grad[2]], 1)

    down_part = weight_gradient(hidden, cotangent, 0)
    up_part = weight_gradient(normed_two, before_grad, 1)
    proj_part = weight_gradient(attended, branch_grad, 1)
    qkv_part = weight_gradient(normed_one, mixed_flat, 1)

    up_owner, qkv_owner, proj_owner, down_owner = range(4)
    down_own = collect(down_part, down_owner, 2)
    up_own = collect(up_part, up_owner, 2)
    proj_own = collect(proj_part, proj_owner, 1)
    qkv_own = collect(qkv_part, qkv_owner, 1)

    normed_one_grad = mm(mixed_flat, qkv_weight, NT)
    input_back, gain_one_grad, offset_one_grad = norm_backward(
        normed_one_grad, unit_one, scale_one, norm_gains[0]
    )
    tokens_grad = middle_grad + input_back

    def columns(value):
        return jnp.sum(value.astype(F32), axis=0)

    vectors = jnp.stack(
        [
            gain_one_grad,
            gain_two_grad,
            offset_one_grad,
            columns(mixed_grad[0]),
            columns(mixed_grad[2]),
            columns(branch_grad),
            offset_two_grad,
            columns(upstream),
        ]
    )
    vectors = jnp.concatenate([vectors, columns(before_grad).reshape(-1, width)], 0)
    vectors = sum_everywhere(vectors)

    def own_columns(matrix, count):
        return lax.dynamic_slice_in_dim(matrix, me * count, count, 1).astype(F32)

    gains_sum = own_columns(vectors[:2], gains_moment.shape[1])
    biases_sum = own_columns(vectors[2:8], biases_moment.shape[1])
    upbias_count = upbias_moment.shape[0]
    upbias_sum = lax.dynamic_slice_in_dim(
        vectors[8:].reshape(-1), me * upbias_count, upbias_count, 0
    )

    def state_of(moment, grad):
        return MOMENTUM * moment + grad.astype(F32)

    oriented = [
        state_of(up_moment, up_own).astype(LOW),
        state_of(qkv_moment, qkv_own).astype(LOW),
        state_of(proj_moment, proj_own).astype(LOW),
        state_of(down_moment, down_own).astype(LOW).T,
    ]
    pad_width = max(member.shape[1] for member in oriented)
    stacked = jnp.stack(
        [jnp.pad(member, ((0, 0), (0, pad_width - member.shape[1]))) for member in oriented]
    )
    owned_block = lax.dynamic_index_in_dim(stacked, here, 0, keepdims=False)
    gram = gram_total(mm(owned_block, owned_block, NT))
    iterate = orthogonal(gram, owned_block)

    up_sum = spread(up_own, up_owner, 1).astype(F32)
    qkv_sum = spread(qkv_own, qkv_owner, 1).astype(F32)
    proj_sum = spread(proj_own, proj_owner, 1).astype(F32)
    down_sum = spread(down_own, down_owner, 1).astype(F32)
    qkv_state = state_of(qkv_moment, qkv_sum)
    proj_state = state_of(proj_moment, proj_sum)
    up_state = state_of(up_moment, up_sum)
    down_state = state_of(down_moment, down_sum)
    gains_state = state_of(gains_moment, gains_sum)
    biases_state = state_of(biases_moment, biases_sum)
    upbias_state = state_of(upbias_moment, upbias_sum)

    def rate_of(shape):
        return -RATE_MATRIX * math.sqrt(max(shape))

    def step_of(owner, count, shape, pieces):
        return rate_of(shape) * spread(iterate[:, :count], owner, pieces).astype(F32)

    qkv_new = own_columns(qkv_weight, qkv_state.shape[1]) + step_of(
        qkv_owner, qkv_state.shape[1], qkv_weight.shape, 1
    )
    proj_new = own_columns(proj_weight, proj_state.shape[1]) + step_of(
        proj_owner, proj_state.shape[1], proj_weight.shape, 1
    )
    up_new = own_columns(up_weight, up_state.shape[1]) + step_of(
        up_owner, up_state.shape[1], up_weight.shape, 4
    )
    down_count = down_state.shape[0]
    down_rows = lax.dynamic_slice_in_dim(down_weight, me * down_count, down_count, 0).astype(F32)
    down_new = down_rows + step_of(down_owner, down_count, down_weight.shape, 4).T
    gains_new = own_columns(norm_gains, gains_state.shape[1]) - RATE_VECTOR * gains_state
    biases_new = own_columns(biases, biases_state.shape[1]) - RATE_VECTOR * biases_state
    upbias_new = (
        lax.dynamic_slice_in_dim(up_bias, me * upbias_count, upbias_count, 0)
        - RATE_VECTOR * upbias_state
    )
    return (
        block_out,
        tokens_grad,
        qkv_sum,
        proj_sum,
        up_sum,
        down_sum,
        gains_sum,
        biases_sum,
        upbias_sum,
        qkv_state,
        proj_state,
        up_state,
        down_state,
        gains_state,
        biases_state,
        upbias_state,
        qkv_new,
        proj_new,
        up_new,
        down_new,
        gains_new,
        biases_new,
        upbias_new,
    )


def solution(mesh):
    rows, columns, copied = P(("dp", "seq"), None), P(None, "dp"), P()
    return jax.shard_map(
        on_device,
        mesh=mesh,
        in_specs=(
            (rows, rows)
            + (copied,) * 8
            + (columns, columns, columns, P("dp", None), columns, columns, P("dp"))
        ),
        out_specs=(
            (rows, rows)
            + (columns, columns, columns, P("dp", None), columns, columns, P("dp")) * 3
        ),
        check_vma=False,
    )
```

```python
import functools
import math

import jax
import jax.numpy as jnp
from jax import lax
from jax.experimental import pallas as pl
from jax.experimental.pallas import tpu as pltpu
from jax.sharding import PartitionSpec as P


NS_ITERS = 5


MOMENTUM = 0.9
RATE_MATRIX = 0.2
RATE_VECTOR = 0.0015
NORM_EPS = 1e-05
ORTHO_EPS = 1e-07
GELU_C = 0.7978845608028654
MASKED = -1e30
HEAD = 64
BLOCK = 256
LOW = jnp.bfloat16
F32 = jnp.float32

NT = (((1,), (1,)), ((), ()))
NN = (((1,), (0,)), ((), ()))
TN = (((0,), (0,)), ((), ()))


def mm(left, right, dims=NN):
    return lax.dot_general(left, right, dims, preferred_element_type=F32)


def stack_heads(block, groups, scale=None):
    lane = lax.broadcasted_iota(jnp.int32, block.shape, 1)
    if scale is not None:
        block = block * scale
    zero = jnp.zeros_like(block)
    return [
        jnp.where((lane >= h * HEAD) & (lane < (h + 1) * HEAD), block, zero)
        for h in range(groups)
    ]


def bias_tiles(slope_row, block, plain_ref, edge_ref, groups):
    shape = plain_ref.shape
    row = lax.broadcasted_iota(jnp.int32, shape, 0)
    col = lax.broadcasted_iota(jnp.int32, (shape[0], block), 1)
    tile = row.astype(F32) * slope_row
    plain_ref[...] = tile
    for h in range(groups):
        part = slice(h * block, (h + 1) * block)
        edge_ref[:, part] = jnp.where(row[:, part] <= col, tile[:, part], MASKED)


def forward_kernel(
    groups, block, slope_ref, q_ref, k_ref, v_ref, out_ref, wide_ref, log_ref, plain, edge, vt, qs, acc
):
    i = pl.program_id(0)
    slope = slope_ref[...]

    @pl.when(i == 0)
    def _():
        bias_tiles(slope, block, plain, edge, groups)
        vt[...] = v_ref[0].T

    for h, part in enumerate(stack_heads(q_ref[0], groups, LOW(1.0 / math.sqrt(HEAD)))):
        qs[h * block : (h + 1) * block, :] = part
    acc[...] = jnp.zeros_like(acc)
    wide = groups * block

    def visit(j, carry, tile_ref):
        peak, total = carry
        start = pl.multiple_of(j * block, block)
        x = mm(k_ref[0, pl.ds(start, block), :], qs[...], NT) + tile_ref[...]
        shift = slope * (j * block).astype(F32)
        new = jnp.maximum(peak, jnp.max(x, axis=0, keepdims=True) + shift)
        p = jnp.exp(x + (shift - new))
        alpha = jnp.exp(peak - new)
        total = total * alpha + jnp.sum(p, axis=0, keepdims=True)
        low = p.astype(LOW)
        for h in range(groups):
            part = slice(h * block, (h + 1) * block)
            rows = slice(h * HEAD, (h + 1) * HEAD)
            acc[rows, :] = acc[rows, :] * alpha[:, part] + mm(
                vt[rows, pl.ds(start, block)], low[:, part]
            )
        return new, total

    start = (jnp.full((1, wide), MASKED, F32), jnp.zeros((1, wide), F32))
    carry = lax.fori_loop(0, i, lambda j, c: visit(j, c, plain), start)
    peak, total = visit(i, carry, edge)
    log_ref[0] = peak + jnp.log(total)
    inverse = 1.0 / total
    for h in range(groups):
        rows = slice(h * HEAD, (h + 1) * HEAD)
        acc[rows, :] = acc[rows, :] * inverse[:, h * block : (h + 1) * block]
    out = acc[...].T
    wide_ref[...] = out
    out_ref[...] = out.astype(LOW)


def attend_forward(qkv, slope_row, block):
    length, width = qkv.shape[1:]
    groups = width // HEAD
    count = length // block
    wide = groups * block
    part = pl.BlockSpec((block, width), lambda i: (i, 0))
    return pl.pallas_call(
        functools.partial(forward_kernel, groups, block),
        grid=(count,),
        in_specs=[
            pl.BlockSpec((1, wide), lambda i: (0, 0)),
            pl.BlockSpec((1, block, width), lambda i: (0, i, 0)),
            pl.BlockSpec((1, length, width), lambda i: (1, 0, 0)),
            pl.BlockSpec((1, length, width), lambda i: (2, 0, 0)),
        ],
        out_specs=[part, part, pl.BlockSpec((1, 1, wide), lambda i: (i, 0, 0))],
        out_shape=[
            jax.ShapeDtypeStruct((length, width), LOW),
            jax.ShapeDtypeStruct((length, width), F32),
            jax.ShapeDtypeStruct((count, 1, wide), F32),
        ],
        scratch_shapes=[
            pltpu.VMEM((block, wide), F32),
            pltpu.VMEM((block, wide), F32),
            pltpu.VMEM((width, length), LOW),
            pltpu.VMEM((wide, width), LOW),
            pltpu.VMEM((width, block), F32),
        ],
        compiler_params=pltpu.CompilerParams(vmem_limit_bytes=32 << 20),
        cost_estimate=pl.CostEstimate(
            flops=16 * length * length * width,
            bytes_accessed=12 * length * width,
            transcendentals=length * length * groups,
        ),
        name="attend_forward",
    )(slope_row, qkv, qkv, qkv)


def backward_kernel(
    groups, block, slope_ref, q_ref, k_ref, v_ref, grad_ref, wide_ref, log_ref,
    out_ref, plain, edge, qs, grads, delta, dq, dk, dv, ks
):
    j = pl.program_id(0)
    count = pl.num_programs(0)
    slope = slope_ref[...]
    scale = 1.0 / math.sqrt(HEAD)

    @pl.when(j == 0)
    def _():
        bias_tiles(slope, block, plain, edge, groups)
        dq[...] = jnp.zeros_like(dq)

        def prepare(i, unused):
            rows = pl.ds(pl.multiple_of(i * block, block), block)
            grad = grad_ref[rows, :]
            for h, part in enumerate(stack_heads(q_ref[0, rows, :], groups, LOW(scale))):
                qs[i, h * block : (h + 1) * block, :] = part
            for h, part in enumerate(stack_heads(grad, groups)):
                grads[i, h * block : (h + 1) * block, :] = part
            both = (wide_ref[rows, :] * grad.astype(F32)).T
            for h in range(groups):
                delta[i, :, h * block : (h + 1) * block] = jnp.sum(
                    both[h * HEAD : (h + 1) * HEAD, :], axis=0, keepdims=True
                )
            return unused

        lax.fori_loop(0, count, prepare, 0)

    keys = k_ref[0]
    values = v_ref[0]
    for h, part in enumerate(stack_heads(keys, groups)):
        ks[h] = part
    dk[...] = jnp.zeros_like(dk)
    dv[...] = jnp.zeros_like(dv)
    shift = slope * (j * block).astype(F32)

    def visit(i, tile_ref):
        heads_q = qs[i]
        heads_grad = grads[i]
        p = jnp.exp(mm(keys, heads_q, NT) + tile_ref[...] + (shift - log_ref[i]))
        ds = p * (mm(values, heads_grad, NT) - delta[i])
        p_low = p.astype(LOW)
        ds_low = ds.astype(LOW)
        dv[...] += mm(p_low, heads_grad)
        dk[...] += mm(ds_low, heads_q)
        total = mm(ds_low[:, :block], ks[0], TN)
        for h in range(1, groups):
            total += mm(ds_low[:, h * block : (h + 1) * block], ks[h], TN)
        dq[pl.ds(pl.multiple_of(i * block, block), block), :] += total

    visit(j, edge)

    def step(i, unused):
        visit(i, plain)
        return unused

    lax.fori_loop(j + 1, count, step, 0)
    out_ref[0] = (dq[pl.ds(pl.multiple_of(j * block, block), block), :] * scale).astype(LOW)
    out_ref[1] = dk[...].astype(LOW)
    out_ref[2] = dv[...].astype(LOW)


def attend_backward(qkv, grad, attended, log_totals, slope_row, block):
    length, width = qkv.shape[1:]
    groups = width // HEAD
    count = length // block
    wide = groups * block
    whole = pl.BlockSpec((length, width), lambda i: (0, 0))
    return pl.pallas_call(
        functools.partial(backward_kernel, groups, block),
        grid=(count,),
        in_specs=[
            pl.BlockSpec((1, wide), lambda i: (0, 0)),
            pl.BlockSpec((1, length, width), lambda i: (0, 0, 0)),
            pl.BlockSpec((1, block, width), lambda i: (1, i, 0)),
            pl.BlockSpec((1, block, width), lambda i: (2, i, 0)),
            whole,
            whole,
            pl.BlockSpec((count, 1, wide), lambda i: (0, 0, 0)),
        ],
        out_specs=pl.BlockSpec((3, block, width), lambda i: (0, i, 0)),
        out_shape=jax.ShapeDtypeStruct((3, length, width), LOW),
        scratch_shapes=[
            pltpu.VMEM((block, wide), F32),
            pltpu.VMEM((block, wide), F32),
            pltpu.VMEM((count, wide, width), LOW),
            pltpu.VMEM((count, wide, width), LOW),
            pltpu.VMEM((count, 1, wide), F32),
            pltpu.VMEM((length, width), F32),
            pltpu.VMEM((block, width), F32),
            pltpu.VMEM((block, width), F32),
            pltpu.VMEM((groups, block, width), LOW),
        ],
        compiler_params=pltpu.CompilerParams(vmem_limit_bytes=40 << 20),
        cost_estimate=pl.CostEstimate(
            flops=40 * length * length * width,
            bytes_accessed=18 * length * width,
            transcendentals=length * length * groups,
        ),
        name="attend_backward",
    )(slope_row, qkv, qkv, qkv, grad, attended, log_totals)


def ortho_kernel(tile, gram_ref, block_ref, out_ref, square, square_low, cross, cross_low, state):
    size = gram_ref.shape[0]
    steps = size // tile
    trace = jnp.zeros((1, 1), F32)
    for r in range(steps):
        rows = slice(r * tile, (r + 1) * tile)
        piece = gram_ref[rows, rows].astype(F32)
        same = lax.broadcasted_iota(jnp.int32, piece.shape, 0) == lax.broadcasted_iota(
            jnp.int32, piece.shape, 1
        )
        picked = jnp.where(same, piece, 0.0)
        trace += jnp.sum(jnp.sum(picked, axis=1, keepdims=True), axis=0, keepdims=True)
    factor = 1.0 / (jnp.sqrt(trace) + ORTHO_EPS)

    def load(r, unused):
        rows = pl.ds(pl.multiple_of(r * tile, tile), tile)
        first = gram_ref[rows, :].astype(F32) * factor * factor
        square[rows, :] = first
        square_low[rows, :] = first.astype(LOW)
        state[rows, :] = block_ref[rows, :].astype(F32) * factor
        out_ref[rows, :] = state[rows, :].astype(LOW)
        return unused

    lax.fori_loop(0, steps, load, 0)

    def advance():
        for r in range(steps):
            rows = slice(r * tile, (r + 1) * tile)
            state[rows, :] = 2.0 * state[rows, :] - mm(square_low[rows, :], out_ref[...])

    def settle():
        out_ref[...] = state[...].astype(LOW)

    def iterate(t, unused):
        advance()
        for r in range(steps):
            rows = slice(r * tile, (r + 1) * tile)
            value = 2.0 * square[rows, :] - mm(square_low[rows, :], square_low[...])
            cross[rows, :] = value
            cross_low[rows, :] = value.astype(LOW)
        settle()
        for r in range(steps):
            rows = slice(r * tile, (r + 1) * tile)
            square[rows, :] = 2.0 * cross[rows, :] - mm(cross_low[rows, :], square_low[...])
        square_low[...] = square[...].astype(LOW)
        return unused

    lax.fori_loop(0, NS_ITERS - 1, iterate, 0)
    advance()
    settle()


def orthogonal(gram, block):
    size, width = block.shape
    tile = min(256, size)
    return pl.pallas_call(
        functools.partial(ortho_kernel, tile),
        out_shape=jax.ShapeDtypeStruct((size, width), LOW),
        in_specs=[pl.BlockSpec(memory_space=pltpu.VMEM)] * 2,
        out_specs=pl.BlockSpec(memory_space=pltpu.VMEM),
        scratch_shapes=[
            pltpu.VMEM((size, size), F32),
            pltpu.VMEM((size, size), LOW),
            pltpu.VMEM((size, size), F32),
            pltpu.VMEM((size, size), LOW),
            pltpu.VMEM((size, width), F32),
        ],
        compiler_params=pltpu.CompilerParams(vmem_limit_bytes=40 << 20),
        cost_estimate=pl.CostEstimate(
            flops=16 * size**3 + 10 * size * size * width, bytes_accessed=4 * size * size, transcendentals=0
        ),
        name="orthogonal",
    )(gram, block)


def swap(value, axis, bit):
    return lax.ppermute(value, axis, [(i, i ^ bit) for i in range(lax.axis_size(axis))])


def pick(buffer, axis, count, stride, choice):
    size = buffer.shape[axis] // count
    run = stride * size
    parts = [
        lax.dynamic_slice_in_dim(buffer, 2 * i * run + choice * run, run, axis)
        for i in range(count // (2 * stride))
    ]
    return parts[0] if len(parts) == 1 else jnp.concatenate(parts, axis)


def reduce_blocks(buffer, axis, held):
    me = lax.axis_index("dp")
    count = 1 << len(held)

    def ladder(piece, order):
        left = list(held)
        blocks = count
        for bit in order:
            stride = 1 << (len(left) - 1 - left.index(bit))
            mine = (me // bit) % 2
            arrived = swap(pick(piece, axis, blocks, stride, 1 - mine), "dp", bit)
            kept = pick(piece, axis, blocks, stride, mine)
            piece = (kept.astype(F32) + arrived.astype(F32)).astype(LOW)
            left.remove(bit)
            blocks //= 2
        return piece

    if not held:
        return buffer
    other = 1 - axis
    half = buffer.shape[other] // 2
    ascending = sorted(held)
    orders = (ascending, ascending[1:] + ascending[:1])
    pieces = [
        ladder(lax.slice_in_dim(buffer, k * half, (k + 1) * half, axis=other), orders[k])
        for k in range(2)
    ]
    return jnp.concatenate(pieces, other)


def gradient_pair(left, right, axis):
    size = lax.axis_size("dp")
    mine = lax.axis_index("dp") % 2

    def product(choice):
        if axis == 1:
            return mm(left, pick(right, 1, size, 1, choice), TN)
        return mm(pick(left, 1, size, 1, choice), right, TN)

    arrived = swap(product(1 - mine).astype(LOW), "dp", 1)
    return (product(mine) + arrived.astype(F32)).astype(LOW)


def other_bits():
    return [1 << b for b in range(1, lax.axis_size("dp").bit_length() - 1)][::-1]


def collect(value, owner, pieces):
    size = lax.axis_size("seq")
    hops = []
    left = [(i, i - 1) for i in range(size - 1, owner, -1)]
    right = [(i, i + 1) for i in range(owner)]
    while left or right:
        hops.append(left[:1] + right[:1])
        left, right = left[1:], right[1:]
        if len(hops[-1]) == 2 and hops[-1][0][1] == hops[-1][1][1]:
            hops[-1:] = [hops[-1][:1], hops[-1][1:]]
    rows = value.shape[0] // pieces
    parts = []
    for k in range(pieces):
        part = value[k * rows : (k + 1) * rows]
        for hop in hops:
            arrived = lax.ppermute(part, "seq", hop)
            part = (part.astype(F32) + arrived.astype(F32)).astype(LOW)
        parts.append(part)
    return parts[0] if pieces == 1 else jnp.concatenate(parts, 0)


def share(own, widths, after):
    size = lax.axis_size("seq")
    here = lax.axis_index("seq")
    found = {0: own}
    for way in (1, -1):
        moving = own
        for distance in range(1, size):
            pairs = [
                (i, i + way) for i in range(size) if 0 <= i + way < size and 0 <= i + way - way * distance < size
            ]
            moving = lax.ppermute(moving, "seq", pairs)
            found[way * distance] = moving
    if after is not None:
        found, after = lax.optimization_barrier((found, after))
    result = []
    for m, width in enumerate(widths):
        value = own[:, :width]
        for d in range(size):
            if d != m:
                value = jnp.where(here == d, found[d - m][:, :width], value)
        result.append(value)
    return result


def gram_total(gram):
    me = lax.axis_index("dp")
    size = lax.axis_size("dp")
    bits = [1 << b for b in range(size.bit_length() - 1)]

    def ladder(piece, order):
        sizes = []
        for bit in order:
            half = piece.shape[0] // 2
            mine = (me // bit) % 2
            arrived = swap(lax.dynamic_slice_in_dim(piece, (1 - mine) * half, half, 0), "dp", bit)
            kept = lax.dynamic_slice_in_dim(piece, mine * half, half, 0)
            piece = (kept.astype(F32) + arrived.astype(F32)).astype(LOW)
            sizes.append(half)
        for bit, half in zip(reversed(order), reversed(sizes)):
            mine = (me // bit) % 2
            arrived = swap(piece, "dp", bit)
            first = jnp.where(mine == 0, piece, arrived)
            second = jnp.where(mine == 0, arrived, piece)
            piece = jnp.concatenate([first, second], 0)
        return piece

    half = gram.shape[1] // 2
    low = gram.astype(LOW)
    return jnp.concatenate(
        [
            ladder(low[:, :half], bits),
            ladder(low[:, half:], bits[:1] + bits[2:] + bits[1:2]),
        ],
        1,
    )


def sum_everywhere(value):
    for axis in ("dp", "seq"):
        bit = 1
        while bit < lax.axis_size(axis):
            value = value + swap(value, axis, bit)
            bit *= 2
    return value


def depart(source, take):
    size = lax.axis_size("seq")
    here = lax.axis_index("seq")
    pieces = []
    for shift in range(size):
        piece = take(source, (here + shift) % size)
        if shift:
            piece = lax.ppermute(piece, "seq", [(i, (i + shift) % size) for i in range(size)])
        pieces.append(piece)
    return pieces


def arrange(pieces, place, shape):
    size = lax.axis_size("seq")
    here = lax.axis_index("seq")
    result = jnp.zeros(shape, LOW)
    for shift, piece in enumerate(pieces):
        result = lax.dynamic_update_slice(result, piece, place((here - shift) % size))
    return result


MESH = pl.DeviceIdType.MESH
OWNERS = 4


def greet(axes_partners):
    barrier = pltpu.get_barrier_semaphore()
    count = 0
    for axis, partner, real in axes_partners:

        def tell(axis=axis, partner=partner):
            pl.semaphore_signal(barrier, inc=1, device_id={axis: partner}, device_id_type=MESH)

        if real is None:
            tell()
            count = count + 1
        else:
            pl.when(real)(tell)
            count = count + real.astype(jnp.int32)
    pl.semaphore_wait(barrier, count)


def plane():
    me = lax.axis_index("dp")
    core, x, y = lax.rem(me, 2), lax.rem(me // 2, 2), me // 4
    flip = lambda bit: 1 - bit
    return (
        (core, x, y),
        (
            4 * y + 2 * x + flip(core),
            4 * y + 2 * flip(x) + core,
            4 * flip(y) + 2 * x + core,
        ),
    )


def combine_kernel(
    ways, wide_q, wide_p, qkv_ref, proj_ref, up_ref, down_ref, out_ref,
    one, send_two, two, send_three, three, final, from_left, from_right, relay,
    s_one, r_one, s_two, r_two, s_three, r_three, s_left, r_left, s_right, r_right,
):
    (core, x, y), partners = plane()
    z = lax.axis_index("seq")
    size = up_ref.shape[0]
    half = size // 2
    chunks = 4
    step = size // chunks
    width = wide_q + wide_p
    greet(
        [("dp", p, None) for p in partners]
        + [("seq", jnp.maximum(z - 1, 0), z > 0), ("seq", jnp.minimum(z + 1, ways - 1), z < ways - 1)]
    )

    def remote(src, dst, send, recv, axis, target):
        return pltpu.make_async_remote_copy(
            src_ref=src, dst_ref=dst, send_sem=send, recv_sem=recv,
            device_id={axis: target}, device_id_type=MESH,
        )

    owned = ((0, width), (0, wide_q), (wide_q, wide_p), (0, width))

    def source(m, k):
        rows = pl.ds(k * step, step)
        lanes = pl.ds(*owned[m])
        return (up_ref, final, final, down_ref)[m].at[rows, lanes]

    def hop(m, k, left, src):
        lanes = pl.ds(*owned[m])
        box, send, recv = (from_right, s_left, r_left) if left else (from_left, s_right, r_right)
        slot = m
        return remote(
            src, box.at[slot, pl.ds(k * step, step), lanes], send.at[m, k], recv.at[m, k],
            "seq", jnp.maximum(z - 1, 0) if left else jnp.minimum(z + 1, ways - 1),
        )

    def relay_src(m, k):
        return relay.at[m, pl.ds(k * step, step), pl.ds(*owned[m])]

    def begin(m):
        for k in range(chunks):
            if m < ways - 1:
                @pl.when(z == ways - 1)
                def _():
                    hop(m, k, True, source(m, k)).start()
            if m > 0:
                @pl.when(z == 0)
                def _():
                    hop(m, k, False, source(m, k)).start()

    def pass_on(m, k):
        rows = pl.ds(k * step, step)
        lanes = pl.ds(*owned[m])
        strip = 64

        def added(box):
            def body(i, unused):
                part = pl.ds(pl.multiple_of(k * step + i * strip, strip), strip)
                src = (up_ref, final, final, down_ref)[m]
                relay[m, part, lanes] = (
                    src[part, lanes].astype(F32) + box[m, part, lanes].astype(F32)
                ).astype(LOW)
                return unused

            lax.fori_loop(0, step // strip, body, 0)

        if m < ways - 2:
            @pl.when((z > m) & (z < ways - 1))
            def _():
                hop(m, k, True, source(m, k)).wait_recv()
                added(from_right)
                hop(m, k, True, relay_src(m, k)).start()
        if m > 1:
            @pl.when((z < m) & (z > 0))
            def _():
                hop(m, k, False, source(m, k)).wait_recv()
                added(from_left)
                hop(m, k, False, relay_src(m, k)).start()

    def settle(m, k):
        lanes = pl.ds(*owned[m])
        strip = 64

        @pl.when(z == m)
        def _():
            if m < ways - 1:
                hop(m, k, True, source(m, k)).wait_recv()
            if m > 0:
                hop(m, k, False, source(m, k)).wait_recv()

            def body(i, unused):
                part = pl.ds(pl.multiple_of(k * step + i * strip, strip), strip)
                src = (up_ref, final, final, down_ref)[m]
                total = src[part, lanes].astype(F32)
                if m < ways - 1:
                    total += from_right[m, part, lanes].astype(F32)
                if m > 0:
                    total += from_left[m, part, lanes].astype(F32)
                width_m = owned[m][1]
                out_ref[part, pl.ds(0, width_m)] = total.astype(LOW)
                if width_m < width:
                    out_ref[part, pl.ds(width_m, width - width_m)] = jnp.zeros(
                        (strip, width - width_m), LOW
                    )
                return unused

            lax.fori_loop(0, step // strip, body, 0)

    begin(0)
    begin(3)

    strip = 64

    def own(h, block, start, rows):
        part = pl.ds(pl.multiple_of(h * half + start, strip), rows)
        q = qkv_ref[part, pl.ds(pl.multiple_of(block * wide_q, 128), wide_q)]
        p = proj_ref[part, pl.ds(pl.multiple_of(block * wide_p, 128), wide_p)]
        return jnp.concatenate([q, p], axis=1).astype(F32)

    def first(h, k):
        block = 2 * k + (1 - core)
        rows = pl.ds(h * half, half)
        return [
            remote(
                qkv_ref.at[rows, pl.ds(pl.multiple_of(block * wide_q, 128), wide_q)],
                one.at[h, k, :, pl.ds(0, wide_q)], s_one.at[h, k, 0], r_one.at[h, k, 0],
                "dp", partners[0],
            ),
            remote(
                proj_ref.at[rows, pl.ds(pl.multiple_of(block * wide_p, 128), wide_p)],
                one.at[h, k, :, pl.ds(wide_q, wide_p)], s_one.at[h, k, 1], r_one.at[h, k, 1],
                "dp", partners[0],
            ),
        ]

    go = [[(2 * j + (1 - x)) for j in range(2)], [(2 * (1 - y) + j) for j in range(2)]]
    stay = [[(2 * j + x) for j in range(2)], [(2 * y + j) for j in range(2)]]
    for group in (go, stay):
        for j in range(2):
            for h in range(2):
                for copy in first(h, group[h][j]):
                    copy.start()

    def second(h, j):
        return remote(send_two.at[h, j], two.at[h, j], s_two.at[h, j], r_two.at[h, j],
                      "dp", partners[1 + h])

    for j in range(2):
        for h in range(2):
            k = go[h][j]
            for copy in first(h, k):
                copy.wait_recv()

            def body(i, unused):
                part = pl.ds(pl.multiple_of(i * strip, strip), strip)
                value = own(h, 2 * k + core, i * strip, strip) + one[h, k, part, :].astype(F32)
                send_two[h, j, part, :] = value.astype(LOW)
                return unused

            lax.fori_loop(0, half // strip, body, 0)
            second(h, j).start()
    for k in range(chunks):
        pass_on(0, k)
        pass_on(3, k)

    def third(h):
        return remote(send_three.at[h], three.at[h], s_three.at[h], r_three.at[h],
                      "dp", partners[2 - h])

    mine = [y, x]
    for h in range(2):
        for j in range(2):
            for copy in first(h, stay[h][j]):
                copy.wait_recv()
        for j in range(2):
            second(h, j).wait_recv()
        j = 1 - mine[h]
        k = 2 * j + x if h == 0 else 2 * y + j

        def body(i, unused):
            part = pl.ds(pl.multiple_of(i * strip, strip), strip)
            value = (
                own(h, 2 * k + core, i * strip, strip)
                + one[h, k, part, :].astype(F32)
                + two[h, j, part, :].astype(F32)
            )
            send_three[h, part, :] = value.astype(LOW)
            return unused

        lax.fori_loop(0, half // strip, body, 0)
        third(h).start()
    for h in range(2):
        third(h).wait_recv()
        j = mine[h]
        k = 2 * y + x

        def body(i, unused):
            part = pl.ds(pl.multiple_of(i * strip, strip), strip)
            value = (
                own(h, 2 * k + core, i * strip, strip)
                + one[h, k, part, :].astype(F32)
                + two[h, j, part, :].astype(F32)
                + three[h, part, :].astype(F32)
            )
            final[pl.ds(pl.multiple_of(h * half + i * strip, strip), strip), :] = value.astype(LOW)
            return unused

        lax.fori_loop(0, half // strip, body, 0)
    begin(1)
    begin(2)
    for k in range(chunks):
        pass_on(1, k)
        pass_on(2, k)
    for m in (0, 3, 1, 2):
        for k in range(chunks):
            settle(m, k)

    for h in range(2):
        for k in range(4):
            for copy in first(h, k):
                copy.wait_send()
        for j in range(2):
            second(h, j).wait_send()
        third(h).wait_send()
    for m in range(OWNERS):
        for k in range(chunks):
            if m < ways - 1:
                @pl.when(z > m)
                def _():
                    hop(m, k, True, source(m, k)).wait_send()
            if m > 0:
                @pl.when(z < m)
                def _():
                    hop(m, k, False, source(m, k)).wait_send()


def combine(ways, qkv, proj, up, down):
    size, width = up.shape
    wide_q, wide_p = qkv.shape[1] // 8, proj.shape[1] // 8
    half = size // 2
    vmem = pl.BlockSpec(memory_space=pltpu.VMEM)
    dma = pltpu.SemaphoreType.DMA
    return pl.pallas_call(
        functools.partial(combine_kernel, ways, wide_q, wide_p),
        out_shape=jax.ShapeDtypeStruct((size, width), LOW),
        in_specs=[vmem] * 4,
        out_specs=vmem,
        scratch_shapes=[
            pltpu.VMEM((2, 4, half, width), LOW),
            pltpu.VMEM((2, 2, half, width), LOW),
            pltpu.VMEM((2, 2, half, width), LOW),
            pltpu.VMEM((2, half, width), LOW),
            pltpu.VMEM((2, half, width), LOW),
            pltpu.VMEM((size, width), LOW),
            pltpu.VMEM((OWNERS, size, width), LOW),
            pltpu.VMEM((OWNERS, size, width), LOW),
            pltpu.VMEM((OWNERS, size, width), LOW),
            dma((2, 4, 2)), dma((2, 4, 2)), dma((2, 2)), dma((2, 2)), dma((2,)), dma((2,)),
            dma((OWNERS, 4)), dma((OWNERS, 4)), dma((OWNERS, 4)), dma((OWNERS, 4)),
        ],
        compiler_params=pltpu.CompilerParams(
            collective_id=1, has_side_effects=True, vmem_limit_bytes=56 << 20
        ),
        cost_estimate=pl.CostEstimate(flops=50_000_000_000, bytes_accessed=1 << 23, transcendentals=0),
        name="combine",
    )(qkv, proj, up, down)


def gram_kernel(
    gram_ref, out_ref, one, send_two, two, send_three, three,
    s_one, r_one, s_two, r_two, s_three, r_three, s_back, r_back,
):
    (core, x, y), partners = plane()
    size = gram_ref.shape[0]
    rows = size // 8
    half = size // 2
    greet([("dp", p, None) for p in partners])

    def remote(src, dst, send, recv, target):
        return pltpu.make_async_remote_copy(
            src_ref=src, dst_ref=dst, send_sem=send, recv_sem=recv,
            device_id={"dp": target}, device_id_type=MESH,
        )

    def block(ref, h, d):
        return ref.at[pl.ds(pl.multiple_of(d * rows, rows), rows), pl.ds(h * half, half)]

    def own(h, d):
        return gram_ref[
            pl.ds(pl.multiple_of(d * rows, rows), rows), pl.ds(h * half, half)
        ].astype(F32)

    def first(h, k):
        return remote(block(gram_ref, h, 2 * k + 1 - core), one.at[h, k], s_one.at[h, k],
                      r_one.at[h, k], partners[0])

    go = [[(2 * j + (1 - x)) for j in range(2)], [(2 * (1 - y) + j) for j in range(2)]]
    stay = [[(2 * j + x) for j in range(2)], [(2 * y + j) for j in range(2)]]
    for group in (go, stay):
        for j in range(2):
            for h in range(2):
                first(h, group[h][j]).start()

    def second(h, j):
        return remote(send_two.at[h, j], two.at[h, j], s_two.at[h, j], r_two.at[h, j], partners[1 + h])

    for j in range(2):
        for h in range(2):
            k = go[h][j]
            first(h, k).wait_recv()
            send_two[h, j] = (own(h, 2 * k + core) + one[h, k].astype(F32)).astype(LOW)
            second(h, j).start()

    def third(h):
        return remote(send_three.at[h], three.at[h], s_three.at[h], r_three.at[h], partners[2 - h])

    mine = [y, x]
    for h in range(2):
        for j in range(2):
            first(h, stay[h][j]).wait_recv()
        for j in range(2):
            second(h, j).wait_recv()
        j = 1 - mine[h]
        k = 2 * j + x if h == 0 else 2 * y + j
        send_three[h] = (
            own(h, 2 * k + core) + one[h, k].astype(F32) + two[h, j].astype(F32)
        ).astype(LOW)
        third(h).start()

    def back(h, stage, d):
        target = (partners[2 - h], partners[1 + h], partners[0])[stage]
        place = block(out_ref, h, d)
        slot = (0, 1, 3)[stage]
        return lambda i: remote(place, place, s_back.at[h, slot + i], r_back.at[h, slot + i], target)

    k = 2 * y + x
    for h in range(2):
        third(h).wait_recv()
        value = (
            own(h, 2 * k + core)
            + one[h, k].astype(F32)
            + two[h, mine[h]].astype(F32)
            + three[h].astype(F32)
        ).astype(LOW)
        d = 2 * k + core
        out_ref[pl.ds(pl.multiple_of(d * rows, rows), rows), pl.ds(h * half, half)] = value
        back(h, 0, d)(0).start()
        back(h, 1, d)(0).start()
        back(h, 2, d)(0).start()
    k_next = [2 * (1 - y) + x, 2 * y + (1 - x)]
    for h in range(2):
        d = 2 * k_next[h] + core
        back(h, 0, d)(0).wait_recv()
        back(h, 1, d)(1).start()
        back(h, 2, d)(1).start()
    for h in range(2):
        for i in range(2):
            if h == 0:
                kk = 2 * (y if i == 0 else 1 - y) + (1 - x)
            else:
                kk = 2 * (1 - y) + (x if i == 0 else 1 - x)
            d = 2 * kk + core
            back(h, 1, d)(i).wait_recv()
            back(h, 2, d)(2 + i).start()
    for h in range(2):
        for i, kk in enumerate(
            (
                2 * y + x,
                k_next[h],
                2 * y + (1 - x) if h == 0 else 2 * (1 - y) + x,
                2 * (1 - y) + (1 - x),
            )
        ):
            back(h, 2, 2 * kk + 1 - core)(i).wait_recv()

    for h in range(2):
        for j in range(4):
            first(h, j).wait_send()
        for j in range(2):
            second(h, j).wait_send()
        third(h).wait_send()
        d = 2 * k + core
        back(h, 0, d)(0).wait_send()
        for i in range(2):
            back(h, 1, d)(i).wait_send()
        for i in range(4):
            back(h, 2, d)(i).wait_send()


def gram_sum(gram):
    size = gram.shape[0]
    rows, half = size // 8, size // 2
    vmem = pl.BlockSpec(memory_space=pltpu.VMEM)
    dma = pltpu.SemaphoreType.DMA
    return pl.pallas_call(
        gram_kernel,
        out_shape=jax.ShapeDtypeStruct((size, size), LOW),
        in_specs=[vmem],
        out_specs=vmem,
        scratch_shapes=[
            pltpu.VMEM((2, 4, rows, half), LOW),
            pltpu.VMEM((2, 2, rows, half), LOW),
            pltpu.VMEM((2, 2, rows, half), LOW),
            pltpu.VMEM((2, rows, half), LOW),
            pltpu.VMEM((2, rows, half), LOW),
            dma((2, 4)), dma((2, 4)), dma((2, 2)), dma((2, 2)), dma((2,)), dma((2,)),
            dma((2, 7)), dma((2, 7)),
        ],
        compiler_params=pltpu.CompilerParams(
            collective_id=2, has_side_effects=True, vmem_limit_bytes=24 << 20
        ),
        cost_estimate=pl.CostEstimate(flops=20_000_000_000, bytes_accessed=1 << 22, transcendentals=0),
        name="gram_sum",
    )(gram)


def spread_kernel(ways, widths, chunks, own_ref, *refs):
    outs = refs[:OWNERS]
    s_left, r_left, s_right, r_right, s_own = refs[OWNERS:]
    z = lax.axis_index("seq")
    step = own_ref.shape[0] // chunks
    greet([("seq", jnp.maximum(z - 1, 0), z > 0), ("seq", jnp.minimum(z + 1, ways - 1), z < ways - 1)])

    def hop(m, k, left, relayed):
        rows = pl.ds(k * step, step)
        place = outs[m].at[rows, :]
        src = place if relayed else own_ref.at[rows, pl.ds(0, widths[m])]
        send, recv = (s_left, r_left) if left else (s_right, r_right)
        return pltpu.make_async_remote_copy(
            src_ref=src, dst_ref=place, send_sem=send.at[m, k], recv_sem=recv.at[m, k],
            device_id={"seq": jnp.maximum(z - 1, 0) if left else jnp.minimum(z + 1, ways - 1)},
            device_id_type=MESH,
        )

    def local(m):
        return pltpu.make_async_copy(own_ref.at[:, pl.ds(0, widths[m])], outs[m], s_own)

    for m in range(OWNERS):
        @pl.when(z == m)
        def _():
            for k in range(chunks):
                if m < ways - 1:
                    hop(m, k, False, False).start()
                if m > 0:
                    hop(m, k, True, False).start()
            local(m).start()

    for distance in range(1, ways):
        for k in range(chunks):
            for m in range(OWNERS):
                if m + distance < ways:
                    @pl.when(z == m + distance)
                    def _():
                        hop(m, k, False, True).wait_recv()
                        if m + distance < ways - 1:
                            hop(m, k, False, True).start()
                if m - distance >= 0:
                    @pl.when(z == m - distance)
                    def _():
                        hop(m, k, True, True).wait_recv()
                        if m - distance > 0:
                            hop(m, k, True, True).start()
    for m in range(OWNERS):
        @pl.when(z == m)
        def _():
            local(m).wait()

        for k in range(chunks):
            @pl.when((z >= m) & (z < ways - 1))
            def _():
                hop(m, k, False, True).wait_send()

            @pl.when((z <= m) & (z > 0))
            def _():
                hop(m, k, True, True).wait_send()


def spread_all(ways, own, widths, number):
    size = own.shape[0]
    chunks = 8
    vmem = pl.BlockSpec(memory_space=pltpu.VMEM)
    dma = pltpu.SemaphoreType.DMA
    return pl.pallas_call(
        functools.partial(spread_kernel, ways, widths, chunks),
        out_shape=[jax.ShapeDtypeStruct((size, w), LOW) for w in widths],
        in_specs=[vmem],
        out_specs=[vmem] * OWNERS,
        scratch_shapes=[dma((OWNERS, chunks))] * 4 + [dma(())],
        compiler_params=pltpu.CompilerParams(
            collective_id=number, has_side_effects=True, vmem_limit_bytes=24 << 20
        ),
        cost_estimate=pl.CostEstimate(flops=30_000_000_000, bytes_accessed=1 << 22, transcendentals=0),
    )(own)


def norm_forward(values, gain_row, offset):
    center = values - jnp.mean(values, axis=-1, keepdims=True)
    inv_scale = lax.rsqrt(jnp.mean(center * center, axis=-1, keepdims=True) + NORM_EPS)
    unit_values = center * inv_scale
    return (unit_values * gain_row + offset, unit_values, inv_scale)


def norm_backward(upstream, unit_values, inv_scale, gain_row):
    scaled = upstream * gain_row
    inner_sum = jnp.mean(scaled * unit_values, axis=-1, keepdims=True)
    input_grad = inv_scale * (
        scaled - jnp.mean(scaled, axis=-1, keepdims=True) - unit_values * inner_sum
    )
    return (input_grad, jnp.sum(upstream * unit_values, axis=0), jnp.sum(upstream, axis=0))


def gelu_both(values):
    square = values * values
    tangent = jnp.tanh(GELU_C * (values + 0.044715 * square * values))
    slope = 0.5 * (1.0 + tangent) + 0.5 * values * (1.0 - tangent * tangent) * GELU_C * (
        1.0 + 3.0 * 0.044715 * square
    )
    return 0.5 * values * (1.0 + tangent), slope


def on_device(
    tokens,
    cotangent,
    qkv_weight,
    proj_weight,
    up_weight,
    down_weight,
    norm_gains,
    biases,
    up_bias,
    head_slopes,
    qkv_moment,
    proj_moment,
    up_moment,
    down_moment,
    gains_moment,
    biases_moment,
    upbias_moment,
):
    rows, width = tokens.shape
    ways = lax.axis_size("seq")
    here = lax.axis_index("seq")
    me = lax.axis_index("dp")
    length = rows * ways
    own_width = width // ways
    chunks = 2
    chunk = own_width // chunks
    chunk_heads = chunk // HEAD
    own_slopes = lax.dynamic_slice_in_dim(
        head_slopes, here * (own_width // HEAD), own_width // HEAD, 0
    )
    slope_rows = [
        jnp.repeat(own_slopes[c * chunk_heads : (c + 1) * chunk_heads], BLOCK)[None]
        for c in range(chunks)
    ]

    inputs = tokens.astype(F32)
    normed_one, unit_one, scale_one = norm_forward(inputs, norm_gains[0], biases[0])
    normed_one = normed_one.astype(LOW)
    bias_row = jnp.concatenate([biases[1], jnp.zeros_like(biases[1]), biases[2]])
    mixed = (mm(normed_one, qkv_weight) + bias_row).astype(LOW)

    def take_mixed(c):
        def take(source, d):
            return jnp.stack(
                [
                    lax.dynamic_slice_in_dim(
                        source, part * width + d * own_width + c * chunk, chunk, 1
                    )
                    for part in range(3)
                ]
            )

        return take

    qkv_pieces = [depart(mixed, take_mixed(c)) for c in range(chunks)]
    qkv = []
    attended = jnp.zeros((rows, width), LOW)
    kept = []
    for c in range(chunks):
        if c:
            qkv_pieces[c], out = lax.optimization_barrier((qkv_pieces[c], out))
        qkv.append(arrange(qkv_pieces[c], lambda d: (0, d * rows, 0), (3, length, chunk)))
        out, wide, log_totals = attend_forward(qkv[c], slope_rows[c], BLOCK)
        kept.append((wide, log_totals))
        for shift in range(ways):
            piece = lax.dynamic_slice_in_dim(out, ((here + shift) % ways) * rows, rows, 0)
            if shift:
                piece = lax.ppermute(piece, "seq", [(i, (i + shift) % ways) for i in range(ways)])
            attended = lax.dynamic_update_slice(
                attended, piece, (0, ((here - shift) % ways) * own_width + c * chunk)
            )

    middle = inputs + mm(attended, proj_weight) + biases[3]
    normed_two, unit_two, scale_two = norm_forward(middle, norm_gains[1], biases[4])
    normed_two = normed_two.astype(LOW)
    before = mm(normed_two, up_weight) + up_bias
    hidden, slope = gelu_both(before)
    hidden = hidden.astype(LOW)
    block_out = (middle + mm(hidden, down_weight) + biases[5]).astype(LOW)
    upstream = cotangent.astype(F32)
    hidden_grad = mm(cotangent, down_weight, NT)
    before_grad = (hidden_grad * slope).astype(LOW)
    normed_two_grad = mm(before_grad, up_weight, NT)
    middle_back, gain_two_grad, offset_two_grad = norm_backward(
        normed_two_grad, unit_two, scale_two, norm_gains[1]
    )
    middle_grad = upstream + middle_back
    branch_grad = middle_grad.astype(LOW)
    heads_grad = mm(branch_grad, proj_weight, NT).astype(LOW)

    grad_pieces = [
        depart(
            heads_grad,
            lambda source, d: lax.dynamic_slice_in_dim(source, d * own_width + c * chunk, chunk, 1),
        )
        for c in range(chunks)
    ]
    down_pair = gradient_pair(cotangent, hidden, 1)
    up_pair = gradient_pair(normed_two, before_grad, 1)
    grad_pieces[0], down_pair, up_pair = lax.optimization_barrier(
        (grad_pieces[0], down_pair, up_pair)
    )

    mixed_grad = jnp.zeros((3, rows, width), LOW)
    for c in range(chunks):
        if c:
            grad_pieces[c], back = lax.optimization_barrier((grad_pieces[c], back))
        grad = arrange(grad_pieces[c], lambda d: (d * rows, 0), (length, chunk))
        back = attend_backward(qkv[c], grad, *kept[c], slope_rows[c], BLOCK)
        for shift in range(ways):
            piece = lax.dynamic_slice_in_dim(back, ((here + shift) % ways) * rows, rows, 1)
            if shift:
                piece = lax.ppermute(piece, "seq", [(i, (i + shift) % ways) for i in range(ways)])
            mixed_grad = lax.dynamic_update_slice(
                mixed_grad, piece, (0, 0, ((here - shift) % ways) * own_width + c * chunk)
            )
    mixed_flat = jnp.concatenate([mixed_grad[0], mixed_grad[1], mixed_grad[2]], 1)

    down_part = reduce_blocks(down_pair, 1, other_bits())
    up_part = reduce_blocks(up_pair, 1, other_bits())
    widths = tuple(
        moment.shape[1] for moment in (up_moment, qkv_moment, proj_moment, down_moment.T)
    )
    quick = lax.axis_size("dp") == 8 and ways == OWNERS and all(w % 128 == 0 for w in widths)
    up_owner, qkv_owner, proj_owner, down_owner = range(OWNERS)
    pad_width = max(widths)

    def owned_of(members):
        padded = [jnp.pad(m, ((0, 0), (0, pad_width - m.shape[1]))) for m in members]
        return jnp.where(
            here < 2,
            jnp.where(here == 0, padded[0], padded[1]),
            jnp.where(here == 2, padded[2], padded[3]),
        )

    if quick:
        owned_grad = combine(
            ways,
            mm(normed_one, mixed_flat, TN).astype(LOW),
            mm(attended, branch_grad, TN).astype(LOW),
            up_part,
            down_part,
        )
    else:
        proj_part = reduce_blocks(gradient_pair(attended, branch_grad, 1), 1, other_bits())
        qkv_part = reduce_blocks(gradient_pair(normed_one, mixed_flat, 1), 1, other_bits())
        owned_grad = owned_of(
            [
                collect(up_part, up_owner, 2),
                collect(qkv_part, qkv_owner, 1),
                collect(proj_part, proj_owner, 1),
                collect(down_part, down_owner, 2),
            ]
        )

    normed_one_grad = mm(mixed_flat, qkv_weight, NT)
    input_back, gain_one_grad, offset_one_grad = norm_backward(
        normed_one_grad, unit_one, scale_one, norm_gains[0]
    )
    tokens_grad = middle_grad + input_back

    def columns(value):
        return jnp.sum(value.astype(F32), axis=0)

    vectors = jnp.stack(
        [
            gain_one_grad,
            gain_two_grad,
            offset_one_grad,
            columns(mixed_grad[0]),
            columns(mixed_grad[2]),
            columns(branch_grad),
            offset_two_grad,
            columns(upstream),
        ]
    )
    vectors = jnp.concatenate([vectors, columns(before_grad).reshape(-1, width)], 0)
    vectors = sum_everywhere(vectors)

    def own_columns(matrix, count):
        return lax.dynamic_slice_in_dim(matrix, me * count, count, 1).astype(F32)

    gains_sum = own_columns(vectors[:2], gains_moment.shape[1])
    biases_sum = own_columns(vectors[2:8], biases_moment.shape[1])
    upbias_count = upbias_moment.shape[0]
    upbias_sum = lax.dynamic_slice_in_dim(
        vectors[8:].reshape(-1), me * upbias_count, upbias_count, 0
    )

    def state_of(moment, grad):
        return MOMENTUM * moment + grad.astype(F32)

    owned_moment = owned_of([up_moment, qkv_moment, proj_moment, down_moment.T])
    owned_block = state_of(owned_moment, owned_grad).astype(LOW)
    gram = mm(owned_block, owned_block, NT)
    gram = gram_sum(gram.astype(LOW)) if quick else gram_total(gram)
    iterate = orthogonal(gram, owned_block)

    up_sum, qkv_sum, proj_sum, down_sum = [g.astype(F32) for g in share(owned_grad, widths, iterate)]
    down_sum = down_sum.T
    if quick:
        steps = spread_all(ways, iterate, widths, 3)
    else:
        steps = share(iterate, widths, None)
    qkv_state = state_of(qkv_moment, qkv_sum)
    proj_state = state_of(proj_moment, proj_sum)
    up_state = state_of(up_moment, up_sum)
    down_state = state_of(down_moment, down_sum)
    gains_state = state_of(gains_moment, gains_sum)
    biases_state = state_of(biases_moment, biases_sum)
    upbias_state = state_of(upbias_moment, upbias_sum)

    def rate_of(shape):
        return -RATE_MATRIX * math.sqrt(max(shape))

    def step_of(owner, shape):
        return rate_of(shape) * steps[owner].astype(F32)

    qkv_new = own_columns(qkv_weight, qkv_state.shape[1]) + step_of(
        qkv_owner, qkv_weight.shape
    )
    proj_new = own_columns(proj_weight, proj_state.shape[1]) + step_of(
        proj_owner, proj_weight.shape
    )
    up_new = own_columns(up_weight, up_state.shape[1]) + step_of(
        up_owner, up_weight.shape
    )
    down_count = down_state.shape[0]
    down_rows = lax.dynamic_slice_in_dim(down_weight, me * down_count, down_count, 0).astype(F32)
    down_new = down_rows + step_of(down_owner, down_weight.shape).T
    gains_new = own_columns(norm_gains, gains_state.shape[1]) - RATE_VECTOR * gains_state
    biases_new = own_columns(biases, biases_state.shape[1]) - RATE_VECTOR * biases_state
    upbias_new = (
        lax.dynamic_slice_in_dim(up_bias, me * upbias_count, upbias_count, 0)
        - RATE_VECTOR * upbias_state
    )
    return (
        block_out,
        tokens_grad,
        qkv_sum,
        proj_sum,
        up_sum,
        down_sum,
        gains_sum,
        biases_sum,
        upbias_sum,
        qkv_state,
        proj_state,
        up_state,
        down_state,
        gains_state,
        biases_state,
        upbias_state,
        qkv_new,
        proj_new,
        up_new,
        down_new,
        gains_new,
        biases_new,
        upbias_new,
    )


def solution(mesh):
    rows, columns, copied = P(("dp", "seq"), None), P(None, "dp"), P()

    return jax.shard_map(
        on_device,
        mesh=mesh,
        in_specs=(
            (rows, rows)
            + (copied,) * 8
            + (columns, columns, columns, P("dp", None), columns, columns, P("dp"))
        ),
        out_specs=(
            (rows, rows)
            + (columns, columns, columns, P("dp", None), columns, columns, P("dp")) * 3
        ),
        check_vma=False,
    )
```

```python
import functools
import math

import jax
import jax.numpy as jnp
from jax import lax
from jax.experimental import pallas as pl
from jax.experimental.pallas import tpu as pltpu
from jax.sharding import PartitionSpec as P


NS_ITERS = 5


MOMENTUM = 0.9
RATE_MATRIX = 0.2
RATE_VECTOR = 0.0015
NORM_EPS = 1e-05
ORTHO_EPS = 1e-07
GELU_C = 0.7978845608028654
MASKED = -1e30
HEAD = 64
BLOCK = 256
LOW = jnp.bfloat16
F32 = jnp.float32

NT = (((1,), (1,)), ((), ()))
NN = (((1,), (0,)), ((), ()))
TN = (((0,), (0,)), ((), ()))


def mm(left, right, dims=NN):
    return lax.dot_general(left, right, dims, preferred_element_type=F32)


def stack_heads(block, groups, scale=None):
    lane = lax.broadcasted_iota(jnp.int32, block.shape, 1)
    if scale is not None:
        block = block * scale
    zero = jnp.zeros_like(block)
    return [
        jnp.where((lane >= h * HEAD) & (lane < (h + 1) * HEAD), block, zero)
        for h in range(groups)
    ]


def bias_tiles(slope_row, block, plain_ref, edge_ref, groups):
    shape = plain_ref.shape
    row = lax.broadcasted_iota(jnp.int32, shape, 0)
    col = lax.broadcasted_iota(jnp.int32, (shape[0], block), 1)
    tile = row.astype(F32) * slope_row
    plain_ref[...] = tile
    for h in range(groups):
        part = slice(h * block, (h + 1) * block)
        edge_ref[:, part] = jnp.where(row[:, part] <= col, tile[:, part], MASKED)


def forward_kernel(
    groups, block, slope_ref, q_ref, k_ref, v_ref, out_ref, wide_ref, log_ref, plain, edge, vt, qs, acc
):
    i = pl.program_id(0)
    slope = slope_ref[...]

    @pl.when(i == 0)
    def _():
        bias_tiles(slope, block, plain, edge, groups)
        vt[...] = v_ref[0].T

    for h, part in enumerate(stack_heads(q_ref[0], groups, LOW(1.0 / math.sqrt(HEAD)))):
        qs[h * block : (h + 1) * block, :] = part
    acc[...] = jnp.zeros_like(acc)
    wide = groups * block

    def visit(j, carry, tile_ref):
        peak, total = carry
        start = pl.multiple_of(j * block, block)
        x = mm(k_ref[0, pl.ds(start, block), :], qs[...], NT) + tile_ref[...]
        shift = slope * (j * block).astype(F32)
        new = jnp.maximum(peak, jnp.max(x, axis=0, keepdims=True) + shift)
        p = jnp.exp(x + (shift - new))
        alpha = jnp.exp(peak - new)
        total = total * alpha + jnp.sum(p, axis=0, keepdims=True)
        low = p.astype(LOW)
        for h in range(groups):
            part = slice(h * block, (h + 1) * block)
            rows = slice(h * HEAD, (h + 1) * HEAD)
            acc[rows, :] = acc[rows, :] * alpha[:, part] + mm(
                vt[rows, pl.ds(start, block)], low[:, part]
            )
        return new, total

    start = (jnp.full((1, wide), MASKED, F32), jnp.zeros((1, wide), F32))
    carry = lax.fori_loop(0, i, lambda j, c: visit(j, c, plain), start)
    peak, total = visit(i, carry, edge)
    log_ref[0] = peak + jnp.log(total)
    inverse = 1.0 / total
    for h in range(groups):
        rows = slice(h * HEAD, (h + 1) * HEAD)
        acc[rows, :] = acc[rows, :] * inverse[:, h * block : (h + 1) * block]
    out = acc[...].T
    wide_ref[...] = out
    out_ref[...] = out.astype(LOW)


def attend_forward(qkv, slope_row, block):
    length, width = qkv.shape[1:]
    groups = width // HEAD
    count = length // block
    wide = groups * block
    part = pl.BlockSpec((block, width), lambda i: (i, 0))
    return pl.pallas_call(
        functools.partial(forward_kernel, groups, block),
        grid=(count,),
        in_specs=[
            pl.BlockSpec((1, wide), lambda i: (0, 0)),
            pl.BlockSpec((1, block, width), lambda i: (0, i, 0)),
            pl.BlockSpec((1, length, width), lambda i: (1, 0, 0)),
            pl.BlockSpec((1, length, width), lambda i: (2, 0, 0)),
        ],
        out_specs=[part, part, pl.BlockSpec((1, 1, wide), lambda i: (i, 0, 0))],
        out_shape=[
            jax.ShapeDtypeStruct((length, width), LOW),
            jax.ShapeDtypeStruct((length, width), F32),
            jax.ShapeDtypeStruct((count, 1, wide), F32),
        ],
        scratch_shapes=[
            pltpu.VMEM((block, wide), F32),
            pltpu.VMEM((block, wide), F32),
            pltpu.VMEM((width, length), LOW),
            pltpu.VMEM((wide, width), LOW),
            pltpu.VMEM((width, block), F32),
        ],
        compiler_params=pltpu.CompilerParams(vmem_limit_bytes=32 << 20),
        cost_estimate=pl.CostEstimate(
            flops=16 * length * length * width,
            bytes_accessed=12 * length * width,
            transcendentals=length * length * groups,
        ),
        name="attend_forward",
    )(slope_row, qkv, qkv, qkv)


def backward_kernel(
    groups, block, slope_ref, q_ref, k_ref, v_ref, grad_ref, wide_ref, log_ref,
    out_ref, plain, edge, qs, grads, delta, dq, dk, dv, ks
):
    j = pl.program_id(0)
    count = pl.num_programs(0)
    slope = slope_ref[...]
    scale = 1.0 / math.sqrt(HEAD)

    @pl.when(j == 0)
    def _():
        bias_tiles(slope, block, plain, edge, groups)
        dq[...] = jnp.zeros_like(dq)

        def prepare(i, unused):
            rows = pl.ds(pl.multiple_of(i * block, block), block)
            grad = grad_ref[rows, :]
            for h, part in enumerate(stack_heads(q_ref[0, rows, :], groups, LOW(scale))):
                qs[i, h * block : (h + 1) * block, :] = part
            for h, part in enumerate(stack_heads(grad, groups)):
                grads[i, h * block : (h + 1) * block, :] = part
            both = (wide_ref[rows, :] * grad.astype(F32)).T
            for h in range(groups):
                delta[i, :, h * block : (h + 1) * block] = jnp.sum(
                    both[h * HEAD : (h + 1) * HEAD, :], axis=0, keepdims=True
                )
            return unused

        lax.fori_loop(0, count, prepare, 0)

    keys = k_ref[0]
    values = v_ref[0]
    for h, part in enumerate(stack_heads(keys, groups)):
        ks[h] = part
    dk[...] = jnp.zeros_like(dk)
    dv[...] = jnp.zeros_like(dv)
    shift = slope * (j * block).astype(F32)

    def visit(i, tile_ref):
        heads_q = qs[i]
        heads_grad = grads[i]
        p = jnp.exp(mm(keys, heads_q, NT) + tile_ref[...] + (shift - log_ref[i]))
        ds = p * (mm(values, heads_grad, NT) - delta[i])
        p_low = p.astype(LOW)
        ds_low = ds.astype(LOW)
        dv[...] += mm(p_low, heads_grad)
        dk[...] += mm(ds_low, heads_q)
        total = mm(ds_low[:, :block], ks[0], TN)
        for h in range(1, groups):
            total += mm(ds_low[:, h * block : (h + 1) * block], ks[h], TN)
        dq[pl.ds(pl.multiple_of(i * block, block), block), :] += total

    visit(j, edge)

    def step(i, unused):
        visit(i, plain)
        return unused

    lax.fori_loop(j + 1, count, step, 0)
    out_ref[0] = (dq[pl.ds(pl.multiple_of(j * block, block), block), :] * scale).astype(LOW)
    out_ref[1] = dk[...].astype(LOW)
    out_ref[2] = dv[...].astype(LOW)


def attend_backward(qkv, grad, attended, log_totals, slope_row, block):
    length, width = qkv.shape[1:]
    groups = width // HEAD
    count = length // block
    wide = groups * block
    whole = pl.BlockSpec((length, width), lambda i: (0, 0))
    return pl.pallas_call(
        functools.partial(backward_kernel, groups, block),
        grid=(count,),
        in_specs=[
            pl.BlockSpec((1, wide), lambda i: (0, 0)),
            pl.BlockSpec((1, length, width), lambda i: (0, 0, 0)),
            pl.BlockSpec((1, block, width), lambda i: (1, i, 0)),
            pl.BlockSpec((1, block, width), lambda i: (2, i, 0)),
            whole,
            whole,
            pl.BlockSpec((count, 1, wide), lambda i: (0, 0, 0)),
        ],
        out_specs=pl.BlockSpec((3, block, width), lambda i: (0, i, 0)),
        out_shape=jax.ShapeDtypeStruct((3, length, width), LOW),
        scratch_shapes=[
            pltpu.VMEM((block, wide), F32),
            pltpu.VMEM((block, wide), F32),
            pltpu.VMEM((count, wide, width), LOW),
            pltpu.VMEM((count, wide, width), LOW),
            pltpu.VMEM((count, 1, wide), F32),
            pltpu.VMEM((length, width), F32),
            pltpu.VMEM((block, width), F32),
            pltpu.VMEM((block, width), F32),
            pltpu.VMEM((groups, block, width), LOW),
        ],
        compiler_params=pltpu.CompilerParams(vmem_limit_bytes=40 << 20),
        cost_estimate=pl.CostEstimate(
            flops=40 * length * length * width,
            bytes_accessed=18 * length * width,
            transcendentals=length * length * groups,
        ),
        name="attend_backward",
    )(slope_row, qkv, qkv, qkv, grad, attended, log_totals)


def ortho_kernel(tile, gram_ref, block_ref, out_ref, square, square_low, cross, cross_low, state):
    size = gram_ref.shape[0]
    steps = size // tile
    trace = jnp.zeros((1, 1), F32)
    for r in range(steps):
        rows = slice(r * tile, (r + 1) * tile)
        piece = gram_ref[rows, rows].astype(F32)
        same = lax.broadcasted_iota(jnp.int32, piece.shape, 0) == lax.broadcasted_iota(
            jnp.int32, piece.shape, 1
        )
        picked = jnp.where(same, piece, 0.0)
        trace += jnp.sum(jnp.sum(picked, axis=1, keepdims=True), axis=0, keepdims=True)
    factor = 1.0 / (jnp.sqrt(trace) + ORTHO_EPS)

    def load(r, unused):
        rows = pl.ds(pl.multiple_of(r * tile, tile), tile)
        first = gram_ref[rows, :].astype(F32) * factor * factor
        square[rows, :] = first
        square_low[rows, :] = first.astype(LOW)
        state[rows, :] = block_ref[rows, :].astype(F32) * factor
        out_ref[rows, :] = state[rows, :].astype(LOW)
        return unused

    lax.fori_loop(0, steps, load, 0)

    def advance():
        for r in range(steps):
            rows = slice(r * tile, (r + 1) * tile)
            state[rows, :] = 2.0 * state[rows, :] - mm(square_low[rows, :], out_ref[...])

    def settle():
        out_ref[...] = state[...].astype(LOW)

    def iterate(t, unused):
        advance()
        for r in range(steps):
            rows = slice(r * tile, (r + 1) * tile)
            value = 2.0 * square[rows, :] - mm(square_low[rows, :], square_low[...])
            cross[rows, :] = value
            cross_low[rows, :] = value.astype(LOW)
        settle()
        for r in range(steps):
            rows = slice(r * tile, (r + 1) * tile)
            square[rows, :] = 2.0 * cross[rows, :] - mm(cross_low[rows, :], square_low[...])
        square_low[...] = square[...].astype(LOW)
        return unused

    lax.fori_loop(0, NS_ITERS - 1, iterate, 0)
    advance()
    settle()


def orthogonal(gram, block):
    size, width = block.shape
    tile = min(256, size)
    return pl.pallas_call(
        functools.partial(ortho_kernel, tile),
        out_shape=jax.ShapeDtypeStruct((size, width), LOW),
        in_specs=[pl.BlockSpec(memory_space=pltpu.VMEM)] * 2,
        out_specs=pl.BlockSpec(memory_space=pltpu.VMEM),
        scratch_shapes=[
            pltpu.VMEM((size, size), F32),
            pltpu.VMEM((size, size), LOW),
            pltpu.VMEM((size, size), F32),
            pltpu.VMEM((size, size), LOW),
            pltpu.VMEM((size, width), F32),
        ],
        compiler_params=pltpu.CompilerParams(vmem_limit_bytes=40 << 20),
        cost_estimate=pl.CostEstimate(
            flops=16 * size**3 + 10 * size * size * width, bytes_accessed=4 * size * size, transcendentals=0
        ),
        name="orthogonal",
    )(gram, block)


def swap(value, axis, bit):
    return lax.ppermute(value, axis, [(i, i ^ bit) for i in range(lax.axis_size(axis))])


def pick(buffer, axis, count, stride, choice):
    size = buffer.shape[axis] // count
    run = stride * size
    parts = [
        lax.dynamic_slice_in_dim(buffer, 2 * i * run + choice * run, run, axis)
        for i in range(count // (2 * stride))
    ]
    return parts[0] if len(parts) == 1 else jnp.concatenate(parts, axis)


def reduce_blocks(buffer, axis, held):
    me = lax.axis_index("dp")
    count = 1 << len(held)

    def ladder(piece, order):
        left = list(held)
        blocks = count
        for bit in order:
            stride = 1 << (len(left) - 1 - left.index(bit))
            mine = (me // bit) % 2
            arrived = swap(pick(piece, axis, blocks, stride, 1 - mine), "dp", bit)
            kept = pick(piece, axis, blocks, stride, mine)
            piece = (kept.astype(F32) + arrived.astype(F32)).astype(LOW)
            left.remove(bit)
            blocks //= 2
        return piece

    if not held:
        return buffer
    other = 1 - axis
    half = buffer.shape[other] // 2
    ascending = sorted(held)
    orders = (ascending, ascending[1:] + ascending[:1])
    pieces = [
        ladder(lax.slice_in_dim(buffer, k * half, (k + 1) * half, axis=other), orders[k])
        for k in range(2)
    ]
    return jnp.concatenate(pieces, other)


def gradient_pair(left, right, axis):
    size = lax.axis_size("dp")
    mine = lax.axis_index("dp") % 2

    def product(choice):
        if axis == 1:
            return mm(left, pick(right, 1, size, 1, choice), TN)
        return mm(pick(left, 1, size, 1, choice), right, TN)

    arrived = swap(product(1 - mine).astype(LOW), "dp", 1)
    return (product(mine) + arrived.astype(F32)).astype(LOW)


def other_bits():
    return [1 << b for b in range(1, lax.axis_size("dp").bit_length() - 1)][::-1]


def collect(value, owner, pieces):
    size = lax.axis_size("seq")
    hops = []
    left = [(i, i - 1) for i in range(size - 1, owner, -1)]
    right = [(i, i + 1) for i in range(owner)]
    while left or right:
        hops.append(left[:1] + right[:1])
        left, right = left[1:], right[1:]
        if len(hops[-1]) == 2 and hops[-1][0][1] == hops[-1][1][1]:
            hops[-1:] = [hops[-1][:1], hops[-1][1:]]
    rows = value.shape[0] // pieces
    parts = []
    for k in range(pieces):
        part = value[k * rows : (k + 1) * rows]
        for hop in hops:
            arrived = lax.ppermute(part, "seq", hop)
            part = (part.astype(F32) + arrived.astype(F32)).astype(LOW)
        parts.append(part)
    return parts[0] if pieces == 1 else jnp.concatenate(parts, 0)


def share(own, widths):
    size = lax.axis_size("seq")
    here = lax.axis_index("seq")
    found = {0: own}
    for way in (1, -1):
        moving = own
        for distance in range(1, size):
            pairs = [
                (i, i + way) for i in range(size) if 0 <= i + way < size and 0 <= i + way - way * distance < size
            ]
            moving = lax.ppermute(moving, "seq", pairs)
            found[way * distance] = moving
    result = []
    for m, width in enumerate(widths):
        value = own[:, :width]
        for d in range(size):
            if d != m:
                value = jnp.where(here == d, found[d - m][:, :width], value)
        result.append(value)
    return result


def gram_total(gram):
    me = lax.axis_index("dp")
    size = lax.axis_size("dp")
    bits = [1 << b for b in range(size.bit_length() - 1)]

    def ladder(piece, order):
        sizes = []
        for bit in order:
            half = piece.shape[0] // 2
            mine = (me // bit) % 2
            arrived = swap(lax.dynamic_slice_in_dim(piece, (1 - mine) * half, half, 0), "dp", bit)
            kept = lax.dynamic_slice_in_dim(piece, mine * half, half, 0)
            piece = (kept.astype(F32) + arrived.astype(F32)).astype(LOW)
            sizes.append(half)
        for bit, half in zip(reversed(order), reversed(sizes)):
            mine = (me // bit) % 2
            arrived = swap(piece, "dp", bit)
            first = jnp.where(mine == 0, piece, arrived)
            second = jnp.where(mine == 0, arrived, piece)
            piece = jnp.concatenate([first, second], 0)
        return piece

    half = gram.shape[1] // 2
    low = gram.astype(LOW)
    return jnp.concatenate(
        [
            ladder(low[:, :half], bits),
            ladder(low[:, half:], bits[:1] + bits[2:] + bits[1:2]),
        ],
        1,
    )


def sum_everywhere(value):
    for axis in ("dp", "seq"):
        bit = 1
        while bit < lax.axis_size(axis):
            value = value + swap(value, axis, bit)
            bit *= 2
    return value


def depart(source, take):
    size = lax.axis_size("seq")
    here = lax.axis_index("seq")
    pieces = []
    for shift in range(size):
        piece = take(source, (here + shift) % size)
        if shift:
            piece = lax.ppermute(piece, "seq", [(i, (i + shift) % size) for i in range(size)])
        pieces.append(piece)
    return pieces


def arrange(pieces, place, shape):
    size = lax.axis_size("seq")
    here = lax.axis_index("seq")
    result = jnp.zeros(shape, LOW)
    for shift, piece in enumerate(pieces):
        result = lax.dynamic_update_slice(result, piece, place((here - shift) % size))
    return result


MESH = pl.DeviceIdType.MESH
OWNERS = 4


def greet(axes_partners):
    barrier = pltpu.get_barrier_semaphore()
    count = 0
    for axis, partner, real in axes_partners:

        def tell(axis=axis, partner=partner):
            pl.semaphore_signal(barrier, inc=1, device_id={axis: partner}, device_id_type=MESH)

        if real is None:
            tell()
            count = count + 1
        else:
            pl.when(real)(tell)
            count = count + real.astype(jnp.int32)
    pl.semaphore_wait(barrier, count)


def plane():
    me = lax.axis_index("dp")
    core, x, y = lax.rem(me, 2), lax.rem(me // 2, 2), me // 4
    flip = lambda bit: 1 - bit
    return (
        (core, x, y),
        (
            4 * y + 2 * x + flip(core),
            4 * y + 2 * flip(x) + core,
            4 * flip(y) + 2 * x + core,
        ),
    )


def combine_kernel(
    ways, wide_q, wide_p, qkv_ref, proj_ref, up_ref, down_ref, out_ref,
    one, send_two, two, send_three, three, final, from_left, from_right, relay,
    s_one, r_one, s_two, r_two, s_three, r_three, s_left, r_left, s_right, r_right,
):
    (core, x, y), partners = plane()
    z = lax.axis_index("seq")
    size = up_ref.shape[0]
    half = size // 2
    chunks = 4
    step = size // chunks
    width = wide_q + wide_p
    greet(
        [("dp", p, None) for p in partners]
        + [("seq", jnp.maximum(z - 1, 0), z > 0), ("seq", jnp.minimum(z + 1, ways - 1), z < ways - 1)]
    )

    def remote(src, dst, send, recv, axis, target):
        return pltpu.make_async_remote_copy(
            src_ref=src, dst_ref=dst, send_sem=send, recv_sem=recv,
            device_id={axis: target}, device_id_type=MESH,
        )

    owned = ((0, width), (0, wide_q), (wide_q, wide_p), (0, width))

    def source(m, k):
        rows = pl.ds(k * step, step)
        lanes = pl.ds(*owned[m])
        return (up_ref, final, final, down_ref)[m].at[rows, lanes]

    def hop(m, k, left, src):
        lanes = pl.ds(*owned[m])
        box, send, recv = (from_right, s_left, r_left) if left else (from_left, s_right, r_right)
        slot = m
        return remote(
            src, box.at[slot, pl.ds(k * step, step), lanes], send.at[m, k], recv.at[m, k],
            "seq", jnp.maximum(z - 1, 0) if left else jnp.minimum(z + 1, ways - 1),
        )

    def relay_src(m, k):
        return relay.at[m, pl.ds(k * step, step), pl.ds(*owned[m])]

    def begin(m):
        for k in range(chunks):
            if m < ways - 1:
                @pl.when(z == ways - 1)
                def _():
                    hop(m, k, True, source(m, k)).start()
            if m > 0:
                @pl.when(z == 0)
                def _():
                    hop(m, k, False, source(m, k)).start()

    def pass_on(m, k):
        rows = pl.ds(k * step, step)
        lanes = pl.ds(*owned[m])
        strip = 64

        def added(box):
            def body(i, unused):
                part = pl.ds(pl.multiple_of(k * step + i * strip, strip), strip)
                src = (up_ref, final, final, down_ref)[m]
                relay[m, part, lanes] = (
                    src[part, lanes].astype(F32) + box[m, part, lanes].astype(F32)
                ).astype(LOW)
                return unused

            lax.fori_loop(0, step // strip, body, 0)

        if m < ways - 2:
            @pl.when((z > m) & (z < ways - 1))
            def _():
                hop(m, k, True, source(m, k)).wait_recv()
                added(from_right)
                hop(m, k, True, relay_src(m, k)).start()
        if m > 1:
            @pl.when((z < m) & (z > 0))
            def _():
                hop(m, k, False, source(m, k)).wait_recv()
                added(from_left)
                hop(m, k, False, relay_src(m, k)).start()

    def settle(m, k):
        lanes = pl.ds(*owned[m])
        strip = 64

        @pl.when(z == m)
        def _():
            if m < ways - 1:
                hop(m, k, True, source(m, k)).wait_recv()
            if m > 0:
                hop(m, k, False, source(m, k)).wait_recv()

            def body(i, unused):
                part = pl.ds(pl.multiple_of(k * step + i * strip, strip), strip)
                src = (up_ref, final, final, down_ref)[m]
                total = src[part, lanes].astype(F32)
                if m < ways - 1:
                    total += from_right[m, part, lanes].astype(F32)
                if m > 0:
                    total += from_left[m, part, lanes].astype(F32)
                width_m = owned[m][1]
                out_ref[part, pl.ds(0, width_m)] = total.astype(LOW)
                if width_m < width:
                    out_ref[part, pl.ds(width_m, width - width_m)] = jnp.zeros(
                        (strip, width - width_m), LOW
                    )
                return unused

            lax.fori_loop(0, step // strip, body, 0)

    begin(0)
    begin(3)

    strip = 64

    def own(h, block, start, rows):
        part = pl.ds(pl.multiple_of(h * half + start, strip), rows)
        q = qkv_ref[part, pl.ds(pl.multiple_of(block * wide_q, 128), wide_q)]
        p = proj_ref[part, pl.ds(pl.multiple_of(block * wide_p, 128), wide_p)]
        return jnp.concatenate([q, p], axis=1).astype(F32)

    def first(h, k):
        block = 2 * k + (1 - core)
        rows = pl.ds(h * half, half)
        return [
            remote(
                qkv_ref.at[rows, pl.ds(pl.multiple_of(block * wide_q, 128), wide_q)],
                one.at[h, k, :, pl.ds(0, wide_q)], s_one.at[h, k, 0], r_one.at[h, k, 0],
                "dp", partners[0],
            ),
            remote(
                proj_ref.at[rows, pl.ds(pl.multiple_of(block * wide_p, 128), wide_p)],
                one.at[h, k, :, pl.ds(wide_q, wide_p)], s_one.at[h, k, 1], r_one.at[h, k, 1],
                "dp", partners[0],
            ),
        ]

    go = [[(2 * j + (1 - x)) for j in range(2)], [(2 * (1 - y) + j) for j in range(2)]]
    stay = [[(2 * j + x) for j in range(2)], [(2 * y + j) for j in range(2)]]
    for group in (go, stay):
        for j in range(2):
            for h in range(2):
                for copy in first(h, group[h][j]):
                    copy.start()

    def second(h, j):
        return remote(send_two.at[h, j], two.at[h, j], s_two.at[h, j], r_two.at[h, j],
                      "dp", partners[1 + h])

    for j in range(2):
        for h in range(2):
            k = go[h][j]
            for copy in first(h, k):
                copy.wait_recv()

            def body(i, unused):
                part = pl.ds(pl.multiple_of(i * strip, strip), strip)
                value = own(h, 2 * k + core, i * strip, strip) + one[h, k, part, :].astype(F32)
                send_two[h, j, part, :] = value.astype(LOW)
                return unused

            lax.fori_loop(0, half // strip, body, 0)
            second(h, j).start()
    for k in range(chunks):
        pass_on(0, k)
        pass_on(3, k)

    def third(h):
        return remote(send_three.at[h], three.at[h], s_three.at[h], r_three.at[h],
                      "dp", partners[2 - h])

    mine = [y, x]
    for h in range(2):
        for j in range(2):
            for copy in first(h, stay[h][j]):
                copy.wait_recv()
        for j in range(2):
            second(h, j).wait_recv()
        j = 1 - mine[h]
        k = 2 * j + x if h == 0 else 2 * y + j

        def body(i, unused):
            part = pl.ds(pl.multiple_of(i * strip, strip), strip)
            value = (
                own(h, 2 * k + core, i * strip, strip)
                + one[h, k, part, :].astype(F32)
                + two[h, j, part, :].astype(F32)
            )
            send_three[h, part, :] = value.astype(LOW)
            return unused

        lax.fori_loop(0, half // strip, body, 0)
        third(h).start()
    for h in range(2):
        third(h).wait_recv()
        j = mine[h]
        k = 2 * y + x

        def body(i, unused):
            part = pl.ds(pl.multiple_of(i * strip, strip), strip)
            value = (
                own(h, 2 * k + core, i * strip, strip)
                + one[h, k, part, :].astype(F32)
                + two[h, j, part, :].astype(F32)
                + three[h, part, :].astype(F32)
            )
            final[pl.ds(pl.multiple_of(h * half + i * strip, strip), strip), :] = value.astype(LOW)
            return unused

        lax.fori_loop(0, half // strip, body, 0)
    begin(1)
    begin(2)
    for k in range(chunks):
        pass_on(1, k)
        pass_on(2, k)
    for m in (0, 3, 1, 2):
        for k in range(chunks):
            settle(m, k)

    for h in range(2):
        for k in range(4):
            for copy in first(h, k):
                copy.wait_send()
        for j in range(2):
            second(h, j).wait_send()
        third(h).wait_send()
    for m in range(OWNERS):
        for k in range(chunks):
            if m < ways - 1:
                @pl.when(z > m)
                def _():
                    hop(m, k, True, source(m, k)).wait_send()
            if m > 0:
                @pl.when(z < m)
                def _():
                    hop(m, k, False, source(m, k)).wait_send()


def combine(ways, qkv, proj, up, down):
    size, width = up.shape
    wide_q, wide_p = qkv.shape[1] // 8, proj.shape[1] // 8
    half = size // 2
    vmem = pl.BlockSpec(memory_space=pltpu.VMEM)
    dma = pltpu.SemaphoreType.DMA
    return pl.pallas_call(
        functools.partial(combine_kernel, ways, wide_q, wide_p),
        out_shape=jax.ShapeDtypeStruct((size, width), LOW),
        in_specs=[vmem] * 4,
        out_specs=vmem,
        scratch_shapes=[
            pltpu.VMEM((2, 4, half, width), LOW),
            pltpu.VMEM((2, 2, half, width), LOW),
            pltpu.VMEM((2, 2, half, width), LOW),
            pltpu.VMEM((2, half, width), LOW),
            pltpu.VMEM((2, half, width), LOW),
            pltpu.VMEM((size, width), LOW),
            pltpu.VMEM((OWNERS, size, width), LOW),
            pltpu.VMEM((OWNERS, size, width), LOW),
            pltpu.VMEM((OWNERS, size, width), LOW),
            dma((2, 4, 2)), dma((2, 4, 2)), dma((2, 2)), dma((2, 2)), dma((2,)), dma((2,)),
            dma((OWNERS, 4)), dma((OWNERS, 4)), dma((OWNERS, 4)), dma((OWNERS, 4)),
        ],
        compiler_params=pltpu.CompilerParams(
            collective_id=1, has_side_effects=True, vmem_limit_bytes=56 << 20
        ),
        cost_estimate=pl.CostEstimate(flops=50_000_000_000, bytes_accessed=1 << 23, transcendentals=0),
        name="combine",
    )(qkv, proj, up, down)


def finish_kernel(
    ways, widths, chunks, gram_ref, block_ref, grad_ref, vector_ref,
    g0, g1, g2, g3, y0, y1, y2, y3, total_ref,
    one, send_two, two, send_three, three, whole,
    square, square_low, cross, cross_low, state, low, g_down, y_down, vectors, arrived,
    s_one, r_one, s_two, r_two, s_three, r_three, s_back, r_back,
    gs_left, gr_left, gs_right, gr_right, ys_left, yr_left, ys_right, yr_right, s_own, s_vec, r_vec,
):
    (core, x, y), partners = plane()
    z = lax.axis_index("seq")
    across = lax.rem(z + 2, 4)
    beside = z + 1 - 2 * lax.rem(z, 2)
    size = gram_ref.shape[0]
    rows = size // 8
    half = size // 2
    step = size // chunks
    greet(
        [("dp", p, None) for p in partners]
        + [
            ("seq", across, None),
            ("seq", jnp.maximum(z - 1, 0), z > 0),
            ("seq", jnp.minimum(z + 1, ways - 1), z < ways - 1),
        ]
    )

    class Trip:
        def __init__(self, own, outs, s_left, r_left, s_right, r_right, local):
            self.own, self.outs, self.local = own, outs, local
            self.left, self.right = (s_left, r_left), (s_right, r_right)

        def hop(self, m, k, left, relayed):
            part = pl.ds(pl.multiple_of(k * step, step), step)
            place = self.outs[m].at[part, :]
            src = place if relayed else self.own.at[part, pl.ds(0, widths[m])]
            send, recv = self.left if left else self.right
            return pltpu.make_async_remote_copy(
                src_ref=src, dst_ref=place, send_sem=send.at[m, k], recv_sem=recv.at[m, k],
                device_id={"seq": jnp.maximum(z - 1, 0) if left else jnp.minimum(z + 1, ways - 1)},
                device_id_type=MESH,
            )

        def copy(self, m):
            return pltpu.make_async_copy(
                self.own.at[:, pl.ds(0, widths[m])], self.outs[m], s_own.at[self.local]
            )

        def begin(self):
            for m in range(OWNERS):
                @pl.when(z == m)
                def _():
                    for k in range(chunks):
                        if m < ways - 1:
                            self.hop(m, k, False, False).start()
                        if m > 0:
                            self.hop(m, k, True, False).start()
                    self.copy(m).start()

        def relay(self, distance, k):
            for m in range(OWNERS):
                if m + distance < ways:
                    @pl.when(z == m + distance)
                    def _():
                        self.hop(m, k, False, True).wait_recv()
                        if m + distance < ways - 1:
                            self.hop(m, k, False, True).start()
                if m - distance >= 0:
                    @pl.when(z == m - distance)
                    def _():
                        self.hop(m, k, True, True).wait_recv()
                        if m - distance > 0:
                            self.hop(m, k, True, True).start()

        def end(self):
            for m in range(OWNERS):
                @pl.when(z == m)
                def _():
                    self.copy(m).wait()

                for k in range(chunks):
                    @pl.when((z >= m) & (z < ways - 1))
                    def _():
                        self.hop(m, k, False, True).wait_send()

                    @pl.when((z <= m) & (z > 0))
                    def _():
                        self.hop(m, k, True, True).wait_send()

    grads = Trip(grad_ref, (g0, g1, g2, g_down), gs_left, gr_left, gs_right, gr_right, 0)
    steps = Trip(low, (y0, y1, y2, y_down), ys_left, yr_left, ys_right, yr_right, 1)
    grads.begin()

    def vector_copy(i):
        source = vector_ref if i == 0 else vectors.at[i - 1]
        target = (
            [{"dp": p} for p in partners] + [{"seq": beside}, {"seq": across}]
        )[i]
        return pltpu.make_async_remote_copy(
            src_ref=source, dst_ref=arrived.at[i], send_sem=s_vec.at[i], recv_sem=r_vec.at[i],
            device_id=target, device_id_type=MESH,
        )

    def vector_step(i):
        vector_copy(i).wait_recv()
        value = (vector_ref[...] if i == 0 else vectors[i - 1]) + arrived[i]
        if i < 4:
            vectors[i] = value
            vector_copy(i + 1).start()
        else:
            total_ref[...] = value

    vector_copy(0).start()

    def remote(src, dst, send, recv, target):
        return pltpu.make_async_remote_copy(
            src_ref=src, dst_ref=dst, send_sem=send, recv_sem=recv,
            device_id={"dp": target}, device_id_type=MESH,
        )

    def block(ref, h, d):
        return ref.at[pl.ds(pl.multiple_of(d * rows, rows), rows), pl.ds(h * half, half)]

    def own(h, d):
        return gram_ref[
            pl.ds(pl.multiple_of(d * rows, rows), rows), pl.ds(h * half, half)
        ].astype(F32)

    def first(h, k):
        return remote(block(gram_ref, h, 2 * k + 1 - core), one.at[h, k], s_one.at[h, k],
                      r_one.at[h, k], partners[0])

    go = [[(2 * j + (1 - x)) for j in range(2)], [(2 * (1 - y) + j) for j in range(2)]]
    stay = [[(2 * j + x) for j in range(2)], [(2 * y + j) for j in range(2)]]
    for group in (go, stay):
        for j in range(2):
            for h in range(2):
                first(h, group[h][j]).start()

    def second(h, j):
        return remote(send_two.at[h, j], two.at[h, j], s_two.at[h, j], r_two.at[h, j], partners[1 + h])

    for j in range(2):
        for h in range(2):
            k = go[h][j]
            first(h, k).wait_recv()
            send_two[h, j] = (own(h, 2 * k + core) + one[h, k].astype(F32)).astype(LOW)
            second(h, j).start()
    vector_step(0)

    def third(h):
        return remote(send_three.at[h], three.at[h], s_three.at[h], r_three.at[h], partners[2 - h])

    mine = [y, x]
    for h in range(2):
        for j in range(2):
            first(h, stay[h][j]).wait_recv()
        for j in range(2):
            second(h, j).wait_recv()
        j = 1 - mine[h]
        k = 2 * j + x if h == 0 else 2 * y + j
        send_three[h] = (
            own(h, 2 * k + core) + one[h, k].astype(F32) + two[h, j].astype(F32)
        ).astype(LOW)
        third(h).start()
    vector_step(1)
    for c in range(chunks // 4):
        grads.relay(1, c)

    def back(h, stage, d):
        target = (partners[2 - h], partners[1 + h], partners[0])[stage]
        place = block(whole, h, d)
        slot = (0, 1, 3)[stage]
        return lambda i: remote(place, place, s_back.at[h, slot + i], r_back.at[h, slot + i], target)

    k = 2 * y + x
    for h in range(2):
        third(h).wait_recv()
        value = (
            own(h, 2 * k + core)
            + one[h, k].astype(F32)
            + two[h, mine[h]].astype(F32)
            + three[h].astype(F32)
        ).astype(LOW)
        d = 2 * k + core
        whole[pl.ds(pl.multiple_of(d * rows, rows), rows), pl.ds(h * half, half)] = value
        for stage in range(3):
            back(h, stage, d)(0).start()
    vector_step(2)
    k_next = [2 * (1 - y) + x, 2 * y + (1 - x)]
    for h in range(2):
        d = 2 * k_next[h] + core
        back(h, 0, d)(0).wait_recv()
        back(h, 1, d)(1).start()
        back(h, 2, d)(1).start()
    for c in range(chunks // 4, chunks // 2):
        grads.relay(1, c)
    for h in range(2):
        for i in range(2):
            if h == 0:
                kk = 2 * (y if i == 0 else 1 - y) + (1 - x)
            else:
                kk = 2 * (1 - y) + (x if i == 0 else 1 - x)
            d = 2 * kk + core
            back(h, 1, d)(i).wait_recv()
            back(h, 2, d)(2 + i).start()
    for h in range(2):
        for i, kk in enumerate(
            (
                2 * y + x,
                k_next[h],
                2 * y + (1 - x) if h == 0 else 2 * (1 - y) + x,
                2 * (1 - y) + (1 - x),
            )
        ):
            back(h, 2, 2 * kk + 1 - core)(i).wait_recv()
    vector_step(3)
    for c in range(chunks // 2, chunks):
        grads.relay(1, c)

    tile = 256
    count = size // tile
    trace = jnp.zeros((1, 1), F32)
    for r in range(count):
        part = slice(r * tile, (r + 1) * tile)
        piece = whole[part, part].astype(F32)
        same = lax.broadcasted_iota(jnp.int32, piece.shape, 0) == lax.broadcasted_iota(
            jnp.int32, piece.shape, 1
        )
        picked = jnp.where(same, piece, 0.0)
        trace += jnp.sum(jnp.sum(picked, axis=1, keepdims=True), axis=0, keepdims=True)
    factor = 1.0 / (jnp.sqrt(trace) + ORTHO_EPS)

    def load(r, unused):
        part = pl.ds(pl.multiple_of(r * tile, tile), tile)
        begun = whole[part, :].astype(F32) * factor * factor
        square[part, :] = begun
        square_low[part, :] = begun.astype(LOW)
        state[part, :] = block_ref[part, :].astype(F32) * factor
        low[part, :] = state[part, :].astype(LOW)
        return unused

    lax.fori_loop(0, count, load, 0)

    def advance():
        for r in range(count):
            part = slice(r * tile, (r + 1) * tile)
            state[part, :] = 2.0 * state[part, :] - mm(square_low[part, :], low[...])

    def iterate(t, unused):
        advance()
        for r in range(count):
            part = slice(r * tile, (r + 1) * tile)
            value = 2.0 * square[part, :] - mm(square_low[part, :], square_low[...])
            cross[part, :] = value
            cross_low[part, :] = value.astype(LOW)
        low[...] = state[...].astype(LOW)
        for r in range(count):
            part = slice(r * tile, (r + 1) * tile)
            square[part, :] = 2.0 * cross[part, :] - mm(cross_low[part, :], square_low[...])
        square_low[...] = square[...].astype(LOW)
        for c in range(chunks // 4):
            grads.relay(2, t * (chunks // 4) + c)
        return unused

    lax.fori_loop(0, NS_ITERS - 1, iterate, 0)
    advance()
    low[...] = state[...].astype(LOW)

    steps.begin()
    vector_step(4)
    for c in range(chunks):
        grads.relay(3, c)
    grads.end()

    def turn(ref, out):
        for c in range(size // 256):
            out[:, c * 256 : (c + 1) * 256] = ref[c * 256 : (c + 1) * 256, :].T

    for distance in range(1, ways):
        for c in range(chunks):
            steps.relay(distance, c)
        if distance == 1:
            turn(g_down, g3)
    steps.end()
    turn(y_down, y3)

    for h in range(2):
        for j in range(4):
            first(h, j).wait_send()
        for j in range(2):
            second(h, j).wait_send()
        third(h).wait_send()
        d = 2 * k + core
        back(h, 0, d)(0).wait_send()
        for i in range(2):
            back(h, 1, d)(i).wait_send()
        for i in range(4):
            back(h, 2, d)(i).wait_send()
    for i in range(5):
        vector_copy(i).wait_send()


def finish(ways, gram, block, grad, vectors, widths):
    size, width = block.shape
    rows, half = size // 8, size // 2
    chunks = 8
    vmem = pl.BlockSpec(memory_space=pltpu.VMEM)
    dma = pltpu.SemaphoreType.DMA
    shapes = [
        jax.ShapeDtypeStruct((size, w) if m < OWNERS - 1 else (w, size), LOW)
        for m, w in enumerate(widths)
    ]
    down = pltpu.VMEM((size, widths[-1]), LOW)
    result = pl.pallas_call(
        functools.partial(finish_kernel, ways, widths, chunks),
        out_shape=shapes * 2 + [jax.ShapeDtypeStruct(vectors.shape, F32)],
        in_specs=[vmem] * 4,
        out_specs=[vmem] * 9,
        scratch_shapes=[
            pltpu.VMEM((2, 4, rows, half), LOW),
            pltpu.VMEM((2, 2, rows, half), LOW),
            pltpu.VMEM((2, 2, rows, half), LOW),
            pltpu.VMEM((2, rows, half), LOW),
            pltpu.VMEM((2, rows, half), LOW),
            pltpu.VMEM((size, size), LOW),
            pltpu.VMEM((size, size), F32),
            pltpu.VMEM((size, size), LOW),
            pltpu.VMEM((size, size), F32),
            pltpu.VMEM((size, size), LOW),
            pltpu.VMEM((size, width), F32),
            pltpu.VMEM((size, width), LOW),
            down,
            down,
            pltpu.VMEM((4,) + vectors.shape, F32),
            pltpu.VMEM((5,) + vectors.shape, F32),
            dma((2, 4)), dma((2, 4)), dma((2, 2)), dma((2, 2)), dma((2,)), dma((2,)),
            dma((2, 7)), dma((2, 7)),
        ]
        + [dma((OWNERS, chunks))] * 8
        + [dma((2,)), dma((5,)), dma((5,))],
        compiler_params=pltpu.CompilerParams(
            collective_id=2, has_side_effects=True, vmem_limit_bytes=56 << 20
        ),
        cost_estimate=pl.CostEstimate(
            flops=80_000_000_000, bytes_accessed=1 << 24, transcendentals=0
        ),
        name="finish",
    )(gram, block, grad, vectors)
    return result[:4], result[4:8], result[8]


def norm_forward(values, gain_row, offset):
    center = values - jnp.mean(values, axis=-1, keepdims=True)
    inv_scale = lax.rsqrt(jnp.mean(center * center, axis=-1, keepdims=True) + NORM_EPS)
    unit_values = center * inv_scale
    return (unit_values * gain_row + offset, unit_values, inv_scale)


def norm_backward(upstream, unit_values, inv_scale, gain_row):
    scaled = upstream * gain_row
    inner_sum = jnp.mean(scaled * unit_values, axis=-1, keepdims=True)
    input_grad = inv_scale * (
        scaled - jnp.mean(scaled, axis=-1, keepdims=True) - unit_values * inner_sum
    )
    return (input_grad, jnp.sum(upstream * unit_values, axis=0), jnp.sum(upstream, axis=0))


def gelu_both(values):
    square = values * values
    tangent = jnp.tanh(GELU_C * (values + 0.044715 * square * values))
    slope = 0.5 * (1.0 + tangent) + 0.5 * values * (1.0 - tangent * tangent) * GELU_C * (
        1.0 + 3.0 * 0.044715 * square
    )
    return 0.5 * values * (1.0 + tangent), slope


def on_device(
    tokens,
    cotangent,
    qkv_weight,
    proj_weight,
    up_weight,
    down_weight,
    norm_gains,
    biases,
    up_bias,
    head_slopes,
    qkv_moment,
    proj_moment,
    up_moment,
    down_moment,
    gains_moment,
    biases_moment,
    upbias_moment,
):
    rows, width = tokens.shape
    ways = lax.axis_size("seq")
    here = lax.axis_index("seq")
    me = lax.axis_index("dp")
    length = rows * ways
    own_width = width // ways
    chunks = 2
    chunk = own_width // chunks
    chunk_heads = chunk // HEAD
    own_slopes = lax.dynamic_slice_in_dim(
        head_slopes, here * (own_width // HEAD), own_width // HEAD, 0
    )
    slope_rows = [
        jnp.repeat(own_slopes[c * chunk_heads : (c + 1) * chunk_heads], BLOCK)[None]
        for c in range(chunks)
    ]

    inputs = tokens.astype(F32)
    normed_one, unit_one, scale_one = norm_forward(inputs, norm_gains[0], biases[0])
    normed_one = normed_one.astype(LOW)
    bias_row = jnp.concatenate([biases[1], jnp.zeros_like(biases[1]), biases[2]])
    mixed = (mm(normed_one, qkv_weight) + bias_row).astype(LOW)

    def take_mixed(c):
        def take(source, d):
            return jnp.stack(
                [
                    lax.dynamic_slice_in_dim(
                        source, part * width + d * own_width + c * chunk, chunk, 1
                    )
                    for part in range(3)
                ]
            )

        return take

    qkv_pieces = [depart(mixed, take_mixed(c)) for c in range(chunks)]
    qkv = []
    attended = jnp.zeros((rows, width), LOW)
    kept = []
    for c in range(chunks):
        if c:
            qkv_pieces[c], out = lax.optimization_barrier((qkv_pieces[c], out))
        qkv.append(arrange(qkv_pieces[c], lambda d: (0, d * rows, 0), (3, length, chunk)))
        out, wide, log_totals = attend_forward(qkv[c], slope_rows[c], BLOCK)
        kept.append((wide, log_totals))
        for shift in range(ways):
            piece = lax.dynamic_slice_in_dim(out, ((here + shift) % ways) * rows, rows, 0)
            if shift:
                piece = lax.ppermute(piece, "seq", [(i, (i + shift) % ways) for i in range(ways)])
            attended = lax.dynamic_update_slice(
                attended, piece, (0, ((here - shift) % ways) * own_width + c * chunk)
            )

    middle = inputs + mm(attended, proj_weight) + biases[3]
    normed_two, unit_two, scale_two = norm_forward(middle, norm_gains[1], biases[4])
    normed_two = normed_two.astype(LOW)
    before = mm(normed_two, up_weight) + up_bias
    hidden, slope = gelu_both(before)
    hidden = hidden.astype(LOW)
    block_out = (middle + mm(hidden, down_weight) + biases[5]).astype(LOW)
    upstream = cotangent.astype(F32)
    hidden_grad = mm(cotangent, down_weight, NT)
    before_grad = (hidden_grad * slope).astype(LOW)
    normed_two_grad = mm(before_grad, up_weight, NT)
    middle_back, gain_two_grad, offset_two_grad = norm_backward(
        normed_two_grad, unit_two, scale_two, norm_gains[1]
    )
    middle_grad = upstream + middle_back
    branch_grad = middle_grad.astype(LOW)
    heads_grad = mm(branch_grad, proj_weight, NT).astype(LOW)

    grad_pieces = [
        depart(
            heads_grad,
            lambda source, d: lax.dynamic_slice_in_dim(source, d * own_width + c * chunk, chunk, 1),
        )
        for c in range(chunks)
    ]
    down_pair = gradient_pair(cotangent, hidden, 1)
    up_pair = gradient_pair(normed_two, before_grad, 1)
    grad_pieces[0], down_pair, up_pair = lax.optimization_barrier(
        (grad_pieces[0], down_pair, up_pair)
    )

    mixed_pieces = []
    for c in range(chunks):
        if c:
            grad_pieces[c], back = lax.optimization_barrier((grad_pieces[c], back))
        grad = arrange(grad_pieces[c], lambda d: (d * rows, 0), (length, chunk))
        back = attend_backward(qkv[c], grad, *kept[c], slope_rows[c], BLOCK)
        mixed_pieces.append(
            depart(back, lambda source, d: lax.dynamic_slice_in_dim(source, d * rows, rows, 1))
        )
    down_part = reduce_blocks(down_pair, 1, other_bits())
    up_part = reduce_blocks(up_pair, 1, other_bits())
    mixed_pieces[-1], down_part, up_part = lax.optimization_barrier(
        (mixed_pieces[-1], down_part, up_part)
    )
    mixed_grad = jnp.zeros((3, rows, width), LOW)
    for c in range(chunks):
        for shift, piece in enumerate(mixed_pieces[c]):
            mixed_grad = lax.dynamic_update_slice(
                mixed_grad, piece, (0, 0, ((here - shift) % ways) * own_width + c * chunk)
            )
    mixed_flat = jnp.concatenate([mixed_grad[0], mixed_grad[1], mixed_grad[2]], 1)

    widths = tuple(
        moment.shape[1] for moment in (up_moment, qkv_moment, proj_moment, down_moment.T)
    )
    quick = lax.axis_size("dp") == 8 and ways == OWNERS and all(w % 128 == 0 for w in widths)
    up_owner, qkv_owner, proj_owner, down_owner = range(OWNERS)
    pad_width = max(widths)

    def owned_of(members):
        padded = [jnp.pad(m, ((0, 0), (0, pad_width - m.shape[1]))) for m in members]
        return jnp.where(
            here < 2,
            jnp.where(here == 0, padded[0], padded[1]),
            jnp.where(here == 2, padded[2], padded[3]),
        )

    if quick:
        owned_grad = combine(
            ways,
            mm(normed_one, mixed_flat, TN).astype(LOW),
            mm(attended, branch_grad, TN).astype(LOW),
            up_part,
            down_part,
        )
    else:
        proj_part = reduce_blocks(gradient_pair(attended, branch_grad, 1), 1, other_bits())
        qkv_part = reduce_blocks(gradient_pair(normed_one, mixed_flat, 1), 1, other_bits())
        owned_grad = owned_of(
            [
                collect(up_part, up_owner, 2),
                collect(qkv_part, qkv_owner, 1),
                collect(proj_part, proj_owner, 1),
                collect(down_part, down_owner, 2),
            ]
        )

    normed_one_grad = mm(mixed_flat, qkv_weight, NT)
    input_back, gain_one_grad, offset_one_grad = norm_backward(
        normed_one_grad, unit_one, scale_one, norm_gains[0]
    )
    tokens_grad = middle_grad + input_back

    def columns(value):
        return jnp.sum(value.astype(F32), axis=0)

    vectors = jnp.stack(
        [
            gain_one_grad,
            gain_two_grad,
            offset_one_grad,
            columns(mixed_grad[0]),
            columns(mixed_grad[2]),
            columns(branch_grad),
            offset_two_grad,
            columns(upstream),
        ]
    )
    vectors = jnp.concatenate([vectors, columns(before_grad).reshape(-1, width)], 0)

    owned_moment = owned_of([up_moment, qkv_moment, proj_moment, down_moment.T])
    owned_block = (MOMENTUM * owned_moment + owned_grad.astype(F32)).astype(LOW)
    gram = mm(owned_block, owned_block, NT)
    if quick:
        sums, steps, vectors = finish(ways, gram.astype(LOW), owned_block, owned_grad, vectors, widths)
    else:
        vectors = sum_everywhere(vectors)
        iterate = orthogonal(gram_total(gram), owned_block)
        sums = share(owned_grad, widths)
        steps = share(iterate, widths)
        sums[3], steps[3] = sums[3].T, steps[3].T

    def own_columns(matrix, count):
        return lax.dynamic_slice_in_dim(matrix, me * count, count, 1).astype(F32)

    gains_sum = own_columns(vectors[:2], gains_moment.shape[1])
    biases_sum = own_columns(vectors[2:8], biases_moment.shape[1])
    upbias_count = upbias_moment.shape[0]
    upbias_sum = lax.dynamic_slice_in_dim(
        vectors[8:].reshape(-1), me * upbias_count, upbias_count, 0
    )

    def state_of(moment, grad):
        return MOMENTUM * moment + grad.astype(F32)

    up_sum, qkv_sum, proj_sum, down_sum = [g.astype(F32) for g in sums]
    qkv_state = state_of(qkv_moment, qkv_sum)
    proj_state = state_of(proj_moment, proj_sum)
    up_state = state_of(up_moment, up_sum)
    down_state = state_of(down_moment, down_sum)
    gains_state = state_of(gains_moment, gains_sum)
    biases_state = state_of(biases_moment, biases_sum)
    upbias_state = state_of(upbias_moment, upbias_sum)

    def rate_of(shape):
        return -RATE_MATRIX * math.sqrt(max(shape))

    def step_of(owner, shape):
        return rate_of(shape) * steps[owner].astype(F32)

    qkv_new = own_columns(qkv_weight, qkv_state.shape[1]) + step_of(
        qkv_owner, qkv_weight.shape
    )
    proj_new = own_columns(proj_weight, proj_state.shape[1]) + step_of(
        proj_owner, proj_weight.shape
    )
    up_new = own_columns(up_weight, up_state.shape[1]) + step_of(
        up_owner, up_weight.shape
    )
    down_count = down_state.shape[0]
    down_rows = lax.dynamic_slice_in_dim(down_weight, me * down_count, down_count, 0).astype(F32)
    down_new = down_rows + step_of(down_owner, down_weight.shape)
    gains_new = own_columns(norm_gains, gains_state.shape[1]) - RATE_VECTOR * gains_state
    biases_new = own_columns(biases, biases_state.shape[1]) - RATE_VECTOR * biases_state
    upbias_new = (
        lax.dynamic_slice_in_dim(up_bias, me * upbias_count, upbias_count, 0)
        - RATE_VECTOR * upbias_state
    )
    return (
        block_out,
        tokens_grad,
        qkv_sum,
        proj_sum,
        up_sum,
        down_sum,
        gains_sum,
        biases_sum,
        upbias_sum,
        qkv_state,
        proj_state,
        up_state,
        down_state,
        gains_state,
        biases_state,
        upbias_state,
        qkv_new,
        proj_new,
        up_new,
        down_new,
        gains_new,
        biases_new,
        upbias_new,
    )


def solution(mesh):
    rows, columns, copied = P(("dp", "seq"), None), P(None, "dp"), P()

    return jax.shard_map(
        on_device,
        mesh=mesh,
        in_specs=(
            (rows, rows)
            + (copied,) * 8
            + (columns, columns, columns, P("dp", None), columns, columns, P("dp"))
        ),
        out_specs=(
            (rows, rows)
            + (columns, columns, columns, P("dp", None), columns, columns, P("dp")) * 3
        ),
        check_vma=False,
    )
```

```python
import functools
import math

import jax
import jax.numpy as jnp
from jax import lax
from jax.experimental import pallas as pl
from jax.experimental.pallas import tpu as pltpu
from jax.sharding import PartitionSpec as P


NS_ITERS = 5


MOMENTUM = 0.9
RATE_MATRIX = 0.2
RATE_VECTOR = 0.0015
NORM_EPS = 1e-05
ORTHO_EPS = 1e-07
GELU_C = 0.7978845608028654
MASKED = -1e30
HEAD = 64
BLOCK = 512
LOW = jnp.bfloat16
F32 = jnp.float32

NT = (((1,), (1,)), ((), ()))
NN = (((1,), (0,)), ((), ()))
TN = (((0,), (0,)), ((), ()))


def mm(left, right, dims=NN):
    return lax.dot_general(left, right, dims, preferred_element_type=F32)


def stack_heads(block, groups, scale=None):
    lane = lax.broadcasted_iota(jnp.int32, block.shape, 1)
    if scale is not None:
        block = block * scale
    zero = jnp.zeros_like(block)
    return [
        jnp.where((lane >= h * HEAD) & (lane < (h + 1) * HEAD), block, zero)
        for h in range(groups)
    ]


def bias_tiles(slope_row, block, plain_ref, edge_ref, groups):
    shape = plain_ref.shape
    row = lax.broadcasted_iota(jnp.int32, shape, 0)
    col = lax.broadcasted_iota(jnp.int32, (shape[0], block), 1)
    tile = row.astype(F32) * slope_row
    plain_ref[...] = tile
    for h in range(groups):
        part = slice(h * block, (h + 1) * block)
        edge_ref[:, part] = jnp.where(row[:, part] <= col, tile[:, part], MASKED)


def forward_kernel(
    groups, block, inner, slope_ref, q_ref, k_ref, v_ref, out_ref, wide_ref, log_ref,
    plain, edge, vt, qs, acc, scores
):
    i = pl.program_id(0)
    slope = slope_ref[...]

    @pl.when(i == 0)
    def _():
        bias_tiles(slope, block, plain, edge, groups)
        vt[...] = v_ref[0].T

    for h, part in enumerate(stack_heads(q_ref[0], groups, LOW(1.0 / math.sqrt(HEAD)))):
        qs[h * block : (h + 1) * block, :] = part
    acc[...] = jnp.zeros_like(acc)
    wide = groups * block

    def score(j, peak, tile_ref):
        keys = k_ref[0, pl.ds(pl.multiple_of(j * block, block), block), :]
        x = mm(keys, qs[...], NT) + tile_ref[...] + slope * (j * block).astype(F32)
        scores[j] = x
        return jnp.maximum(peak, jnp.max(x.reshape(block // 8, 8, wide), axis=0))

    peak = lax.fori_loop(
        0, i, lambda j, p: score(j, p, plain), jnp.full((8, wide), MASKED, F32)
    )
    peak = jnp.max(score(i, peak, edge), axis=0, keepdims=True)

    def weigh(j, total):
        p = jnp.exp(scores[j] - peak)
        low = p.astype(LOW)
        for h in range(groups):
            rows = slice(h * HEAD, (h + 1) * HEAD)
            acc[rows, :] += mm(
                vt[rows, pl.ds(pl.multiple_of(j * block, block), block)],
                low[:, h * block : (h + 1) * block],
            )
        return total + jnp.sum(p.reshape(block // 8, 8, wide), axis=0)

    total = lax.fori_loop(0, i + 1, weigh, jnp.zeros((8, wide), F32))
    total = jnp.sum(total, axis=0, keepdims=True)
    logs = peak + jnp.log(total)
    inverse = 1.0 / total
    for h in range(groups):
        rows = slice(h * HEAD, (h + 1) * HEAD)
        acc[rows, :] = acc[rows, :] * inverse[:, h * block : (h + 1) * block]
        for s in range(block // inner):
            log_ref[s, :, h * inner : (h + 1) * inner] = logs[
                :, h * block + s * inner : h * block + (s + 1) * inner
            ]
    out = acc[...].T
    wide_ref[...] = out
    out_ref[...] = out.astype(LOW)


def attend_forward(qkv, slope_row, block, inner):
    length, width = qkv.shape[1:]
    groups = width // HEAD
    count = length // block
    wide = groups * block
    ratio = block // inner
    part = pl.BlockSpec((block, width), lambda i: (i, 0))
    return pl.pallas_call(
        functools.partial(forward_kernel, groups, block, inner),
        grid=(count,),
        in_specs=[
            pl.BlockSpec((1, wide), lambda i: (0, 0)),
            pl.BlockSpec((1, block, width), lambda i: (0, i, 0)),
            pl.BlockSpec((1, length, width), lambda i: (1, 0, 0)),
            pl.BlockSpec((1, length, width), lambda i: (2, 0, 0)),
        ],
        out_specs=[
            part,
            part,
            pl.BlockSpec((ratio, 1, groups * inner), lambda i: (i, 0, 0)),
        ],
        out_shape=[
            jax.ShapeDtypeStruct((length, width), LOW),
            jax.ShapeDtypeStruct((length, width), F32),
            jax.ShapeDtypeStruct((length // inner, 1, groups * inner), F32),
        ],
        scratch_shapes=[
            pltpu.VMEM((block, wide), F32),
            pltpu.VMEM((block, wide), F32),
            pltpu.VMEM((width, length), LOW),
            pltpu.VMEM((wide, width), LOW),
            pltpu.VMEM((width, block), F32),
            pltpu.VMEM((count, block, wide), F32),
        ],
        compiler_params=pltpu.CompilerParams(vmem_limit_bytes=40 << 20),
        cost_estimate=pl.CostEstimate(
            flops=16 * length * length * width,
            bytes_accessed=12 * length * width,
            transcendentals=length * length * groups,
        ),
        name="attend_forward",
    )(slope_row, qkv, qkv, qkv)


def backward_kernel(
    groups, block, slope_ref, q_ref, k_ref, v_ref, grad_ref, wide_ref, log_ref,
    out_ref, plain, edge, qs, grads, delta, dq, dk, dv, ks
):
    j = pl.program_id(0)
    count = pl.num_programs(0)
    slope = slope_ref[...]
    scale = 1.0 / math.sqrt(HEAD)

    @pl.when(j == 0)
    def _():
        bias_tiles(slope, block, plain, edge, groups)
        dq[...] = jnp.zeros_like(dq)

        def prepare(i, unused):
            rows = pl.ds(pl.multiple_of(i * block, block), block)
            grad = grad_ref[rows, :]
            for h, part in enumerate(stack_heads(q_ref[0, rows, :], groups, LOW(scale))):
                qs[i, h * block : (h + 1) * block, :] = part
            for h, part in enumerate(stack_heads(grad, groups)):
                grads[i, h * block : (h + 1) * block, :] = part
            both = (wide_ref[rows, :] * grad.astype(F32)).T
            for h in range(groups):
                delta[i, :, h * block : (h + 1) * block] = jnp.sum(
                    both[h * HEAD : (h + 1) * HEAD, :], axis=0, keepdims=True
                )
            return unused

        lax.fori_loop(0, count, prepare, 0)

    keys = k_ref[0]
    values = v_ref[0]
    for h, part in enumerate(stack_heads(keys, groups)):
        ks[h] = part
    dk[...] = jnp.zeros_like(dk)
    dv[...] = jnp.zeros_like(dv)
    shift = slope * (j * block).astype(F32)

    def visit(i, tile_ref):
        heads_q = qs[i]
        heads_grad = grads[i]
        p = jnp.exp(mm(keys, heads_q, NT) + tile_ref[...] + (shift - log_ref[i]))
        ds = p * (mm(values, heads_grad, NT) - delta[i])
        p_low = p.astype(LOW)
        ds_low = ds.astype(LOW)
        dv[...] += mm(p_low, heads_grad)
        dk[...] += mm(ds_low, heads_q)
        total = mm(ds_low[:, :block], ks[0], TN)
        for h in range(1, groups):
            total += mm(ds_low[:, h * block : (h + 1) * block], ks[h], TN)
        dq[pl.ds(pl.multiple_of(i * block, block), block), :] += total

    visit(j, edge)

    def step(i, unused):
        visit(i, plain)
        return unused

    lax.fori_loop(j + 1, count, step, 0)
    out_ref[0] = (dq[pl.ds(pl.multiple_of(j * block, block), block), :] * scale).astype(LOW)
    out_ref[1] = dk[...].astype(LOW)
    out_ref[2] = dv[...].astype(LOW)


def attend_backward(qkv, grad, attended, log_totals, slope_row, block):
    length, width = qkv.shape[1:]
    groups = width // HEAD
    count = length // block
    wide = groups * block
    whole = pl.BlockSpec((length, width), lambda i: (0, 0))
    return pl.pallas_call(
        functools.partial(backward_kernel, groups, block),
        grid=(count,),
        in_specs=[
            pl.BlockSpec((1, wide), lambda i: (0, 0)),
            pl.BlockSpec((1, length, width), lambda i: (0, 0, 0)),
            pl.BlockSpec((1, block, width), lambda i: (1, i, 0)),
            pl.BlockSpec((1, block, width), lambda i: (2, i, 0)),
            whole,
            whole,
            pl.BlockSpec((count, 1, wide), lambda i: (0, 0, 0)),
        ],
        out_specs=pl.BlockSpec((3, block, width), lambda i: (0, i, 0)),
        out_shape=jax.ShapeDtypeStruct((3, length, width), LOW),
        scratch_shapes=[
            pltpu.VMEM((block, wide), F32),
            pltpu.VMEM((block, wide), F32),
            pltpu.VMEM((count, wide, width), LOW),
            pltpu.VMEM((count, wide, width), LOW),
            pltpu.VMEM((count, 1, wide), F32),
            pltpu.VMEM((length, width), F32),
            pltpu.VMEM((block, width), F32),
            pltpu.VMEM((block, width), F32),
            pltpu.VMEM((groups, block, width), LOW),
        ],
        compiler_params=pltpu.CompilerParams(vmem_limit_bytes=40 << 20),
        cost_estimate=pl.CostEstimate(
            flops=40 * length * length * width,
            bytes_accessed=18 * length * width,
            transcendentals=length * length * groups,
        ),
        name="attend_backward",
    )(slope_row, qkv, qkv, qkv, grad, attended, log_totals)


def ortho_kernel(tile, gram_ref, block_ref, out_ref, square, square_low, cross, cross_low, state):
    size = gram_ref.shape[0]
    steps = size // tile
    trace = jnp.zeros((1, 1), F32)
    for r in range(steps):
        rows = slice(r * tile, (r + 1) * tile)
        piece = gram_ref[rows, rows].astype(F32)
        same = lax.broadcasted_iota(jnp.int32, piece.shape, 0) == lax.broadcasted_iota(
            jnp.int32, piece.shape, 1
        )
        picked = jnp.where(same, piece, 0.0)
        trace += jnp.sum(jnp.sum(picked, axis=1, keepdims=True), axis=0, keepdims=True)
    factor = 1.0 / (jnp.sqrt(trace) + ORTHO_EPS)

    def load(r, unused):
        rows = pl.ds(pl.multiple_of(r * tile, tile), tile)
        first = gram_ref[rows, :].astype(F32) * factor * factor
        square[rows, :] = first
        square_low[rows, :] = first.astype(LOW)
        state[rows, :] = block_ref[rows, :].astype(F32) * factor
        out_ref[rows, :] = state[rows, :].astype(LOW)
        return unused

    lax.fori_loop(0, steps, load, 0)

    def advance():
        for r in range(steps):
            rows = slice(r * tile, (r + 1) * tile)
            state[rows, :] = 2.0 * state[rows, :] - mm(square_low[rows, :], out_ref[...])

    def settle():
        out_ref[...] = state[...].astype(LOW)

    def iterate(t, unused):
        advance()
        for r in range(steps):
            rows = slice(r * tile, (r + 1) * tile)
            value = 2.0 * square[rows, :] - mm(square_low[rows, :], square_low[...])
            cross[rows, :] = value
            cross_low[rows, :] = value.astype(LOW)
        settle()
        for r in range(steps):
            rows = slice(r * tile, (r + 1) * tile)
            square[rows, :] = 2.0 * cross[rows, :] - mm(cross_low[rows, :], square_low[...])
        square_low[...] = square[...].astype(LOW)
        return unused

    lax.fori_loop(0, NS_ITERS - 1, iterate, 0)
    advance()
    settle()


def orthogonal(gram, block):
    size, width = block.shape
    tile = min(256, size)
    return pl.pallas_call(
        functools.partial(ortho_kernel, tile),
        out_shape=jax.ShapeDtypeStruct((size, width), LOW),
        in_specs=[pl.BlockSpec(memory_space=pltpu.VMEM)] * 2,
        out_specs=pl.BlockSpec(memory_space=pltpu.VMEM),
        scratch_shapes=[
            pltpu.VMEM((size, size), F32),
            pltpu.VMEM((size, size), LOW),
            pltpu.VMEM((size, size), F32),
            pltpu.VMEM((size, size), LOW),
            pltpu.VMEM((size, width), F32),
        ],
        compiler_params=pltpu.CompilerParams(vmem_limit_bytes=40 << 20),
        cost_estimate=pl.CostEstimate(
            flops=16 * size**3 + 10 * size * size * width, bytes_accessed=4 * size * size, transcendentals=0
        ),
        name="orthogonal",
    )(gram, block)


def swap(value, axis, bit):
    return lax.ppermute(value, axis, [(i, i ^ bit) for i in range(lax.axis_size(axis))])


def pick(buffer, axis, count, stride, choice):
    size = buffer.shape[axis] // count
    run = stride * size
    parts = [
        lax.dynamic_slice_in_dim(buffer, 2 * i * run + choice * run, run, axis)
        for i in range(count // (2 * stride))
    ]
    return parts[0] if len(parts) == 1 else jnp.concatenate(parts, axis)


def reduce_blocks(buffer, axis, held):
    me = lax.axis_index("dp")
    count = 1 << len(held)

    def ladder(piece, order):
        left = list(held)
        blocks = count
        for bit in order:
            stride = 1 << (len(left) - 1 - left.index(bit))
            mine = (me // bit) % 2
            arrived = swap(pick(piece, axis, blocks, stride, 1 - mine), "dp", bit)
            kept = pick(piece, axis, blocks, stride, mine)
            piece = (kept.astype(F32) + arrived.astype(F32)).astype(LOW)
            left.remove(bit)
            blocks //= 2
        return piece

    if not held:
        return buffer
    other = 1 - axis
    half = buffer.shape[other] // 2
    ascending = sorted(held)
    orders = (ascending, ascending[1:] + ascending[:1])
    pieces = [
        ladder(lax.slice_in_dim(buffer, k * half, (k + 1) * half, axis=other), orders[k])
        for k in range(2)
    ]
    return jnp.concatenate(pieces, other)


def gradient_pair(left, right, axis):
    size = lax.axis_size("dp")
    mine = lax.axis_index("dp") % 2

    def product(choice):
        if axis == 1:
            return mm(left, pick(right, 1, size, 1, choice), TN)
        return mm(pick(left, 1, size, 1, choice), right, TN)

    arrived = swap(product(1 - mine).astype(LOW), "dp", 1)
    return (product(mine) + arrived.astype(F32)).astype(LOW)


def other_bits():
    return [1 << b for b in range(1, lax.axis_size("dp").bit_length() - 1)][::-1]


def collect(value, owner, pieces):
    size = lax.axis_size("seq")
    hops = []
    left = [(i, i - 1) for i in range(size - 1, owner, -1)]
    right = [(i, i + 1) for i in range(owner)]
    while left or right:
        hops.append(left[:1] + right[:1])
        left, right = left[1:], right[1:]
        if len(hops[-1]) == 2 and hops[-1][0][1] == hops[-1][1][1]:
            hops[-1:] = [hops[-1][:1], hops[-1][1:]]
    rows = value.shape[0] // pieces
    parts = []
    for k in range(pieces):
        part = value[k * rows : (k + 1) * rows]
        for hop in hops:
            arrived = lax.ppermute(part, "seq", hop)
            part = (part.astype(F32) + arrived.astype(F32)).astype(LOW)
        parts.append(part)
    return parts[0] if pieces == 1 else jnp.concatenate(parts, 0)


def share(own, widths):
    size = lax.axis_size("seq")
    here = lax.axis_index("seq")
    found = {0: own}
    for way in (1, -1):
        moving = own
        for distance in range(1, size):
            pairs = [
                (i, i + way) for i in range(size) if 0 <= i + way < size and 0 <= i + way - way * distance < size
            ]
            moving = lax.ppermute(moving, "seq", pairs)
            found[way * distance] = moving
    result = []
    for m, width in enumerate(widths):
        value = own[:, :width]
        for d in range(size):
            if d != m:
                value = jnp.where(here == d, found[d - m][:, :width], value)
        result.append(value)
    return result


def gram_total(gram):
    me = lax.axis_index("dp")
    size = lax.axis_size("dp")
    bits = [1 << b for b in range(size.bit_length() - 1)]

    def ladder(piece, order):
        sizes = []
        for bit in order:
            half = piece.shape[0] // 2
            mine = (me // bit) % 2
            arrived = swap(lax.dynamic_slice_in_dim(piece, (1 - mine) * half, half, 0), "dp", bit)
            kept = lax.dynamic_slice_in_dim(piece, mine * half, half, 0)
            piece = (kept.astype(F32) + arrived.astype(F32)).astype(LOW)
            sizes.append(half)
        for bit, half in zip(reversed(order), reversed(sizes)):
            mine = (me // bit) % 2
            arrived = swap(piece, "dp", bit)
            first = jnp.where(mine == 0, piece, arrived)
            second = jnp.where(mine == 0, arrived, piece)
            piece = jnp.concatenate([first, second], 0)
        return piece

    half = gram.shape[1] // 2
    low = gram.astype(LOW)
    return jnp.concatenate(
        [
            ladder(low[:, :half], bits),
            ladder(low[:, half:], bits[:1] + bits[2:] + bits[1:2]),
        ],
        1,
    )


def sum_everywhere(value):
    for axis in ("dp", "seq"):
        bit = 1
        while bit < lax.axis_size(axis):
            value = value + swap(value, axis, bit)
            bit *= 2
    return value


def depart(source, take):
    size = lax.axis_size("seq")
    here = lax.axis_index("seq")
    pieces = []
    for shift in range(size):
        piece = take(source, (here + shift) % size)
        if shift:
            piece = lax.ppermute(piece, "seq", [(i, (i + shift) % size) for i in range(size)])
        pieces.append(piece)
    return pieces


def arrange(pieces, place, shape):
    size = lax.axis_size("seq")
    here = lax.axis_index("seq")
    result = jnp.zeros(shape, LOW)
    for shift, piece in enumerate(pieces):
        result = lax.dynamic_update_slice(result, piece, place((here - shift) % size))
    return result


MESH = pl.DeviceIdType.MESH
TRIPS = 8
OWNERS = 4


def greet(axes_partners):
    barrier = pltpu.get_barrier_semaphore()
    count = 0
    for axis, partner, real in axes_partners:

        def tell(axis=axis, partner=partner):
            pl.semaphore_signal(barrier, inc=1, device_id={axis: partner}, device_id_type=MESH)

        if real is None:
            tell()
            count = count + 1
        else:
            pl.when(real)(tell)
            count = count + real.astype(jnp.int32)
    pl.semaphore_wait(barrier, count)


def plane():
    me = lax.axis_index("dp")
    core, x, y = lax.rem(me, 2), lax.rem(me // 2, 2), me // 4
    flip = lambda bit: 1 - bit
    return (
        (core, x, y),
        (
            4 * y + 2 * x + flip(core),
            4 * y + 2 * flip(x) + core,
            4 * flip(y) + 2 * x + core,
        ),
    )


def combine_kernel(
    ways, wide_q, wide_p, qkv_ref, proj_ref, up_ref, down_ref, out_ref,
    one, send_two, two, send_three, three, final, from_left, from_right, relay,
    s_one, r_one, s_two, r_two, s_three, r_three, s_left, r_left, s_right, r_right,
):
    (core, x, y), partners = plane()
    z = lax.axis_index("seq")
    size = up_ref.shape[0]
    half = size // 2
    chunks = TRIPS
    step = size // chunks
    width = wide_q + wide_p
    greet(
        [("dp", p, None) for p in partners]
        + [("seq", jnp.maximum(z - 1, 0), z > 0), ("seq", jnp.minimum(z + 1, ways - 1), z < ways - 1)]
    )

    def remote(src, dst, send, recv, axis, target):
        return pltpu.make_async_remote_copy(
            src_ref=src, dst_ref=dst, send_sem=send, recv_sem=recv,
            device_id={axis: target}, device_id_type=MESH,
        )

    owned = ((0, width), (0, wide_q), (wide_q, wide_p), (0, width))

    def source(m, k):
        rows = pl.ds(k * step, step)
        lanes = pl.ds(*owned[m])
        return (up_ref, final, final, down_ref)[m].at[rows, lanes]

    def hop(m, k, left, src):
        lanes = pl.ds(*owned[m])
        box, send, recv = (from_right, s_left, r_left) if left else (from_left, s_right, r_right)
        slot = m
        return remote(
            src, box.at[slot, pl.ds(k * step, step), lanes], send.at[m, k], recv.at[m, k],
            "seq", jnp.maximum(z - 1, 0) if left else jnp.minimum(z + 1, ways - 1),
        )

    def relay_src(m, k):
        return relay.at[m, pl.ds(k * step, step), pl.ds(*owned[m])]

    def begin(m, parts):
        for k in parts:
            if m < ways - 1:
                @pl.when(z == ways - 1)
                def _():
                    hop(m, k, True, source(m, k)).start()
            if m > 0:
                @pl.when(z == 0)
                def _():
                    hop(m, k, False, source(m, k)).start()

    def pass_on(m, k):
        rows = pl.ds(k * step, step)
        lanes = pl.ds(*owned[m])
        strip = 64

        def added(box):
            def body(i, unused):
                part = pl.ds(pl.multiple_of(k * step + i * strip, strip), strip)
                src = (up_ref, final, final, down_ref)[m]
                relay[m, part, lanes] = (
                    src[part, lanes].astype(F32) + box[m, part, lanes].astype(F32)
                ).astype(LOW)
                return unused

            lax.fori_loop(0, step // strip, body, 0)

        if m < ways - 2:
            @pl.when((z > m) & (z < ways - 1))
            def _():
                hop(m, k, True, source(m, k)).wait_recv()
                added(from_right)
                hop(m, k, True, relay_src(m, k)).start()
        if m > 1:
            @pl.when((z < m) & (z > 0))
            def _():
                hop(m, k, False, source(m, k)).wait_recv()
                added(from_left)
                hop(m, k, False, relay_src(m, k)).start()

    def settle(m, k):
        lanes = pl.ds(*owned[m])
        strip = 64

        @pl.when(z == m)
        def _():
            if m < ways - 1:
                hop(m, k, True, source(m, k)).wait_recv()
            if m > 0:
                hop(m, k, False, source(m, k)).wait_recv()

            def body(i, unused):
                part = pl.ds(pl.multiple_of(k * step + i * strip, strip), strip)
                src = (up_ref, final, final, down_ref)[m]
                total = src[part, lanes].astype(F32)
                if m < ways - 1:
                    total += from_right[m, part, lanes].astype(F32)
                if m > 0:
                    total += from_left[m, part, lanes].astype(F32)
                width_m = owned[m][1]
                out_ref[part, pl.ds(0, width_m)] = total.astype(LOW)
                if width_m < width:
                    out_ref[part, pl.ds(width_m, width - width_m)] = jnp.zeros(
                        (strip, width - width_m), LOW
                    )
                return unused

            lax.fori_loop(0, step // strip, body, 0)

    begin(0, range(chunks))
    begin(3, range(chunks))

    strip = 64

    def own(h, block, start, rows):
        part = pl.ds(pl.multiple_of(h * half + start, strip), rows)
        q = qkv_ref[part, pl.ds(pl.multiple_of(block * wide_q, 128), wide_q)]
        p = proj_ref[part, pl.ds(pl.multiple_of(block * wide_p, 128), wide_p)]
        return jnp.concatenate([q, p], axis=1).astype(F32)

    def first(h, k):
        block = 2 * k + (1 - core)
        rows = pl.ds(h * half, half)
        return [
            remote(
                qkv_ref.at[rows, pl.ds(pl.multiple_of(block * wide_q, 128), wide_q)],
                one.at[h, k, :, pl.ds(0, wide_q)], s_one.at[h, k, 0], r_one.at[h, k, 0],
                "dp", partners[0],
            ),
            remote(
                proj_ref.at[rows, pl.ds(pl.multiple_of(block * wide_p, 128), wide_p)],
                one.at[h, k, :, pl.ds(wide_q, wide_p)], s_one.at[h, k, 1], r_one.at[h, k, 1],
                "dp", partners[0],
            ),
        ]

    go = [[(2 * j + (1 - x)) for j in range(2)], [(2 * (1 - y) + j) for j in range(2)]]
    stay = [[(2 * j + x) for j in range(2)], [(2 * y + j) for j in range(2)]]
    for group in (go, stay):
        for j in range(2):
            for h in range(2):
                for copy in first(h, group[h][j]):
                    copy.start()

    def second(h, j):
        return remote(send_two.at[h, j], two.at[h, j], s_two.at[h, j], r_two.at[h, j],
                      "dp", partners[1 + h])

    for j in range(2):
        for h in range(2):
            k = go[h][j]
            for copy in first(h, k):
                copy.wait_recv()

            def body(i, unused):
                part = pl.ds(pl.multiple_of(i * strip, strip), strip)
                value = own(h, 2 * k + core, i * strip, strip) + one[h, k, part, :].astype(F32)
                send_two[h, j, part, :] = value.astype(LOW)
                return unused

            lax.fori_loop(0, half // strip, body, 0)
            second(h, j).start()
    for k in range(chunks // 2):
        pass_on(0, k)
        pass_on(3, k)

    def third(h):
        return remote(send_three.at[h], three.at[h], s_three.at[h], r_three.at[h],
                      "dp", partners[2 - h])

    mine = [y, x]
    for h in range(2):
        for j in range(2):
            for copy in first(h, stay[h][j]):
                copy.wait_recv()
        for j in range(2):
            second(h, j).wait_recv()
        j = 1 - mine[h]
        k = 2 * j + x if h == 0 else 2 * y + j

        def body(i, unused):
            part = pl.ds(pl.multiple_of(i * strip, strip), strip)
            value = (
                own(h, 2 * k + core, i * strip, strip)
                + one[h, k, part, :].astype(F32)
                + two[h, j, part, :].astype(F32)
            )
            send_three[h, part, :] = value.astype(LOW)
            return unused

        lax.fori_loop(0, half // strip, body, 0)
        third(h).start()
    for k in range(chunks // 2, chunks):
        pass_on(0, k)
        pass_on(3, k)
    for h in range(2):
        third(h).wait_recv()
        j = mine[h]
        k = 2 * y + x

        def body(i, unused):
            part = pl.ds(pl.multiple_of(i * strip, strip), strip)
            value = (
                own(h, 2 * k + core, i * strip, strip)
                + one[h, k, part, :].astype(F32)
                + two[h, j, part, :].astype(F32)
                + three[h, part, :].astype(F32)
            )
            final[pl.ds(pl.multiple_of(h * half + i * strip, strip), strip), :] = value.astype(LOW)
            return unused

        lax.fori_loop(0, half // strip, body, 0)
        parts = range(h * chunks // 2, (h + 1) * chunks // 2)
        begin(1, parts)
        begin(2, parts)
    for k in range(chunks):
        pass_on(1, k)
        pass_on(2, k)
    for m in (0, 3, 1, 2):
        for k in range(chunks):
            settle(m, k)

    for h in range(2):
        for k in range(4):
            for copy in first(h, k):
                copy.wait_send()
        for j in range(2):
            second(h, j).wait_send()
        third(h).wait_send()
    for m in range(OWNERS):
        for k in range(chunks):
            if m < ways - 1:
                @pl.when(z > m)
                def _():
                    hop(m, k, True, source(m, k)).wait_send()
            if m > 0:
                @pl.when(z < m)
                def _():
                    hop(m, k, False, source(m, k)).wait_send()


def combine(ways, qkv, proj, up, down):
    size, width = up.shape
    wide_q, wide_p = qkv.shape[1] // 8, proj.shape[1] // 8
    half = size // 2
    vmem = pl.BlockSpec(memory_space=pltpu.VMEM)
    dma = pltpu.SemaphoreType.DMA
    return pl.pallas_call(
        functools.partial(combine_kernel, ways, wide_q, wide_p),
        out_shape=jax.ShapeDtypeStruct((size, width), LOW),
        in_specs=[vmem] * 4,
        out_specs=vmem,
        scratch_shapes=[
            pltpu.VMEM((2, 4, half, width), LOW),
            pltpu.VMEM((2, 2, half, width), LOW),
            pltpu.VMEM((2, 2, half, width), LOW),
            pltpu.VMEM((2, half, width), LOW),
            pltpu.VMEM((2, half, width), LOW),
            pltpu.VMEM((size, width), LOW),
            pltpu.VMEM((OWNERS, size, width), LOW),
            pltpu.VMEM((OWNERS, size, width), LOW),
            pltpu.VMEM((OWNERS, size, width), LOW),
            dma((2, 4, 2)), dma((2, 4, 2)), dma((2, 2)), dma((2, 2)), dma((2,)), dma((2,)),
            dma((OWNERS, TRIPS)), dma((OWNERS, TRIPS)), dma((OWNERS, TRIPS)), dma((OWNERS, TRIPS)),
        ],
        compiler_params=pltpu.CompilerParams(
            collective_id=1, has_side_effects=True, vmem_limit_bytes=56 << 20
        ),
        cost_estimate=pl.CostEstimate(flops=50_000_000_000, bytes_accessed=1 << 23, transcendentals=0),
        name="combine",
    )(qkv, proj, up, down)


def finish_kernel(
    ways, widths, chunks, gram_ref, block_ref, grad_ref, vector_ref,
    g0, g1, g2, g3, y0, y1, y2, y3, total_ref,
    one, send_two, two, send_three, three, whole,
    square, square_low, cross, cross_low, state, low, g_down, y_down, vectors, arrived,
    s_one, r_one, s_two, r_two, s_three, r_three, s_back, r_back,
    gs_left, gr_left, gs_right, gr_right, ys_left, yr_left, ys_right, yr_right, s_own, s_vec, r_vec,
):
    (core, x, y), partners = plane()
    z = lax.axis_index("seq")
    across = lax.rem(z + 2, 4)
    beside = z + 1 - 2 * lax.rem(z, 2)
    size = gram_ref.shape[0]
    rows = size // 8
    half = size // 2
    step = size // chunks
    greet(
        [("dp", p, None) for p in partners]
        + [
            ("seq", across, None),
            ("seq", jnp.maximum(z - 1, 0), z > 0),
            ("seq", jnp.minimum(z + 1, ways - 1), z < ways - 1),
        ]
    )

    class Trip:
        def __init__(self, own, outs, s_left, r_left, s_right, r_right, local):
            self.own, self.outs, self.local = own, outs, local
            self.left, self.right = (s_left, r_left), (s_right, r_right)

        def hop(self, m, k, left, relayed):
            part = pl.ds(pl.multiple_of(k * step, step), step)
            place = self.outs[m].at[part, :]
            src = place if relayed else self.own.at[part, pl.ds(0, widths[m])]
            send, recv = self.left if left else self.right
            return pltpu.make_async_remote_copy(
                src_ref=src, dst_ref=place, send_sem=send.at[m, k], recv_sem=recv.at[m, k],
                device_id={"seq": jnp.maximum(z - 1, 0) if left else jnp.minimum(z + 1, ways - 1)},
                device_id_type=MESH,
            )

        def copy(self, m):
            return pltpu.make_async_copy(
                self.own.at[:, pl.ds(0, widths[m])], self.outs[m], s_own.at[self.local]
            )

        def begin(self):
            for m in range(OWNERS):
                @pl.when(z == m)
                def _():
                    for k in range(chunks):
                        if m < ways - 1:
                            self.hop(m, k, False, False).start()
                        if m > 0:
                            self.hop(m, k, True, False).start()
                    self.copy(m).start()

        def relay(self, distance, k):
            for m in range(OWNERS):
                if m + distance < ways:
                    @pl.when(z == m + distance)
                    def _():
                        self.hop(m, k, False, True).wait_recv()
                        if m + distance < ways - 1:
                            self.hop(m, k, False, True).start()
                if m - distance >= 0:
                    @pl.when(z == m - distance)
                    def _():
                        self.hop(m, k, True, True).wait_recv()
                        if m - distance > 0:
                            self.hop(m, k, True, True).start()

        def end(self):
            for m in range(OWNERS):
                @pl.when(z == m)
                def _():
                    self.copy(m).wait()

                for k in range(chunks):
                    @pl.when((z >= m) & (z < ways - 1))
                    def _():
                        self.hop(m, k, False, True).wait_send()

                    @pl.when((z <= m) & (z > 0))
                    def _():
                        self.hop(m, k, True, True).wait_send()

    grads = Trip(grad_ref, (g0, g1, g2, g_down), gs_left, gr_left, gs_right, gr_right, 0)
    steps = Trip(low, (y0, y1, y2, y_down), ys_left, yr_left, ys_right, yr_right, 1)
    grads.begin()

    def vector_copy(i):
        source = vector_ref if i == 0 else vectors.at[i - 1]
        target = (
            [{"dp": p} for p in partners] + [{"seq": beside}, {"seq": across}]
        )[i]
        return pltpu.make_async_remote_copy(
            src_ref=source, dst_ref=arrived.at[i], send_sem=s_vec.at[i], recv_sem=r_vec.at[i],
            device_id=target, device_id_type=MESH,
        )

    def vector_step(i):
        vector_copy(i).wait_recv()
        value = (vector_ref[...] if i == 0 else vectors[i - 1]) + arrived[i]
        if i < 4:
            vectors[i] = value
            vector_copy(i + 1).start()
        else:
            total_ref[...] = value

    vector_copy(0).start()

    def remote(src, dst, send, recv, target):
        return pltpu.make_async_remote_copy(
            src_ref=src, dst_ref=dst, send_sem=send, recv_sem=recv,
            device_id={"dp": target}, device_id_type=MESH,
        )

    def block(ref, h, d):
        return ref.at[pl.ds(pl.multiple_of(d * rows, rows), rows), pl.ds(h * half, half)]

    def own(h, d):
        return gram_ref[
            pl.ds(pl.multiple_of(d * rows, rows), rows), pl.ds(h * half, half)
        ].astype(F32)

    def first(h, k):
        return remote(block(gram_ref, h, 2 * k + 1 - core), one.at[h, k], s_one.at[h, k],
                      r_one.at[h, k], partners[0])

    go = [[(2 * j + (1 - x)) for j in range(2)], [(2 * (1 - y) + j) for j in range(2)]]
    stay = [[(2 * j + x) for j in range(2)], [(2 * y + j) for j in range(2)]]
    for group in (go, stay):
        for j in range(2):
            for h in range(2):
                first(h, group[h][j]).start()

    def second(h, j):
        return remote(send_two.at[h, j], two.at[h, j], s_two.at[h, j], r_two.at[h, j], partners[1 + h])

    for j in range(2):
        for h in range(2):
            k = go[h][j]
            first(h, k).wait_recv()
            send_two[h, j] = (own(h, 2 * k + core) + one[h, k].astype(F32)).astype(LOW)
            second(h, j).start()
    vector_step(0)

    def third(h):
        return remote(send_three.at[h], three.at[h], s_three.at[h], r_three.at[h], partners[2 - h])

    mine = [y, x]
    for h in range(2):
        for j in range(2):
            first(h, stay[h][j]).wait_recv()
        for j in range(2):
            second(h, j).wait_recv()
        j = 1 - mine[h]
        k = 2 * j + x if h == 0 else 2 * y + j
        send_three[h] = (
            own(h, 2 * k + core) + one[h, k].astype(F32) + two[h, j].astype(F32)
        ).astype(LOW)
        third(h).start()
    vector_step(1)
    for c in range(chunks // 4):
        grads.relay(1, c)

    def back(h, stage, d):
        target = (partners[2 - h], partners[1 + h], partners[0])[stage]
        place = block(whole, h, d)
        slot = (0, 1, 3)[stage]
        return lambda i: remote(place, place, s_back.at[h, slot + i], r_back.at[h, slot + i], target)

    k = 2 * y + x
    for h in range(2):
        third(h).wait_recv()
        value = (
            own(h, 2 * k + core)
            + one[h, k].astype(F32)
            + two[h, mine[h]].astype(F32)
            + three[h].astype(F32)
        ).astype(LOW)
        d = 2 * k + core
        whole[pl.ds(pl.multiple_of(d * rows, rows), rows), pl.ds(h * half, half)] = value
        for stage in range(3):
            back(h, stage, d)(0).start()
    vector_step(2)
    k_next = [2 * (1 - y) + x, 2 * y + (1 - x)]
    for h in range(2):
        d = 2 * k_next[h] + core
        back(h, 0, d)(0).wait_recv()
        back(h, 1, d)(1).start()
        back(h, 2, d)(1).start()
    for c in range(chunks // 4, chunks // 2):
        grads.relay(1, c)
    for h in range(2):
        for i in range(2):
            if h == 0:
                kk = 2 * (y if i == 0 else 1 - y) + (1 - x)
            else:
                kk = 2 * (1 - y) + (x if i == 0 else 1 - x)
            d = 2 * kk + core
            back(h, 1, d)(i).wait_recv()
            back(h, 2, d)(2 + i).start()
    for h in range(2):
        for i, kk in enumerate(
            (
                2 * y + x,
                k_next[h],
                2 * y + (1 - x) if h == 0 else 2 * (1 - y) + x,
                2 * (1 - y) + (1 - x),
            )
        ):
            back(h, 2, 2 * kk + 1 - core)(i).wait_recv()
    vector_step(3)
    for c in range(chunks // 2, chunks):
        grads.relay(1, c)

    tile = 256
    count = size // tile
    trace = jnp.zeros((1, 1), F32)
    for r in range(count):
        part = slice(r * tile, (r + 1) * tile)
        piece = whole[part, part].astype(F32)
        same = lax.broadcasted_iota(jnp.int32, piece.shape, 0) == lax.broadcasted_iota(
            jnp.int32, piece.shape, 1
        )
        picked = jnp.where(same, piece, 0.0)
        trace += jnp.sum(jnp.sum(picked, axis=1, keepdims=True), axis=0, keepdims=True)
    factor = 1.0 / (jnp.sqrt(trace) + ORTHO_EPS)

    def load(r, unused):
        part = pl.ds(pl.multiple_of(r * tile, tile), tile)
        begun = whole[part, :].astype(F32) * factor * factor
        square[part, :] = begun
        square_low[part, :] = begun.astype(LOW)
        state[part, :] = block_ref[part, :].astype(F32) * factor
        low[part, :] = state[part, :].astype(LOW)
        return unused

    lax.fori_loop(0, count, load, 0)

    def advance():
        for r in range(count):
            part = slice(r * tile, (r + 1) * tile)
            state[part, :] = 2.0 * state[part, :] - mm(square_low[part, :], low[...])

    def iterate(t, unused):
        advance()
        for r in range(count):
            part = slice(r * tile, (r + 1) * tile)
            value = 2.0 * square[part, :] - mm(square_low[part, :], square_low[...])
            cross[part, :] = value
            cross_low[part, :] = value.astype(LOW)
        low[...] = state[...].astype(LOW)
        for r in range(count):
            part = slice(r * tile, (r + 1) * tile)
            square[part, :] = 2.0 * cross[part, :] - mm(cross_low[part, :], square_low[...])
        square_low[...] = square[...].astype(LOW)
        for c in range(chunks // 4):
            grads.relay(2, t * (chunks // 4) + c)
        return unused

    lax.fori_loop(0, NS_ITERS - 1, iterate, 0)
    advance()
    low[...] = state[...].astype(LOW)

    steps.begin()
    vector_step(4)
    for c in range(chunks):
        grads.relay(3, c)
    grads.end()

    def turn(ref, out):
        for c in range(size // 256):
            out[:, c * 256 : (c + 1) * 256] = ref[c * 256 : (c + 1) * 256, :].T

    for distance in range(1, ways):
        for c in range(chunks):
            steps.relay(distance, c)
        if distance == 1:
            turn(g_down, g3)
    steps.end()
    turn(y_down, y3)

    for h in range(2):
        for j in range(4):
            first(h, j).wait_send()
        for j in range(2):
            second(h, j).wait_send()
        third(h).wait_send()
        d = 2 * k + core
        back(h, 0, d)(0).wait_send()
        for i in range(2):
            back(h, 1, d)(i).wait_send()
        for i in range(4):
            back(h, 2, d)(i).wait_send()
    for i in range(5):
        vector_copy(i).wait_send()


def finish(ways, gram, block, grad, vectors, widths):
    size, width = block.shape
    rows, half = size // 8, size // 2
    chunks = 8
    vmem = pl.BlockSpec(memory_space=pltpu.VMEM)
    dma = pltpu.SemaphoreType.DMA
    shapes = [
        jax.ShapeDtypeStruct((size, w) if m < OWNERS - 1 else (w, size), LOW)
        for m, w in enumerate(widths)
    ]
    down = pltpu.VMEM((size, widths[-1]), LOW)
    result = pl.pallas_call(
        functools.partial(finish_kernel, ways, widths, chunks),
        out_shape=shapes * 2 + [jax.ShapeDtypeStruct(vectors.shape, F32)],
        in_specs=[vmem] * 4,
        out_specs=[vmem] * 9,
        scratch_shapes=[
            pltpu.VMEM((2, 4, rows, half), LOW),
            pltpu.VMEM((2, 2, rows, half), LOW),
            pltpu.VMEM((2, 2, rows, half), LOW),
            pltpu.VMEM((2, rows, half), LOW),
            pltpu.VMEM((2, rows, half), LOW),
            pltpu.VMEM((size, size), LOW),
            pltpu.VMEM((size, size), F32),
            pltpu.VMEM((size, size), LOW),
            pltpu.VMEM((size, size), F32),
            pltpu.VMEM((size, size), LOW),
            pltpu.VMEM((size, width), F32),
            pltpu.VMEM((size, width), LOW),
            down,
            down,
            pltpu.VMEM((4,) + vectors.shape, F32),
            pltpu.VMEM((5,) + vectors.shape, F32),
            dma((2, 4)), dma((2, 4)), dma((2, 2)), dma((2, 2)), dma((2,)), dma((2,)),
            dma((2, 7)), dma((2, 7)),
        ]
        + [dma((OWNERS, chunks))] * 8
        + [dma((2,)), dma((5,)), dma((5,))],
        compiler_params=pltpu.CompilerParams(
            collective_id=2, has_side_effects=True, vmem_limit_bytes=56 << 20
        ),
        cost_estimate=pl.CostEstimate(
            flops=80_000_000_000, bytes_accessed=1 << 24, transcendentals=0
        ),
        name="finish",
    )(gram, block, grad, vectors)
    return result[:4], result[4:8], result[8]


def norm_forward(values, gain_row, offset):
    center = values - jnp.mean(values, axis=-1, keepdims=True)
    inv_scale = lax.rsqrt(jnp.mean(center * center, axis=-1, keepdims=True) + NORM_EPS)
    unit_values = center * inv_scale
    return (unit_values * gain_row + offset, unit_values, inv_scale)


def norm_backward(upstream, unit_values, inv_scale, gain_row):
    scaled = upstream * gain_row
    inner_sum = jnp.mean(scaled * unit_values, axis=-1, keepdims=True)
    input_grad = inv_scale * (
        scaled - jnp.mean(scaled, axis=-1, keepdims=True) - unit_values * inner_sum
    )
    return (input_grad, jnp.sum(upstream * unit_values, axis=0), jnp.sum(upstream, axis=0))


def gelu_both(values):
    square = values * values
    tangent = jnp.tanh(GELU_C * (values + 0.044715 * square * values))
    slope = 0.5 * (1.0 + tangent) + 0.5 * values * (1.0 - tangent * tangent) * GELU_C * (
        1.0 + 3.0 * 0.044715 * square
    )
    return 0.5 * values * (1.0 + tangent), slope


def on_device(
    tokens,
    cotangent,
    qkv_weight,
    proj_weight,
    up_weight,
    down_weight,
    norm_gains,
    biases,
    up_bias,
    head_slopes,
    qkv_moment,
    proj_moment,
    up_moment,
    down_moment,
    gains_moment,
    biases_moment,
    upbias_moment,
):
    rows, width = tokens.shape
    ways = lax.axis_size("seq")
    here = lax.axis_index("seq")
    me = lax.axis_index("dp")
    length = rows * ways
    own_width = width // ways
    chunks = 2
    chunk = own_width // chunks
    chunk_heads = chunk // HEAD
    own_slopes = lax.dynamic_slice_in_dim(
        head_slopes, here * (own_width // HEAD), own_width // HEAD, 0
    )
    chunk_slopes = [own_slopes[c * chunk_heads : (c + 1) * chunk_heads] for c in range(chunks)]

    inputs = tokens.astype(F32)
    normed_one, unit_one, scale_one = norm_forward(inputs, norm_gains[0], biases[0])
    normed_one = normed_one.astype(LOW)
    bias_row = jnp.concatenate([biases[1], jnp.zeros_like(biases[1]), biases[2]])
    mixed = (mm(normed_one, qkv_weight) + bias_row).astype(LOW)

    def take_mixed(c):
        def take(source, d):
            return jnp.stack(
                [
                    lax.dynamic_slice_in_dim(
                        source, part * width + d * own_width + c * chunk, chunk, 1
                    )
                    for part in range(3)
                ]
            )

        return take

    qkv_pieces = [depart(mixed, take_mixed(c)) for c in range(chunks)]
    qkv = []
    attended = jnp.zeros((rows, width), LOW)
    kept = []
    for c in range(chunks):
        if c:
            qkv_pieces[c], out = lax.optimization_barrier((qkv_pieces[c], out))
        qkv.append(arrange(qkv_pieces[c], lambda d: (0, d * rows, 0), (3, length, chunk)))
        out, wide, log_totals = attend_forward(
            qkv[c], jnp.repeat(chunk_slopes[c], BLOCK)[None], BLOCK, BLOCK
        )
        kept.append((wide, log_totals))
        for shift in range(ways):
            piece = lax.dynamic_slice_in_dim(out, ((here + shift) % ways) * rows, rows, 0)
            if shift:
                piece = lax.ppermute(piece, "seq", [(i, (i + shift) % ways) for i in range(ways)])
            attended = lax.dynamic_update_slice(
                attended, piece, (0, ((here - shift) % ways) * own_width + c * chunk)
            )

    middle = inputs + mm(attended, proj_weight) + biases[3]
    normed_two, unit_two, scale_two = norm_forward(middle, norm_gains[1], biases[4])
    normed_two = normed_two.astype(LOW)
    before = mm(normed_two, up_weight) + up_bias
    hidden, slope = gelu_both(before)
    hidden = hidden.astype(LOW)
    upstream = cotangent.astype(F32)
    hidden_grad = mm(cotangent, down_weight, NT)
    before_grad = (hidden_grad * slope).astype(LOW)
    normed_two_grad = mm(before_grad, up_weight, NT)
    middle_back, gain_two_grad, offset_two_grad = norm_backward(
        normed_two_grad, unit_two, scale_two, norm_gains[1]
    )
    middle_grad = upstream + middle_back
    branch_grad = middle_grad.astype(LOW)
    heads_grad = mm(branch_grad, proj_weight, NT).astype(LOW)

    grad_pieces = [
        depart(
            heads_grad,
            lambda source, d: lax.dynamic_slice_in_dim(source, d * own_width + c * chunk, chunk, 1),
        )
        for c in range(chunks)
    ]
    down_pair = gradient_pair(cotangent, hidden, 1)
    grad_pieces[0], down_pair = lax.optimization_barrier((grad_pieces[0], down_pair))

    mixed_pieces = []
    for c in range(chunks):
        if c:
            grad_pieces[c], back = lax.optimization_barrier((grad_pieces[c], back))
        grad = arrange(grad_pieces[c], lambda d: (d * rows, 0), (length, chunk))
        back = attend_backward(qkv[c], grad, *kept[c], jnp.repeat(chunk_slopes[c], BLOCK)[None], BLOCK)
        mixed_pieces.append(
            depart(back, lambda source, d: lax.dynamic_slice_in_dim(source, d * rows, rows, 1))
        )
    late = lax.optimization_barrier((normed_two, before_grad, hidden, attended, branch_grad, back))
    up_pair = gradient_pair(late[0], late[1], 1)
    block_out = (middle + mm(late[2], down_weight) + biases[5]).astype(LOW)
    proj_grad = mm(late[3], late[4], TN).astype(LOW)
    down_part = reduce_blocks(down_pair, 1, other_bits())
    up_part = reduce_blocks(up_pair, 1, other_bits())
    mixed_pieces[-1], down_part, up_part = lax.optimization_barrier(
        (mixed_pieces[-1], down_part, up_part)
    )
    mixed_grad = jnp.zeros((3, rows, width), LOW)
    for c in range(chunks):
        for shift, piece in enumerate(mixed_pieces[c]):
            mixed_grad = lax.dynamic_update_slice(
                mixed_grad, piece, (0, 0, ((here - shift) % ways) * own_width + c * chunk)
            )
    mixed_flat = jnp.concatenate([mixed_grad[0], mixed_grad[1], mixed_grad[2]], 1)

    widths = tuple(
        moment.shape[1] for moment in (up_moment, qkv_moment, proj_moment, down_moment.T)
    )
    quick = lax.axis_size("dp") == 8 and ways == OWNERS and all(w % 128 == 0 for w in widths)
    up_owner, qkv_owner, proj_owner, down_owner = range(OWNERS)
    pad_width = max(widths)

    def owned_of(members):
        padded = [jnp.pad(m, ((0, 0), (0, pad_width - m.shape[1]))) for m in members]
        return jnp.where(
            here < 2,
            jnp.where(here == 0, padded[0], padded[1]),
            jnp.where(here == 2, padded[2], padded[3]),
        )

    if quick:
        owned_grad = combine(
            ways,
            mm(normed_one, mixed_flat, TN).astype(LOW),
            proj_grad,
            up_part,
            down_part,
        )
    else:
        proj_part = reduce_blocks(gradient_pair(attended, branch_grad, 1), 1, other_bits())
        qkv_part = reduce_blocks(gradient_pair(normed_one, mixed_flat, 1), 1, other_bits())
        owned_grad = owned_of(
            [
                collect(up_part, up_owner, 2),
                collect(qkv_part, qkv_owner, 1),
                collect(proj_part, proj_owner, 1),
                collect(down_part, down_owner, 2),
            ]
        )

    normed_one_grad = mm(mixed_flat, qkv_weight, NT)
    input_back, gain_one_grad, offset_one_grad = norm_backward(
        normed_one_grad, unit_one, scale_one, norm_gains[0]
    )
    tokens_grad = middle_grad + input_back

    def columns(value):
        return jnp.sum(value.astype(F32), axis=0)

    vectors = jnp.stack(
        [
            gain_one_grad,
            gain_two_grad,
            offset_one_grad,
            columns(mixed_grad[0]),
            columns(mixed_grad[2]),
            columns(branch_grad),
            offset_two_grad,
            columns(upstream),
        ]
    )
    vectors = jnp.concatenate([vectors, columns(before_grad).reshape(-1, width)], 0)

    owned_moment = owned_of([up_moment, qkv_moment, proj_moment, down_moment.T])
    owned_block = (MOMENTUM * owned_moment + owned_grad.astype(F32)).astype(LOW)
    gram = mm(owned_block, owned_block, NT)
    if quick:
        sums, steps, vectors = finish(ways, gram.astype(LOW), owned_block, owned_grad, vectors, widths)
    else:
        vectors = sum_everywhere(vectors)
        iterate = orthogonal(gram_total(gram), owned_block)
        sums = share(owned_grad, widths)
        steps = share(iterate, widths)
        sums[3], steps[3] = sums[3].T, steps[3].T

    def own_columns(matrix, count):
        return lax.dynamic_slice_in_dim(matrix, me * count, count, 1).astype(F32)

    gains_sum = own_columns(vectors[:2], gains_moment.shape[1])
    biases_sum = own_columns(vectors[2:8], biases_moment.shape[1])
    upbias_count = upbias_moment.shape[0]
    upbias_sum = lax.dynamic_slice_in_dim(
        vectors[8:].reshape(-1), me * upbias_count, upbias_count, 0
    )

    def state_of(moment, grad):
        return MOMENTUM * moment + grad.astype(F32)

    up_sum, qkv_sum, proj_sum, down_sum = [g.astype(F32) for g in sums]
    qkv_state = state_of(qkv_moment, qkv_sum)
    proj_state = state_of(proj_moment, proj_sum)
    up_state = state_of(up_moment, up_sum)
    down_state = state_of(down_moment, down_sum)
    gains_state = state_of(gains_moment, gains_sum)
    biases_state = state_of(biases_moment, biases_sum)
    upbias_state = state_of(upbias_moment, upbias_sum)

    def rate_of(shape):
        return -RATE_MATRIX * math.sqrt(max(shape))

    def step_of(owner, shape):
        return rate_of(shape) * steps[owner].astype(F32)

    qkv_new = own_columns(qkv_weight, qkv_state.shape[1]) + step_of(
        qkv_owner, qkv_weight.shape
    )
    proj_new = own_columns(proj_weight, proj_state.shape[1]) + step_of(
        proj_owner, proj_weight.shape
    )
    up_new = own_columns(up_weight, up_state.shape[1]) + step_of(
        up_owner, up_weight.shape
    )
    down_count = down_state.shape[0]
    down_rows = lax.dynamic_slice_in_dim(down_weight, me * down_count, down_count, 0).astype(F32)
    down_new = down_rows + step_of(down_owner, down_weight.shape)
    gains_new = own_columns(norm_gains, gains_state.shape[1]) - RATE_VECTOR * gains_state
    biases_new = own_columns(biases, biases_state.shape[1]) - RATE_VECTOR * biases_state
    upbias_new = (
        lax.dynamic_slice_in_dim(up_bias, me * upbias_count, upbias_count, 0)
        - RATE_VECTOR * upbias_state
    )
    return (
        block_out,
        tokens_grad,
        qkv_sum,
        proj_sum,
        up_sum,
        down_sum,
        gains_sum,
        biases_sum,
        upbias_sum,
        qkv_state,
        proj_state,
        up_state,
        down_state,
        gains_state,
        biases_state,
        upbias_state,
        qkv_new,
        proj_new,
        up_new,
        down_new,
        gains_new,
        biases_new,
        upbias_new,
    )


def solution(mesh):
    rows, columns, copied = P(("dp", "seq"), None), P(None, "dp"), P()

    return jax.shard_map(
        on_device,
        mesh=mesh,
        in_specs=(
            (rows, rows)
            + (copied,) * 8
            + (columns, columns, columns, P("dp", None), columns, columns, P("dp"))
        ),
        out_specs=(
            (rows, rows)
            + (columns, columns, columns, P("dp", None), columns, columns, P("dp")) * 3
        ),
        check_vma=False,
    )
```

```python
import functools
import math

import jax
import jax.numpy as jnp
from jax import lax
from jax.experimental import pallas as pl
from jax.experimental.pallas import tpu as pltpu
from jax.sharding import PartitionSpec as P


NS_ITERS = 5


MOMENTUM = 0.9
RATE_MATRIX = 0.2
RATE_VECTOR = 0.0015
NORM_EPS = 1e-05
ORTHO_EPS = 1e-07
GELU_C = 0.7978845608028654
MASKED = -1e30
HEAD = 64
BLOCK = 512
LOW = jnp.bfloat16
F32 = jnp.float32

NT = (((1,), (1,)), ((), ()))
NN = (((1,), (0,)), ((), ()))
TN = (((0,), (0,)), ((), ()))


def mm(left, right, dims=NN):
    return lax.dot_general(left, right, dims, preferred_element_type=F32)


def stack_heads(block, groups, scale=None):
    lane = lax.broadcasted_iota(jnp.int32, block.shape, 1)
    if scale is not None:
        block = block * scale
    zero = jnp.zeros_like(block)
    return [
        jnp.where((lane >= h * HEAD) & (lane < (h + 1) * HEAD), block, zero)
        for h in range(groups)
    ]


def bias_tiles(slope_row, block, plain_ref, edge_ref, groups):
    shape = plain_ref.shape
    row = lax.broadcasted_iota(jnp.int32, shape, 0)
    col = lax.broadcasted_iota(jnp.int32, (shape[0], block), 1)
    tile = row.astype(F32) * slope_row
    plain_ref[...] = tile
    for h in range(groups):
        part = slice(h * block, (h + 1) * block)
        edge_ref[:, part] = jnp.where(row[:, part] <= col, tile[:, part], MASKED)


def forward_kernel(
    groups, block, inner, slope_ref, q_ref, k_ref, v_ref, out_ref, wide_ref, log_ref,
    plain, edge, vt, qs, acc, scores
):
    i = pl.program_id(0)
    slope = slope_ref[...]

    @pl.when(i == 0)
    def _():
        bias_tiles(slope, block, plain, edge, groups)
        vt[...] = v_ref[0].T

    for h, part in enumerate(stack_heads(q_ref[0], groups, LOW(1.0 / math.sqrt(HEAD)))):
        qs[h * block : (h + 1) * block, :] = part
    acc[...] = jnp.zeros_like(acc)
    wide = groups * block

    def score(j, peak, tile_ref):
        keys = k_ref[0, pl.ds(pl.multiple_of(j * block, block), block), :]
        x = mm(keys, qs[...], NT) + tile_ref[...] + slope * (j * block).astype(F32)
        scores[j] = x
        return jnp.maximum(peak, jnp.max(x.reshape(block // 8, 8, wide), axis=0))

    peak = lax.fori_loop(
        0, i, lambda j, p: score(j, p, plain), jnp.full((8, wide), MASKED, F32)
    )
    peak = jnp.max(score(i, peak, edge), axis=0, keepdims=True)

    def weigh(j, total):
        p = jnp.exp(scores[j] - peak)
        low = p.astype(LOW)
        for h in range(groups):
            rows = slice(h * HEAD, (h + 1) * HEAD)
            acc[rows, :] += mm(
                vt[rows, pl.ds(pl.multiple_of(j * block, block), block)],
                low[:, h * block : (h + 1) * block],
            )
        return total + jnp.sum(p.reshape(block // 8, 8, wide), axis=0)

    total = lax.fori_loop(0, i + 1, weigh, jnp.zeros((8, wide), F32))
    total = jnp.sum(total, axis=0, keepdims=True)
    logs = peak + jnp.log(total)
    inverse = 1.0 / total
    for h in range(groups):
        rows = slice(h * HEAD, (h + 1) * HEAD)
        acc[rows, :] = acc[rows, :] * inverse[:, h * block : (h + 1) * block]
        for s in range(block // inner):
            log_ref[s, :, h * inner : (h + 1) * inner] = logs[
                :, h * block + s * inner : h * block + (s + 1) * inner
            ]
    out = acc[...].T
    wide_ref[...] = out
    out_ref[...] = out.astype(LOW)


def attend_forward(qkv, slope_row, block, inner):
    length, width = qkv.shape[1:]
    groups = width // HEAD
    count = length // block
    wide = groups * block
    ratio = block // inner
    part = pl.BlockSpec((block, width), lambda i: (i, 0))
    return pl.pallas_call(
        functools.partial(forward_kernel, groups, block, inner),
        grid=(count,),
        in_specs=[
            pl.BlockSpec((1, wide), lambda i: (0, 0)),
            pl.BlockSpec((1, block, width), lambda i: (0, i, 0)),
            pl.BlockSpec((1, length, width), lambda i: (1, 0, 0)),
            pl.BlockSpec((1, length, width), lambda i: (2, 0, 0)),
        ],
        out_specs=[
            part,
            part,
            pl.BlockSpec((ratio, 1, groups * inner), lambda i: (i, 0, 0)),
        ],
        out_shape=[
            jax.ShapeDtypeStruct((length, width), LOW),
            jax.ShapeDtypeStruct((length, width), F32),
            jax.ShapeDtypeStruct((length // inner, 1, groups * inner), F32),
        ],
        scratch_shapes=[
            pltpu.VMEM((block, wide), F32),
            pltpu.VMEM((block, wide), F32),
            pltpu.VMEM((width, length), LOW),
            pltpu.VMEM((wide, width), LOW),
            pltpu.VMEM((width, block), F32),
            pltpu.VMEM((count, block, wide), F32),
        ],
        compiler_params=pltpu.CompilerParams(vmem_limit_bytes=40 << 20),
        cost_estimate=pl.CostEstimate(
            flops=16 * length * length * width,
            bytes_accessed=12 * length * width,
            transcendentals=length * length * groups,
        ),
        name="attend_forward",
    )(slope_row, qkv, qkv, qkv)


def backward_kernel(
    groups, block, slope_ref, q_ref, k_ref, v_ref, grad_ref, wide_ref, log_ref,
    out_ref, plain, edge, qs, grads, delta, dq, dk, dv, ks
):
    j = pl.program_id(0)
    count = pl.num_programs(0)
    slope = slope_ref[...]
    scale = 1.0 / math.sqrt(HEAD)

    @pl.when(j == 0)
    def _():
        bias_tiles(slope, block, plain, edge, groups)
        dq[...] = jnp.zeros_like(dq)

        def prepare(i, unused):
            rows = pl.ds(pl.multiple_of(i * block, block), block)
            grad = grad_ref[rows, :]
            for h, part in enumerate(stack_heads(q_ref[0, rows, :], groups, LOW(scale))):
                qs[i, h * block : (h + 1) * block, :] = part
            for h, part in enumerate(stack_heads(grad, groups)):
                grads[i, h * block : (h + 1) * block, :] = part
            both = (wide_ref[rows, :] * grad.astype(F32)).T
            for h in range(groups):
                delta[i, :, h * block : (h + 1) * block] = jnp.sum(
                    both[h * HEAD : (h + 1) * HEAD, :], axis=0, keepdims=True
                )
            return unused

        lax.fori_loop(0, count, prepare, 0)

    keys = k_ref[0]
    values = v_ref[0]
    for h, part in enumerate(stack_heads(keys, groups)):
        ks[h] = part
    dk[...] = jnp.zeros_like(dk)
    dv[...] = jnp.zeros_like(dv)
    shift = slope * (j * block).astype(F32)

    def visit(i, tile_ref):
        heads_q = qs[i]
        heads_grad = grads[i]
        p = jnp.exp(mm(keys, heads_q, NT) + tile_ref[...] + (shift - log_ref[i]))
        ds = p * (mm(values, heads_grad, NT) - delta[i])
        p_low = p.astype(LOW)
        ds_low = ds.astype(LOW)
        dv[...] += mm(p_low, heads_grad)
        dk[...] += mm(ds_low, heads_q)
        total = mm(ds_low[:, :block], ks[0], TN)
        for h in range(1, groups):
            total += mm(ds_low[:, h * block : (h + 1) * block], ks[h], TN)
        dq[pl.ds(pl.multiple_of(i * block, block), block), :] += total

    visit(j, edge)

    def step(i, unused):
        visit(i, plain)
        return unused

    lax.fori_loop(j + 1, count, step, 0)
    out_ref[0] = (dq[pl.ds(pl.multiple_of(j * block, block), block), :] * scale).astype(LOW)
    out_ref[1] = dk[...].astype(LOW)
    out_ref[2] = dv[...].astype(LOW)


def attend_backward(qkv, grad, attended, log_totals, slope_row, block):
    length, width = qkv.shape[1:]
    groups = width // HEAD
    count = length // block
    wide = groups * block
    whole = pl.BlockSpec((length, width), lambda i: (0, 0))
    return pl.pallas_call(
        functools.partial(backward_kernel, groups, block),
        grid=(count,),
        in_specs=[
            pl.BlockSpec((1, wide), lambda i: (0, 0)),
            pl.BlockSpec((1, length, width), lambda i: (0, 0, 0)),
            pl.BlockSpec((1, block, width), lambda i: (1, i, 0)),
            pl.BlockSpec((1, block, width), lambda i: (2, i, 0)),
            whole,
            whole,
            pl.BlockSpec((count, 1, wide), lambda i: (0, 0, 0)),
        ],
        out_specs=pl.BlockSpec((3, block, width), lambda i: (0, i, 0)),
        out_shape=jax.ShapeDtypeStruct((3, length, width), LOW),
        scratch_shapes=[
            pltpu.VMEM((block, wide), F32),
            pltpu.VMEM((block, wide), F32),
            pltpu.VMEM((count, wide, width), LOW),
            pltpu.VMEM((count, wide, width), LOW),
            pltpu.VMEM((count, 1, wide), F32),
            pltpu.VMEM((length, width), F32),
            pltpu.VMEM((block, width), F32),
            pltpu.VMEM((block, width), F32),
            pltpu.VMEM((groups, block, width), LOW),
        ],
        compiler_params=pltpu.CompilerParams(vmem_limit_bytes=40 << 20),
        cost_estimate=pl.CostEstimate(
            flops=40 * length * length * width,
            bytes_accessed=18 * length * width,
            transcendentals=length * length * groups,
        ),
        name="attend_backward",
    )(slope_row, qkv, qkv, qkv, grad, attended, log_totals)


def ortho_kernel(tile, gram_ref, block_ref, out_ref, square, square_low, cross, cross_low, state):
    size = gram_ref.shape[0]
    steps = size // tile
    trace = jnp.zeros((1, 1), F32)
    for r in range(steps):
        rows = slice(r * tile, (r + 1) * tile)
        piece = gram_ref[rows, rows].astype(F32)
        same = lax.broadcasted_iota(jnp.int32, piece.shape, 0) == lax.broadcasted_iota(
            jnp.int32, piece.shape, 1
        )
        picked = jnp.where(same, piece, 0.0)
        trace += jnp.sum(jnp.sum(picked, axis=1, keepdims=True), axis=0, keepdims=True)
    factor = 1.0 / (jnp.sqrt(trace) + ORTHO_EPS)

    def load(r, unused):
        rows = pl.ds(pl.multiple_of(r * tile, tile), tile)
        first = gram_ref[rows, :].astype(F32) * factor * factor
        square[rows, :] = first
        square_low[rows, :] = first.astype(LOW)
        state[rows, :] = block_ref[rows, :].astype(F32) * factor
        out_ref[rows, :] = state[rows, :].astype(LOW)
        return unused

    lax.fori_loop(0, steps, load, 0)

    def advance():
        for r in range(steps):
            rows = slice(r * tile, (r + 1) * tile)
            state[rows, :] = 2.0 * state[rows, :] - mm(square_low[rows, :], out_ref[...])

    def settle():
        out_ref[...] = state[...].astype(LOW)

    def iterate(t, unused):
        advance()
        for r in range(steps):
            rows = slice(r * tile, (r + 1) * tile)
            value = 2.0 * square[rows, :] - mm(square_low[rows, :], square_low[...])
            cross[rows, :] = value
            cross_low[rows, :] = value.astype(LOW)
        settle()
        for r in range(steps):
            rows = slice(r * tile, (r + 1) * tile)
            square[rows, :] = 2.0 * cross[rows, :] - mm(cross_low[rows, :], square_low[...])
        square_low[...] = square[...].astype(LOW)
        return unused

    lax.fori_loop(0, NS_ITERS - 1, iterate, 0)
    advance()
    settle()


def orthogonal(gram, block):
    size, width = block.shape
    tile = min(256, size)
    return pl.pallas_call(
        functools.partial(ortho_kernel, tile),
        out_shape=jax.ShapeDtypeStruct((size, width), LOW),
        in_specs=[pl.BlockSpec(memory_space=pltpu.VMEM)] * 2,
        out_specs=pl.BlockSpec(memory_space=pltpu.VMEM),
        scratch_shapes=[
            pltpu.VMEM((size, size), F32),
            pltpu.VMEM((size, size), LOW),
            pltpu.VMEM((size, size), F32),
            pltpu.VMEM((size, size), LOW),
            pltpu.VMEM((size, width), F32),
        ],
        compiler_params=pltpu.CompilerParams(vmem_limit_bytes=40 << 20),
        cost_estimate=pl.CostEstimate(
            flops=16 * size**3 + 10 * size * size * width, bytes_accessed=4 * size * size, transcendentals=0
        ),
        name="orthogonal",
    )(gram, block)


def swap(value, axis, bit):
    return lax.ppermute(value, axis, [(i, i ^ bit) for i in range(lax.axis_size(axis))])


def pick(buffer, axis, count, stride, choice):
    size = buffer.shape[axis] // count
    run = stride * size
    parts = [
        lax.dynamic_slice_in_dim(buffer, 2 * i * run + choice * run, run, axis)
        for i in range(count // (2 * stride))
    ]
    return parts[0] if len(parts) == 1 else jnp.concatenate(parts, axis)


def reduce_blocks(buffer, axis, held):
    me = lax.axis_index("dp")
    count = 1 << len(held)

    def ladder(piece, order):
        left = list(held)
        blocks = count
        for bit in order:
            stride = 1 << (len(left) - 1 - left.index(bit))
            mine = (me // bit) % 2
            arrived = swap(pick(piece, axis, blocks, stride, 1 - mine), "dp", bit)
            kept = pick(piece, axis, blocks, stride, mine)
            piece = (kept.astype(F32) + arrived.astype(F32)).astype(LOW)
            left.remove(bit)
            blocks //= 2
        return piece

    if not held:
        return buffer
    other = 1 - axis
    half = buffer.shape[other] // 2
    ascending = sorted(held)
    orders = (ascending, ascending[1:] + ascending[:1])
    pieces = [
        ladder(lax.slice_in_dim(buffer, k * half, (k + 1) * half, axis=other), orders[k])
        for k in range(2)
    ]
    return jnp.concatenate(pieces, other)


def gradient_pair(left, right, axis):
    size = lax.axis_size("dp")
    mine = lax.axis_index("dp") % 2

    def product(choice):
        if axis == 1:
            return mm(left, pick(right, 1, size, 1, choice), TN)
        return mm(pick(left, 1, size, 1, choice), right, TN)

    leaving = product(1 - mine).astype(LOW)
    arrived = swap(leaving, "dp", 1)
    return (product(mine) + arrived.astype(F32)).astype(LOW)


def other_bits():
    return [1 << b for b in range(1, lax.axis_size("dp").bit_length() - 1)][::-1]


def collect(value, owner, pieces):
    size = lax.axis_size("seq")
    hops = []
    left = [(i, i - 1) for i in range(size - 1, owner, -1)]
    right = [(i, i + 1) for i in range(owner)]
    while left or right:
        hops.append(left[:1] + right[:1])
        left, right = left[1:], right[1:]
        if len(hops[-1]) == 2 and hops[-1][0][1] == hops[-1][1][1]:
            hops[-1:] = [hops[-1][:1], hops[-1][1:]]
    rows = value.shape[0] // pieces
    parts = []
    for k in range(pieces):
        part = value[k * rows : (k + 1) * rows]
        for hop in hops:
            arrived = lax.ppermute(part, "seq", hop)
            part = (part.astype(F32) + arrived.astype(F32)).astype(LOW)
        parts.append(part)
    return parts[0] if pieces == 1 else jnp.concatenate(parts, 0)


def share(own, widths):
    size = lax.axis_size("seq")
    here = lax.axis_index("seq")
    found = {0: own}
    for way in (1, -1):
        moving = own
        for distance in range(1, size):
            pairs = [
                (i, i + way) for i in range(size) if 0 <= i + way < size and 0 <= i + way - way * distance < size
            ]
            moving = lax.ppermute(moving, "seq", pairs)
            found[way * distance] = moving
    result = []
    for m, width in enumerate(widths):
        value = own[:, :width]
        for d in range(size):
            if d != m:
                value = jnp.where(here == d, found[d - m][:, :width], value)
        result.append(value)
    return result


def gram_total(gram):
    me = lax.axis_index("dp")
    size = lax.axis_size("dp")
    bits = [1 << b for b in range(size.bit_length() - 1)]

    def ladder(piece, order):
        sizes = []
        for bit in order:
            half = piece.shape[0] // 2
            mine = (me // bit) % 2
            arrived = swap(lax.dynamic_slice_in_dim(piece, (1 - mine) * half, half, 0), "dp", bit)
            kept = lax.dynamic_slice_in_dim(piece, mine * half, half, 0)
            piece = (kept.astype(F32) + arrived.astype(F32)).astype(LOW)
            sizes.append(half)
        for bit, half in zip(reversed(order), reversed(sizes)):
            mine = (me // bit) % 2
            arrived = swap(piece, "dp", bit)
            first = jnp.where(mine == 0, piece, arrived)
            second = jnp.where(mine == 0, arrived, piece)
            piece = jnp.concatenate([first, second], 0)
        return piece

    half = gram.shape[1] // 2
    low = gram.astype(LOW)
    return jnp.concatenate(
        [
            ladder(low[:, :half], bits),
            ladder(low[:, half:], bits[:1] + bits[2:] + bits[1:2]),
        ],
        1,
    )


def sum_everywhere(value):
    for axis in ("dp", "seq"):
        bit = 1
        while bit < lax.axis_size(axis):
            value = value + swap(value, axis, bit)
            bit *= 2
    return value


def depart(source, take):
    size = lax.axis_size("seq")
    here = lax.axis_index("seq")
    pieces = []
    for shift in range(size):
        piece = take(source, (here + shift) % size)
        if shift:
            piece = lax.ppermute(piece, "seq", [(i, (i + shift) % size) for i in range(size)])
        pieces.append(piece)
    return pieces


def arrange(pieces, place, shape):
    size = lax.axis_size("seq")
    here = lax.axis_index("seq")
    result = jnp.zeros(shape, LOW)
    for shift, piece in enumerate(pieces):
        result = lax.dynamic_update_slice(result, piece, place((here - shift) % size))
    return result


MESH = pl.DeviceIdType.MESH
TRIPS = 8
OWNERS = 4


def greet(axes_partners):
    barrier = pltpu.get_barrier_semaphore()
    count = 0
    for axis, partner, real in axes_partners:

        def tell(axis=axis, partner=partner):
            pl.semaphore_signal(barrier, inc=1, device_id={axis: partner}, device_id_type=MESH)

        if real is None:
            tell()
            count = count + 1
        else:
            pl.when(real)(tell)
            count = count + real.astype(jnp.int32)
    pl.semaphore_wait(barrier, count)


def plane():
    me = lax.axis_index("dp")
    core, x, y = lax.rem(me, 2), lax.rem(me // 2, 2), me // 4
    flip = lambda bit: 1 - bit
    return (
        (core, x, y),
        (
            4 * y + 2 * x + flip(core),
            4 * y + 2 * flip(x) + core,
            4 * flip(y) + 2 * x + core,
        ),
    )


def combine_kernel(
    ways, wide_q, wide_p, qkv_ref, proj_ref, up_ref, down_ref, out_ref,
    one, send_two, two, send_three, three, final, from_left, from_right, relay,
    s_one, r_one, s_two, r_two, s_three, r_three, s_left, r_left, s_right, r_right,
):
    (core, x, y), partners = plane()
    z = lax.axis_index("seq")
    size = up_ref.shape[0]
    half = size // 2
    chunks = TRIPS
    step = size // chunks
    width = wide_q + wide_p
    greet(
        [("dp", p, None) for p in partners]
        + [("seq", jnp.maximum(z - 1, 0), z > 0), ("seq", jnp.minimum(z + 1, ways - 1), z < ways - 1)]
    )

    def remote(src, dst, send, recv, axis, target):
        return pltpu.make_async_remote_copy(
            src_ref=src, dst_ref=dst, send_sem=send, recv_sem=recv,
            device_id={axis: target}, device_id_type=MESH,
        )

    owned = ((0, width), (0, wide_q), (wide_q, wide_p), (0, width))

    def source(m, k):
        rows = pl.ds(k * step, step)
        lanes = pl.ds(*owned[m])
        return (up_ref, final, final, down_ref)[m].at[rows, lanes]

    def hop(m, k, left, src):
        lanes = pl.ds(*owned[m])
        box, send, recv = (from_right, s_left, r_left) if left else (from_left, s_right, r_right)
        slot = m
        return remote(
            src, box.at[slot, pl.ds(k * step, step), lanes], send.at[m, k], recv.at[m, k],
            "seq", jnp.maximum(z - 1, 0) if left else jnp.minimum(z + 1, ways - 1),
        )

    def relay_src(m, k):
        return relay.at[m, pl.ds(k * step, step), pl.ds(*owned[m])]

    def begin(m, parts):
        for k in parts:
            if m < ways - 1:
                @pl.when(z == ways - 1)
                def _():
                    hop(m, k, True, source(m, k)).start()
            if m > 0:
                @pl.when(z == 0)
                def _():
                    hop(m, k, False, source(m, k)).start()

    def pass_on(m, k, turn):
        lanes = pl.ds(*owned[m])
        strip = 64

        def added(box):
            def body(i, unused):
                part = pl.ds(pl.multiple_of(k * step + i * strip, strip), strip)
                src = (up_ref, final, final, down_ref)[m]
                relay[m, part, lanes] = (
                    src[part, lanes].astype(F32) + box[m, part, lanes].astype(F32)
                ).astype(LOW)
                return unused

            lax.fori_loop(0, step // strip, body, 0)

        if m < ways - 2:
            @pl.when((z > m) & (z == ways - 1 - turn))
            def _():
                hop(m, k, True, source(m, k)).wait_recv()
                added(from_right)
                hop(m, k, True, relay_src(m, k)).start()
        if m > 1:
            @pl.when((z < m) & (z == turn))
            def _():
                hop(m, k, False, source(m, k)).wait_recv()
                added(from_left)
                hop(m, k, False, relay_src(m, k)).start()

    def settle(m, k):
        lanes = pl.ds(*owned[m])
        strip = 64

        @pl.when(z == m)
        def _():
            if m < ways - 1:
                hop(m, k, True, source(m, k)).wait_recv()
            if m > 0:
                hop(m, k, False, source(m, k)).wait_recv()

            def body(i, unused):
                part = pl.ds(pl.multiple_of(k * step + i * strip, strip), strip)
                src = (up_ref, final, final, down_ref)[m]
                total = src[part, lanes].astype(F32)
                if m < ways - 1:
                    total += from_right[m, part, lanes].astype(F32)
                if m > 0:
                    total += from_left[m, part, lanes].astype(F32)
                width_m = owned[m][1]
                out_ref[part, pl.ds(0, width_m)] = total.astype(LOW)
                if width_m < width:
                    out_ref[part, pl.ds(width_m, width - width_m)] = jnp.zeros(
                        (strip, width - width_m), LOW
                    )
                return unused

            lax.fori_loop(0, step // strip, body, 0)

    begin(0, range(chunks))
    begin(3, range(chunks))

    strip = 64

    def own(h, block, start, rows):
        part = pl.ds(pl.multiple_of(h * half + start, strip), rows)
        q = qkv_ref[part, pl.ds(pl.multiple_of(block * wide_q, 128), wide_q)]
        p = proj_ref[part, pl.ds(pl.multiple_of(block * wide_p, 128), wide_p)]
        return jnp.concatenate([q, p], axis=1).astype(F32)

    def first(h, k):
        block = 2 * k + (1 - core)
        rows = pl.ds(h * half, half)
        return [
            remote(
                qkv_ref.at[rows, pl.ds(pl.multiple_of(block * wide_q, 128), wide_q)],
                one.at[h, k, :, pl.ds(0, wide_q)], s_one.at[h, k, 0], r_one.at[h, k, 0],
                "dp", partners[0],
            ),
            remote(
                proj_ref.at[rows, pl.ds(pl.multiple_of(block * wide_p, 128), wide_p)],
                one.at[h, k, :, pl.ds(wide_q, wide_p)], s_one.at[h, k, 1], r_one.at[h, k, 1],
                "dp", partners[0],
            ),
        ]

    go = [[(2 * j + (1 - x)) for j in range(2)], [(2 * (1 - y) + j) for j in range(2)]]
    stay = [[(2 * j + x) for j in range(2)], [(2 * y + j) for j in range(2)]]
    for group in (go, stay):
        for j in range(2):
            for h in range(2):
                for copy in first(h, group[h][j]):
                    copy.start()

    def second(h, j):
        return remote(send_two.at[h, j], two.at[h, j], s_two.at[h, j], r_two.at[h, j],
                      "dp", partners[1 + h])

    for j in range(2):
        for h in range(2):
            k = go[h][j]
            for copy in first(h, k):
                copy.wait_recv()

            def body(i, unused):
                part = pl.ds(pl.multiple_of(i * strip, strip), strip)
                value = own(h, 2 * k + core, i * strip, strip) + one[h, k, part, :].astype(F32)
                send_two[h, j, part, :] = value.astype(LOW)
                return unused

            lax.fori_loop(0, half // strip, body, 0)
            second(h, j).start()
    for k in range(chunks):
        pass_on(0, k, 1)
        pass_on(3, k, 1)

    def third(h):
        return remote(send_three.at[h], three.at[h], s_three.at[h], r_three.at[h],
                      "dp", partners[2 - h])

    mine = [y, x]
    for h in range(2):
        for j in range(2):
            for copy in first(h, stay[h][j]):
                copy.wait_recv()
        for j in range(2):
            second(h, j).wait_recv()
        j = 1 - mine[h]
        k = 2 * j + x if h == 0 else 2 * y + j

        def body(i, unused):
            part = pl.ds(pl.multiple_of(i * strip, strip), strip)
            value = (
                own(h, 2 * k + core, i * strip, strip)
                + one[h, k, part, :].astype(F32)
                + two[h, j, part, :].astype(F32)
            )
            send_three[h, part, :] = value.astype(LOW)
            return unused

        lax.fori_loop(0, half // strip, body, 0)
        third(h).start()
    for k in range(chunks):
        pass_on(0, k, 2)
        pass_on(3, k, 2)
    for h in range(2):
        third(h).wait_recv()
        j = mine[h]
        k = 2 * y + x

        def body(i, unused):
            part = pl.ds(pl.multiple_of(i * strip, strip), strip)
            value = (
                own(h, 2 * k + core, i * strip, strip)
                + one[h, k, part, :].astype(F32)
                + two[h, j, part, :].astype(F32)
                + three[h, part, :].astype(F32)
            )
            final[pl.ds(pl.multiple_of(h * half + i * strip, strip), strip), :] = value.astype(LOW)
            return unused

        lax.fori_loop(0, half // strip, body, 0)
        parts = range(h * chunks // 2, (h + 1) * chunks // 2)
        begin(1, parts)
        begin(2, parts)
    for k in range(chunks):
        pass_on(1, k, 1)
        pass_on(2, k, 1)
    for m in (0, 3, 1, 2):
        for k in range(chunks):
            settle(m, k)

    for h in range(2):
        for k in range(4):
            for copy in first(h, k):
                copy.wait_send()
        for j in range(2):
            second(h, j).wait_send()
        third(h).wait_send()
    for m in range(OWNERS):
        for k in range(chunks):
            if m < ways - 1:
                @pl.when(z > m)
                def _():
                    hop(m, k, True, source(m, k)).wait_send()
            if m > 0:
                @pl.when(z < m)
                def _():
                    hop(m, k, False, source(m, k)).wait_send()


def combine(ways, qkv, proj, up, down):
    size, width = up.shape
    wide_q, wide_p = qkv.shape[1] // 8, proj.shape[1] // 8
    half = size // 2
    vmem = pl.BlockSpec(memory_space=pltpu.VMEM)
    dma = pltpu.SemaphoreType.DMA
    return pl.pallas_call(
        functools.partial(combine_kernel, ways, wide_q, wide_p),
        out_shape=jax.ShapeDtypeStruct((size, width), LOW),
        in_specs=[vmem] * 4,
        out_specs=vmem,
        scratch_shapes=[
            pltpu.VMEM((2, 4, half, width), LOW),
            pltpu.VMEM((2, 2, half, width), LOW),
            pltpu.VMEM((2, 2, half, width), LOW),
            pltpu.VMEM((2, half, width), LOW),
            pltpu.VMEM((2, half, width), LOW),
            pltpu.VMEM((size, width), LOW),
            pltpu.VMEM((OWNERS, size, width), LOW),
            pltpu.VMEM((OWNERS, size, width), LOW),
            pltpu.VMEM((OWNERS, size, width), LOW),
            dma((2, 4, 2)), dma((2, 4, 2)), dma((2, 2)), dma((2, 2)), dma((2,)), dma((2,)),
            dma((OWNERS, TRIPS)), dma((OWNERS, TRIPS)), dma((OWNERS, TRIPS)), dma((OWNERS, TRIPS)),
        ],
        compiler_params=pltpu.CompilerParams(
            collective_id=1, has_side_effects=True, vmem_limit_bytes=56 << 20
        ),
        cost_estimate=pl.CostEstimate(flops=50_000_000_000, bytes_accessed=1 << 23, transcendentals=0),
        name="combine",
    )(qkv, proj, up, down)


def finish_kernel(
    ways, widths, chunks, gram_ref, block_ref, grad_ref, vector_ref,
    g0, g1, g2, g3, y0, y1, y2, y3, total_ref,
    one, send_two, two, send_three, three, whole,
    square, square_low, cross, cross_low, state, low, g_down, y_down, vectors, arrived,
    s_one, r_one, s_two, r_two, s_three, r_three, s_back, r_back,
    gs_left, gr_left, gs_right, gr_right, ys_left, yr_left, ys_right, yr_right, s_own, s_vec, r_vec,
):
    (core, x, y), partners = plane()
    z = lax.axis_index("seq")
    across = lax.rem(z + 2, 4)
    beside = z + 1 - 2 * lax.rem(z, 2)
    size = gram_ref.shape[0]
    rows = size // 8
    half = size // 2
    step = size // chunks
    greet(
        [("dp", p, None) for p in partners]
        + [
            ("seq", across, None),
            ("seq", jnp.maximum(z - 1, 0), z > 0),
            ("seq", jnp.minimum(z + 1, ways - 1), z < ways - 1),
        ]
    )

    class Trip:
        def __init__(self, own, outs, s_left, r_left, s_right, r_right, local):
            self.own, self.outs, self.local = own, outs, local
            self.left, self.right = (s_left, r_left), (s_right, r_right)

        def hop(self, m, k, left, relayed):
            part = pl.ds(pl.multiple_of(k * step, step), step)
            place = self.outs[m].at[part, :]
            src = place if relayed else self.own.at[part, pl.ds(0, widths[m])]
            send, recv = self.left if left else self.right
            return pltpu.make_async_remote_copy(
                src_ref=src, dst_ref=place, send_sem=send.at[m, k], recv_sem=recv.at[m, k],
                device_id={"seq": jnp.maximum(z - 1, 0) if left else jnp.minimum(z + 1, ways - 1)},
                device_id_type=MESH,
            )

        def copy(self, m):
            return pltpu.make_async_copy(
                self.own.at[:, pl.ds(0, widths[m])], self.outs[m], s_own.at[self.local]
            )

        def begin(self):
            for m in range(OWNERS):
                @pl.when(z == m)
                def _():
                    for k in range(chunks):
                        if m < ways - 1:
                            self.hop(m, k, False, False).start()
                        if m > 0:
                            self.hop(m, k, True, False).start()
                    self.copy(m).start()

        def relay(self, distance, k):
            for m in range(OWNERS):
                if m + distance < ways:
                    @pl.when(z == m + distance)
                    def _():
                        self.hop(m, k, False, True).wait_recv()
                        if m + distance < ways - 1:
                            self.hop(m, k, False, True).start()
                if m - distance >= 0:
                    @pl.when(z == m - distance)
                    def _():
                        self.hop(m, k, True, True).wait_recv()
                        if m - distance > 0:
                            self.hop(m, k, True, True).start()

        def end(self):
            for m in range(OWNERS):
                @pl.when(z == m)
                def _():
                    self.copy(m).wait()

                for k in range(chunks):
                    @pl.when((z >= m) & (z < ways - 1))
                    def _():
                        self.hop(m, k, False, True).wait_send()

                    @pl.when((z <= m) & (z > 0))
                    def _():
                        self.hop(m, k, True, True).wait_send()

    grads = Trip(grad_ref, (g0, g1, g2, g_down), gs_left, gr_left, gs_right, gr_right, 0)
    steps = Trip(low, (y0, y1, y2, y_down), ys_left, yr_left, ys_right, yr_right, 1)
    grads.begin()

    def vector_copy(i):
        source = vector_ref if i == 0 else vectors.at[i - 1]
        target = (
            [{"dp": p} for p in partners] + [{"seq": beside}, {"seq": across}]
        )[i]
        return pltpu.make_async_remote_copy(
            src_ref=source, dst_ref=arrived.at[i], send_sem=s_vec.at[i], recv_sem=r_vec.at[i],
            device_id=target, device_id_type=MESH,
        )

    def vector_step(i):
        vector_copy(i).wait_recv()
        value = (vector_ref[...] if i == 0 else vectors[i - 1]) + arrived[i]
        if i < 4:
            vectors[i] = value
            vector_copy(i + 1).start()
        else:
            total_ref[...] = value

    vector_copy(0).start()

    def remote(src, dst, send, recv, target):
        return pltpu.make_async_remote_copy(
            src_ref=src, dst_ref=dst, send_sem=send, recv_sem=recv,
            device_id={"dp": target}, device_id_type=MESH,
        )

    def block(ref, h, d):
        return ref.at[pl.ds(pl.multiple_of(d * rows, rows), rows), pl.ds(h * half, half)]

    def own(h, d):
        return gram_ref[
            pl.ds(pl.multiple_of(d * rows, rows), rows), pl.ds(h * half, half)
        ].astype(F32)

    def first(h, k):
        return remote(block(gram_ref, h, 2 * k + 1 - core), one.at[h, k], s_one.at[h, k],
                      r_one.at[h, k], partners[0])

    go = [[(2 * j + (1 - x)) for j in range(2)], [(2 * (1 - y) + j) for j in range(2)]]
    stay = [[(2 * j + x) for j in range(2)], [(2 * y + j) for j in range(2)]]
    for group in (go, stay):
        for j in range(2):
            for h in range(2):
                first(h, group[h][j]).start()

    def second(h, j):
        return remote(send_two.at[h, j], two.at[h, j], s_two.at[h, j], r_two.at[h, j], partners[1 + h])

    for j in range(2):
        for h in range(2):
            k = go[h][j]
            first(h, k).wait_recv()
            send_two[h, j] = (own(h, 2 * k + core) + one[h, k].astype(F32)).astype(LOW)
            second(h, j).start()
    vector_step(0)

    def third(h):
        return remote(send_three.at[h], three.at[h], s_three.at[h], r_three.at[h], partners[2 - h])

    mine = [y, x]
    for h in range(2):
        for j in range(2):
            first(h, stay[h][j]).wait_recv()
        for j in range(2):
            second(h, j).wait_recv()
        j = 1 - mine[h]
        k = 2 * j + x if h == 0 else 2 * y + j
        send_three[h] = (
            own(h, 2 * k + core) + one[h, k].astype(F32) + two[h, j].astype(F32)
        ).astype(LOW)
        third(h).start()
    vector_step(1)
    for c in range(chunks // 4):
        grads.relay(1, c)

    def back(h, stage, d):
        target = (partners[2 - h], partners[1 + h], partners[0])[stage]
        place = block(whole, h, d)
        slot = (0, 1, 3)[stage]
        return lambda i: remote(place, place, s_back.at[h, slot + i], r_back.at[h, slot + i], target)

    k = 2 * y + x
    for h in range(2):
        third(h).wait_recv()
        value = (
            own(h, 2 * k + core)
            + one[h, k].astype(F32)
            + two[h, mine[h]].astype(F32)
            + three[h].astype(F32)
        ).astype(LOW)
        d = 2 * k + core
        whole[pl.ds(pl.multiple_of(d * rows, rows), rows), pl.ds(h * half, half)] = value
        for stage in range(3):
            back(h, stage, d)(0).start()
    vector_step(2)
    k_next = [2 * (1 - y) + x, 2 * y + (1 - x)]
    for h in range(2):
        d = 2 * k_next[h] + core
        back(h, 0, d)(0).wait_recv()
        back(h, 1, d)(1).start()
        back(h, 2, d)(1).start()
    for c in range(chunks // 4, chunks // 2):
        grads.relay(1, c)
    for h in range(2):
        for i in range(2):
            if h == 0:
                kk = 2 * (y if i == 0 else 1 - y) + (1 - x)
            else:
                kk = 2 * (1 - y) + (x if i == 0 else 1 - x)
            d = 2 * kk + core
            back(h, 1, d)(i).wait_recv()
            back(h, 2, d)(2 + i).start()
    for h in range(2):
        for i, kk in enumerate(
            (
                2 * y + x,
                k_next[h],
                2 * y + (1 - x) if h == 0 else 2 * (1 - y) + x,
                2 * (1 - y) + (1 - x),
            )
        ):
            back(h, 2, 2 * kk + 1 - core)(i).wait_recv()
    vector_step(3)
    for c in range(chunks // 2, chunks):
        grads.relay(1, c)

    tile = 256
    count = size // tile
    trace = jnp.zeros((1, 1), F32)
    for r in range(count):
        part = slice(r * tile, (r + 1) * tile)
        piece = whole[part, part].astype(F32)
        same = lax.broadcasted_iota(jnp.int32, piece.shape, 0) == lax.broadcasted_iota(
            jnp.int32, piece.shape, 1
        )
        picked = jnp.where(same, piece, 0.0)
        trace += jnp.sum(jnp.sum(picked, axis=1, keepdims=True), axis=0, keepdims=True)
    factor = 1.0 / (jnp.sqrt(trace) + ORTHO_EPS)

    def load(r, unused):
        part = pl.ds(pl.multiple_of(r * tile, tile), tile)
        begun = whole[part, :].astype(F32) * factor * factor
        square[part, :] = begun
        square_low[part, :] = begun.astype(LOW)
        state[part, :] = block_ref[part, :].astype(F32) * factor
        low[part, :] = state[part, :].astype(LOW)
        return unused

    lax.fori_loop(0, count, load, 0)

    def advance():
        for r in range(count):
            part = slice(r * tile, (r + 1) * tile)
            state[part, :] = 2.0 * state[part, :] - mm(square_low[part, :], low[...])

    def iterate(t, unused):
        advance()
        for r in range(count):
            part = slice(r * tile, (r + 1) * tile)
            value = 2.0 * square[part, :] - mm(square_low[part, :], square_low[...])
            cross[part, :] = value
            cross_low[part, :] = value.astype(LOW)
        low[...] = state[...].astype(LOW)
        for r in range(count):
            part = slice(r * tile, (r + 1) * tile)
            square[part, :] = 2.0 * cross[part, :] - mm(cross_low[part, :], square_low[...])
        square_low[...] = square[...].astype(LOW)
        for c in range(chunks // 4):
            grads.relay(2, t * (chunks // 4) + c)
        return unused

    lax.fori_loop(0, NS_ITERS - 1, iterate, 0)
    advance()
    low[...] = state[...].astype(LOW)

    steps.begin()
    vector_step(4)
    for c in range(chunks):
        grads.relay(3, c)
    grads.end()

    def turn(ref, out):
        for c in range(size // 256):
            out[:, c * 256 : (c + 1) * 256] = ref[c * 256 : (c + 1) * 256, :].T

    for distance in range(1, ways):
        for c in range(chunks):
            steps.relay(distance, c)
        if distance == 2:
            turn(g_down, g3)
    steps.end()
    turn(y_down, y3)

    for h in range(2):
        for j in range(4):
            first(h, j).wait_send()
        for j in range(2):
            second(h, j).wait_send()
        third(h).wait_send()
        d = 2 * k + core
        back(h, 0, d)(0).wait_send()
        for i in range(2):
            back(h, 1, d)(i).wait_send()
        for i in range(4):
            back(h, 2, d)(i).wait_send()
    for i in range(5):
        vector_copy(i).wait_send()


def finish(ways, gram, block, grad, vectors, widths):
    size, width = block.shape
    rows, half = size // 8, size // 2
    chunks = 8
    vmem = pl.BlockSpec(memory_space=pltpu.VMEM)
    dma = pltpu.SemaphoreType.DMA
    shapes = [
        jax.ShapeDtypeStruct((size, w) if m < OWNERS - 1 else (w, size), LOW)
        for m, w in enumerate(widths)
    ]
    down = pltpu.VMEM((size, widths[-1]), LOW)
    result = pl.pallas_call(
        functools.partial(finish_kernel, ways, widths, chunks),
        out_shape=shapes * 2 + [jax.ShapeDtypeStruct(vectors.shape, F32)],
        in_specs=[vmem] * 4,
        out_specs=[vmem] * 9,
        scratch_shapes=[
            pltpu.VMEM((2, 4, rows, half), LOW),
            pltpu.VMEM((2, 2, rows, half), LOW),
            pltpu.VMEM((2, 2, rows, half), LOW),
            pltpu.VMEM((2, rows, half), LOW),
            pltpu.VMEM((2, rows, half), LOW),
            pltpu.VMEM((size, size), LOW),
            pltpu.VMEM((size, size), F32),
            pltpu.VMEM((size, size), LOW),
            pltpu.VMEM((size, size), F32),
            pltpu.VMEM((size, size), LOW),
            pltpu.VMEM((size, width), F32),
            pltpu.VMEM((size, width), LOW),
            down,
            down,
            pltpu.VMEM((4,) + vectors.shape, F32),
            pltpu.VMEM((5,) + vectors.shape, F32),
            dma((2, 4)), dma((2, 4)), dma((2, 2)), dma((2, 2)), dma((2,)), dma((2,)),
            dma((2, 7)), dma((2, 7)),
        ]
        + [dma((OWNERS, chunks))] * 8
        + [dma((2,)), dma((5,)), dma((5,))],
        compiler_params=pltpu.CompilerParams(
            collective_id=2, has_side_effects=True, vmem_limit_bytes=56 << 20
        ),
        cost_estimate=pl.CostEstimate(
            flops=80_000_000_000, bytes_accessed=1 << 24, transcendentals=0
        ),
        name="finish",
    )(gram, block, grad, vectors)
    return result[:4], result[4:8], result[8]


def norm_forward(values, gain_row, offset):
    center = values - jnp.mean(values, axis=-1, keepdims=True)
    inv_scale = lax.rsqrt(jnp.mean(center * center, axis=-1, keepdims=True) + NORM_EPS)
    unit_values = center * inv_scale
    return (unit_values * gain_row + offset, unit_values, inv_scale)


def norm_backward(upstream, unit_values, inv_scale, gain_row):
    scaled = upstream * gain_row
    inner_sum = jnp.mean(scaled * unit_values, axis=-1, keepdims=True)
    input_grad = inv_scale * (
        scaled - jnp.mean(scaled, axis=-1, keepdims=True) - unit_values * inner_sum
    )
    return (input_grad, jnp.sum(upstream * unit_values, axis=0), jnp.sum(upstream, axis=0))


def gelu_both(values):
    square = values * values
    tangent = jnp.tanh(GELU_C * (values + 0.044715 * square * values))
    slope = 0.5 * (1.0 + tangent) + 0.5 * values * (1.0 - tangent * tangent) * GELU_C * (
        1.0 + 3.0 * 0.044715 * square
    )
    return 0.5 * values * (1.0 + tangent), slope


def on_device(
    tokens,
    cotangent,
    qkv_weight,
    proj_weight,
    up_weight,
    down_weight,
    norm_gains,
    biases,
    up_bias,
    head_slopes,
    qkv_moment,
    proj_moment,
    up_moment,
    down_moment,
    gains_moment,
    biases_moment,
    upbias_moment,
):
    rows, width = tokens.shape
    ways = lax.axis_size("seq")
    here = lax.axis_index("seq")
    me = lax.axis_index("dp")
    length = rows * ways
    own_width = width // ways
    chunks = 2
    chunk = own_width // chunks
    chunk_heads = chunk // HEAD
    own_slopes = lax.dynamic_slice_in_dim(
        head_slopes, here * (own_width // HEAD), own_width // HEAD, 0
    )
    chunk_slopes = [own_slopes[c * chunk_heads : (c + 1) * chunk_heads] for c in range(chunks)]

    inputs = tokens.astype(F32)
    normed_one, unit_one, scale_one = norm_forward(inputs, norm_gains[0], biases[0])
    normed_one = normed_one.astype(LOW)
    bias_row = jnp.concatenate([biases[1], jnp.zeros_like(biases[1]), biases[2]])
    mixed = (mm(normed_one, qkv_weight) + bias_row).astype(LOW)

    def take_mixed(c):
        def take(source, d):
            return jnp.stack(
                [
                    lax.dynamic_slice_in_dim(
                        source, part * width + d * own_width + c * chunk, chunk, 1
                    )
                    for part in range(3)
                ]
            )

        return take

    qkv_pieces = [depart(mixed, take_mixed(c)) for c in range(chunks)]
    widths = tuple(
        moment.shape[1] for moment in (up_moment, qkv_moment, proj_moment, down_moment.T)
    )
    quick = lax.axis_size("dp") == 8 and ways == OWNERS and all(w % 128 == 0 for w in widths)
    up_owner, qkv_owner, proj_owner, down_owner = range(OWNERS)
    pad_width = max(widths)

    def owned_of(members):
        padded = [jnp.pad(m, ((0, 0), (0, pad_width - m.shape[1]))) for m in members]
        return jnp.where(
            here < 2,
            jnp.where(here == 0, padded[0], padded[1]),
            jnp.where(here == 2, padded[2], padded[3]),
        )

    owned_moment = owned_of([up_moment, qkv_moment, proj_moment, down_moment.T])
    qkv_pieces[0], owned_moment = lax.optimization_barrier((qkv_pieces[0], owned_moment))
    qkv = []
    attended = jnp.zeros((rows, width), LOW)
    kept = []
    for c in range(chunks):
        if c:
            qkv_pieces[c], out = lax.optimization_barrier((qkv_pieces[c], out))
        qkv.append(arrange(qkv_pieces[c], lambda d: (0, d * rows, 0), (3, length, chunk)))
        out, wide, log_totals = attend_forward(
            qkv[c], jnp.repeat(chunk_slopes[c], BLOCK)[None], BLOCK, BLOCK
        )
        kept.append((wide, log_totals))
        for shift in range(ways):
            piece = lax.dynamic_slice_in_dim(out, ((here + shift) % ways) * rows, rows, 0)
            if shift:
                piece = lax.ppermute(piece, "seq", [(i, (i + shift) % ways) for i in range(ways)])
            attended = lax.dynamic_update_slice(
                attended, piece, (0, ((here - shift) % ways) * own_width + c * chunk)
            )

    middle = inputs + mm(attended, proj_weight) + biases[3]
    normed_two, unit_two, scale_two = norm_forward(middle, norm_gains[1], biases[4])
    normed_two = normed_two.astype(LOW)
    before = mm(normed_two, up_weight) + up_bias
    hidden, slope = gelu_both(before)
    hidden = hidden.astype(LOW)
    upstream = cotangent.astype(F32)
    hidden_grad = mm(cotangent, down_weight, NT)
    before_grad = (hidden_grad * slope).astype(LOW)
    normed_two_grad = mm(before_grad, up_weight, NT)
    middle_back, gain_two_grad, offset_two_grad = norm_backward(
        normed_two_grad, unit_two, scale_two, norm_gains[1]
    )
    middle_grad = upstream + middle_back
    branch_grad = middle_grad.astype(LOW)
    heads_grad = mm(branch_grad, proj_weight, NT).astype(LOW)

    grad_pieces = [
        depart(
            heads_grad,
            lambda source, d: lax.dynamic_slice_in_dim(source, d * own_width + c * chunk, chunk, 1),
        )
        for c in range(chunks)
    ]
    down_pair = gradient_pair(cotangent, hidden, 1)
    grad_pieces[0], down_pair = lax.optimization_barrier((grad_pieces[0], down_pair))

    mixed_pieces = []
    for c in range(chunks):
        if c == chunks - 1:
            late = lax.optimization_barrier((normed_two, before_grad, back))
            up_pair = gradient_pair(late[0], late[1], 1)
            grad_pieces[c], back, up_pair = lax.optimization_barrier(
                (grad_pieces[c], late[2], up_pair)
            )
        grad = arrange(grad_pieces[c], lambda d: (d * rows, 0), (length, chunk))
        back = attend_backward(qkv[c], grad, *kept[c], jnp.repeat(chunk_slopes[c], BLOCK)[None], BLOCK)
        mixed_pieces.append(
            depart(back, lambda source, d: lax.dynamic_slice_in_dim(source, d * rows, rows, 1))
        )
    late = lax.optimization_barrier((hidden, attended, branch_grad, back))
    block_out = (middle + mm(late[0], down_weight) + biases[5]).astype(LOW)
    proj_grad = mm(late[1], late[2], TN).astype(LOW)
    down_part = reduce_blocks(down_pair, 1, other_bits())
    up_part = reduce_blocks(up_pair, 1, other_bits())
    mixed_pieces[-1], down_part, up_part = lax.optimization_barrier(
        (mixed_pieces[-1], down_part, up_part)
    )
    mixed_grad = jnp.zeros((3, rows, width), LOW)
    for c in range(chunks):
        for shift, piece in enumerate(mixed_pieces[c]):
            mixed_grad = lax.dynamic_update_slice(
                mixed_grad, piece, (0, 0, ((here - shift) % ways) * own_width + c * chunk)
            )
    mixed_flat = jnp.concatenate([mixed_grad[0], mixed_grad[1], mixed_grad[2]], 1)

    if quick:
        owned_grad = combine(
            ways,
            mm(normed_one, mixed_flat, TN).astype(LOW),
            proj_grad,
            up_part,
            down_part,
        )
    else:
        proj_part = reduce_blocks(gradient_pair(attended, branch_grad, 1), 1, other_bits())
        qkv_part = reduce_blocks(gradient_pair(normed_one, mixed_flat, 1), 1, other_bits())
        owned_grad = owned_of(
            [
                collect(up_part, up_owner, 2),
                collect(qkv_part, qkv_owner, 1),
                collect(proj_part, proj_owner, 1),
                collect(down_part, down_owner, 2),
            ]
        )

    normed_one_grad = mm(mixed_flat, qkv_weight, NT)
    input_back, gain_one_grad, offset_one_grad = norm_backward(
        normed_one_grad, unit_one, scale_one, norm_gains[0]
    )
    tokens_grad = middle_grad + input_back

    def columns(value):
        return jnp.sum(value.astype(F32), axis=0)

    vectors = jnp.stack(
        [
            gain_one_grad,
            gain_two_grad,
            offset_one_grad,
            columns(mixed_grad[0]),
            columns(mixed_grad[2]),
            columns(branch_grad),
            offset_two_grad,
            columns(upstream),
        ]
    )
    vectors = jnp.concatenate([vectors, columns(before_grad).reshape(-1, width)], 0)

    owned_block = (MOMENTUM * owned_moment + owned_grad.astype(F32)).astype(LOW)
    gram = mm(owned_block, owned_block, NT)
    if quick:
        sums, steps, vectors = finish(ways, gram.astype(LOW), owned_block, owned_grad, vectors, widths)
    else:
        vectors = sum_everywhere(vectors)
        iterate = orthogonal(gram_total(gram), owned_block)
        sums = share(owned_grad, widths)
        steps = share(iterate, widths)
        sums[3], steps[3] = sums[3].T, steps[3].T

    def own_columns(matrix, count):
        return lax.dynamic_slice_in_dim(matrix, me * count, count, 1).astype(F32)

    gains_sum = own_columns(vectors[:2], gains_moment.shape[1])
    biases_sum = own_columns(vectors[2:8], biases_moment.shape[1])
    upbias_count = upbias_moment.shape[0]
    upbias_sum = lax.dynamic_slice_in_dim(
        vectors[8:].reshape(-1), me * upbias_count, upbias_count, 0
    )

    def state_of(moment, grad):
        return MOMENTUM * moment + grad.astype(F32)

    up_sum, qkv_sum, proj_sum, down_sum = [g.astype(F32) for g in sums]
    qkv_state = state_of(qkv_moment, qkv_sum)
    proj_state = state_of(proj_moment, proj_sum)
    up_state = state_of(up_moment, up_sum)
    down_state = state_of(down_moment, down_sum)
    gains_state = state_of(gains_moment, gains_sum)
    biases_state = state_of(biases_moment, biases_sum)
    upbias_state = state_of(upbias_moment, upbias_sum)

    def rate_of(shape):
        return -RATE_MATRIX * math.sqrt(max(shape))

    def step_of(owner, shape):
        return rate_of(shape) * steps[owner].astype(F32)

    qkv_new = own_columns(qkv_weight, qkv_state.shape[1]) + step_of(
        qkv_owner, qkv_weight.shape
    )
    proj_new = own_columns(proj_weight, proj_state.shape[1]) + step_of(
        proj_owner, proj_weight.shape
    )
    up_new = own_columns(up_weight, up_state.shape[1]) + step_of(
        up_owner, up_weight.shape
    )
    down_count = down_state.shape[0]
    down_rows = lax.dynamic_slice_in_dim(down_weight, me * down_count, down_count, 0).astype(F32)
    down_new = down_rows + step_of(down_owner, down_weight.shape)
    gains_new = own_columns(norm_gains, gains_state.shape[1]) - RATE_VECTOR * gains_state
    biases_new = own_columns(biases, biases_state.shape[1]) - RATE_VECTOR * biases_state
    upbias_new = (
        lax.dynamic_slice_in_dim(up_bias, me * upbias_count, upbias_count, 0)
        - RATE_VECTOR * upbias_state
    )
    return (
        block_out,
        tokens_grad,
        qkv_sum,
        proj_sum,
        up_sum,
        down_sum,
        gains_sum,
        biases_sum,
        upbias_sum,
        qkv_state,
        proj_state,
        up_state,
        down_state,
        gains_state,
        biases_state,
        upbias_state,
        qkv_new,
        proj_new,
        up_new,
        down_new,
        gains_new,
        biases_new,
        upbias_new,
    )


def solution(mesh):
    rows, columns, copied = P(("dp", "seq"), None), P(None, "dp"), P()

    return jax.shard_map(
        on_device,
        mesh=mesh,
        in_specs=(
            (rows, rows)
            + (copied,) * 8
            + (columns, columns, columns, P("dp", None), columns, columns, P("dp"))
        ),
        out_specs=(
            (rows, rows)
            + (columns, columns, columns, P("dp", None), columns, columns, P("dp")) * 3
        ),
        check_vma=False,
    )
```
